32 devices in a mesh: rep: 16 (over z, y, x), grp: 2 (over core).
Axes of the slice: x: 2, y: 2, z: 4, core: 2. Of those that a mesh axis runs over, the one named last changes fastest.
Arguments:
- tokens: bfloat16 [16384, 1600], P(('rep', 'grp')), may hold values from -6 to 6
- first_gain: bfloat16 [1600], P('grp'), may hold values from 0.099609375 to 1.8984375
- first_shift: bfloat16 [1600], P('grp'), may hold values from -3 to 3
- w_heads: bfloat16 [1600, 4800], P('grp'), may hold values from -1 to 1
- query_bias: bfloat16 [1600], P('grp'), may hold values from -3 to 3
- value_bias: bfloat16 [1600], P('grp'), may hold values from -3 to 3
- w_project: bfloat16 [1600, 1600], P('grp'), may hold values from -0.4375 to 0.4375
- project_bias: bfloat16 [1600], P('grp'), may hold values from -3 to 3
- second_gain: bfloat16 [1600], P('grp'), may hold values from 0.099609375 to 1.8984375
- second_shift: bfloat16 [1600], P('grp'), may hold values from -3 to 3
- w_expand: bfloat16 [1600, 6400], P('grp'), may hold values from -0.15625 to 0.15625
- expand_bias: bfloat16 [6400], P('grp'), may hold values from -3 to 3
- w_contract: bfloat16 [6400, 1600], P('grp'), may hold values from -0.078125 to 0.078125
- contract_bias: bfloat16 [1600], P('grp'), may hold values from -3 to 3
- cotangent: bfloat16 [16384, 1600], P(('rep', 'grp')), may hold values from -6 to 6
Outputs:
- block_out: bfloat16 [16384, 1600], P(('rep', 'grp'))
- grad_tokens: bfloat16 [16384, 1600], P(('rep', 'grp'))
- grad_first_gain: float32 [1600], P('grp')
- grad_first_shift: float32 [1600], P('grp')
- grad_w_heads: float32 [1600, 4800], P('grp', 'rep')
- grad_query_bias: float32 [1600], P('grp')
- grad_value_bias: float32 [1600], P('grp')
- grad_w_project: float32 [1600, 1600], P('grp', 'rep')
- grad_project_bias: float32 [1600], P('grp')
- grad_second_gain: float32 [1600], P('grp')
- grad_second_shift: float32 [1600], P('grp')
- grad_w_expand: float32 [1600, 6400], P('grp', 'rep')
- grad_expand_bias: float32 [6400], P('grp')
- grad_w_contract: float32 [6400, 1600], P('grp', 'rep')
- grad_contract_bias: float32 [1600], P('grp')
The draws below stay inside these ranges and needn't reach their ends.
All inputs are finite; a program needn't handle non-finite values.
Results may differ from the reference program's by a relative error of at most 0.013.
Values may be sent and summed in bfloat16 or wider, within the bound.
A program may use at most 576 MiB of HBM per device.

```python
import jax
import jax.numpy as jnp
from jax import lax

D = 1600
H = 25
HD = 64
FF = 6400
LEN = 512
TOKENS = 16384


def draw_w_heads(key, part):
    first_key = jax.random.fold_in(jax.random.fold_in(key, 17), 0)
    return (jnp.clip(jax.random.normal(first_key, (D, 3 * D), jnp.float32), -6.0, 6.0) * D ** (-0.5)).astype(jnp.bfloat16)


def strengthened(values, key, source, target, parts, factor):
    def block_of(dim):
        return (jnp.arange(values.shape[dim]) // (values.shape[dim] // parts)).reshape((-1,) + (1,) * (values.ndim - 1 - dim))

    near = jax.random.permutation(key, parts)[block_of(target)]
    second = (block_of(target) + parts // 2) % parts
    return jnp.where((block_of(source) == near) | (block_of(source) == second), factor * values, values)


def block_scale(stream_key, dims, pieces, low, high):
    loudness = 1.0
    for dim, shards_of in pieces:
        draws = jax.random.uniform(jax.random.fold_in(jax.random.fold_in(stream_key, 6), dim), (shards_of,), jnp.float32, low / len(pieces), high / len(pieces))
        loudness = loudness * jnp.repeat(jnp.exp(draws), dims[dim] // shards_of).reshape((-1,) + (1,) * (len(dims) - 1 - dim))
    return loudness


def scatter_about(key, dims, width, reach, cuts=(), dtype=jnp.bfloat16):
    values = jax.random.normal(key, dims, jnp.float32) * width
    if len(cuts) > 0:
        values = block_scale(key, dims, cuts, -0.22, 0.18) * values
    return jnp.clip(values, min=-reach, max=reach).astype(dtype)


def noise_with(stream_key, dims, width, reach, cuts, heavy, held_as=jnp.bfloat16):
    result = width * jax.random.normal(stream_key, dims, jnp.float32)
    if cuts:
        result = result * block_scale(stream_key, dims, cuts, -0.22, 0.18)
    return jnp.clip(strengthened(result, jax.random.fold_in(stream_key, 3), *heavy), -reach, reach).astype(held_as)


def setup_inputs(seed: int = 0) -> dict:
    arg_keys = jax.random.split(jax.random.key(seed), 16)
    return {
        "tokens": scatter_about(arg_keys[0], (TOKENS, D), 1.0, 6.0, ((0, 32),)),
        "first_gain": jnp.clip(1.0 + 0.18 * jax.random.normal(arg_keys[1], (D,), jnp.float32), 0.099609375, 1.8984375).astype(jnp.bfloat16),
        "first_shift": scatter_about(arg_keys[2], (D,), 0.3, 3.0, ((0, 2),)),
        "w_heads": draw_w_heads(jax.random.fold_in(arg_keys[15], 71), 0),
        "query_bias": scatter_about(arg_keys[4], (D,), 0.3, 3.0, ((0, 2),)),
        "value_bias": scatter_about(arg_keys[5], (D,), 0.3, 3.0, ((0, 2),)),
        "w_project": scatter_about(arg_keys[6], (D, D), (D // 8) ** -0.5, 0.4375, ((0, 2),)),
        "project_bias": scatter_about(arg_keys[7], (D,), 0.3, 3.0, ((0, 2),)),
        "second_gain": jnp.clip(1.0 + 0.18 * jax.random.normal(arg_keys[8], (D,), jnp.float32), 0.099609375, 1.8984375).astype(jnp.bfloat16),
        "second_shift": scatter_about(arg_keys[9], (D,), 0.3, 3.0, ((0, 2),)),
        "w_expand": scatter_about(arg_keys[10], (D, FF), D ** -0.5, 0.15625, ((0, 2),)),
        "expand_bias": scatter_about(arg_keys[11], (FF,), 0.5, 3.0, ((0, 2),)),
        "w_contract": scatter_about(arg_keys[12], (FF, D), FF ** -0.5, 0.078125, ((0, 2),)),
        "contract_bias": scatter_about(arg_keys[13], (D,), 0.3, 3.0, ((0, 2),)),
        "cotangent": noise_with(arg_keys[14], (TOKENS, D), 1.0, 6.0, ((0, 32),), (0, 1, 32, 2.75)),
    }


EPS = 1e-05
TANH_COEF = 0.7978845608028654
CUBIC = 0.044715

def norm_forward(row_block, norm_gain, norm_shift):
    centre = lax.optimization_barrier(jnp.mean(row_block, axis=-1, keepdims=True))
    centred = row_block - centre
    spread = lax.optimization_barrier(jnp.mean(centred * centred, axis=-1, keepdims=True))
    inverse = lax.rsqrt(spread + EPS)
    normed = centred * inverse
    return (normed * norm_gain + norm_shift, normed, inverse)

def norm_backward(incoming, normed, inverse, norm_gain):
    weighted = incoming * norm_gain
    first_mean = lax.optimization_barrier(jnp.mean(weighted, axis=-1, keepdims=True))
    second_mean = lax.optimization_barrier(jnp.mean(weighted * normed, axis=-1, keepdims=True))
    return inverse * (weighted - first_mean - normed * second_mean)

def gelu_parts(expanded):
    argument = TANH_COEF * (expanded + CUBIC * expanded * expanded * expanded)
    tangent = jnp.tanh(argument)
    gelu_value = 0.5 * expanded * (1.0 + tangent)
    gelu_slope = 0.5 * (1.0 + tangent) + 0.5 * expanded * (1.0 - tangent * tangent) * TANH_COEF * (1.0 + 3.0 * CUBIC * expanded * expanded)
    return (gelu_value, gelu_slope)

def causal_mask(length):
    return lax.broadcasted_iota(jnp.int32, (length, length), 0) >= lax.broadcasted_iota(jnp.int32, (length, length), 1)

def head_scores(queries, key_rows):
    factor = HD ** (-0.5)
    scores = jnp.einsum('qhd,khd->hqk', queries.astype(jnp.float32), key_rows.astype(jnp.float32)) * factor
    return jnp.where(causal_mask(queries.shape[0])[None], scores, -jnp.inf)

def attend_forward(queries, key_rows, value_rows):
    scores = head_scores(queries, key_rows)
    highest = lax.optimization_barrier(jnp.max(scores, axis=-1, keepdims=True))
    logsum = highest + jnp.log(lax.optimization_barrier(jnp.sum(jnp.exp(scores - highest), axis=-1, keepdims=True)))
    weights = jnp.exp(scores - logsum).astype(jnp.bfloat16)
    attended = jnp.einsum('hqk,khd->qhd', weights.astype(jnp.float32), value_rows.astype(jnp.float32))
    return (attended.astype(jnp.bfloat16), logsum)

def attend_backward(queries, key_rows, value_rows, logsum, grad_att):
    factor = HD ** (-0.5)
    scores = head_scores(queries, key_rows)
    probs = jnp.exp(scores - logsum)
    weights = probs.astype(jnp.bfloat16)
    grad_values = jnp.einsum('hqk,qhd->khd', weights.astype(jnp.float32), grad_att.astype(jnp.float32))
    grad_probs = jnp.einsum('qhd,khd->hqk', grad_att.astype(jnp.float32), value_rows.astype(jnp.float32))
    rowdot = lax.optimization_barrier(jnp.sum(probs * grad_probs, axis=-1, keepdims=True))
    grad_scores = (probs * (grad_probs - rowdot)).astype(jnp.bfloat16)
    grad_queries = jnp.einsum('hqk,khd->qhd', grad_scores.astype(jnp.float32), key_rows.astype(jnp.float32)) * factor
    grad_keys = jnp.einsum('hqk,qhd->khd', grad_scores.astype(jnp.float32), queries.astype(jnp.float32)) * factor
    return (grad_queries, grad_keys, grad_values)

def sequence_pass(params, row_block, cot_block):
    first_gain, first_shift, w_heads, query_bias, value_bias, w_project, project_bias, second_gain, second_shift, w_expand, expand_bias, w_contract, contract_bias = params
    inputs = row_block.astype(jnp.float32)
    first_out, first_normed, first_inv = norm_forward(inputs, first_gain.astype(jnp.float32), first_shift.astype(jnp.float32))
    first_act = first_out.astype(jnp.bfloat16)
    packed = jnp.dot(first_act, w_heads, preferred_element_type=jnp.float32)
    queries = (packed[:, :D] + query_bias.astype(jnp.float32)).astype(jnp.bfloat16).reshape(LEN, H, HD)
    key_rows = packed[:, D:2 * D].astype(jnp.bfloat16).reshape(LEN, H, HD)
    value_rows = (packed[:, 2 * D:] + value_bias.astype(jnp.float32)).astype(jnp.bfloat16).reshape(LEN, H, HD)
    attended, logsum = attend_forward(queries, key_rows, value_rows)
    attended_flat = attended.reshape(LEN, D)
    middle = inputs + jnp.dot(attended_flat, w_project, preferred_element_type=jnp.float32) + project_bias.astype(jnp.float32)
    second_out, second_normed, second_inv = norm_forward(middle, second_gain.astype(jnp.float32), second_shift.astype(jnp.float32))
    second_act = second_out.astype(jnp.bfloat16)
    expanded = jnp.dot(second_act, w_expand, preferred_element_type=jnp.float32) + expand_bias.astype(jnp.float32)
    gelu_value, gelu_slope = gelu_parts(expanded)
    activated = gelu_value.astype(jnp.bfloat16)
    block_out = (middle + jnp.dot(activated, w_contract, preferred_element_type=jnp.float32) + contract_bias.astype(jnp.float32)).astype(jnp.bfloat16)
    upstream = cot_block.astype(jnp.float32)
    grad_contract_bias = lax.optimization_barrier(jnp.sum(upstream, axis=0))
    grad_w_contract = jnp.dot(activated.T, cot_block, preferred_element_type=jnp.float32)
    grad_expanded = jnp.dot(cot_block, w_contract.T, preferred_element_type=jnp.float32) * gelu_slope
    grad_expand_bias = lax.optimization_barrier(jnp.sum(grad_expanded, axis=0))
    grad_expanded_bf = grad_expanded.astype(jnp.bfloat16)
    grad_w_expand = jnp.dot(second_act.T, grad_expanded_bf, preferred_element_type=jnp.float32)
    grad_second = jnp.dot(grad_expanded_bf, w_expand.T, preferred_element_type=jnp.float32)
    grad_second_gain = lax.optimization_barrier(jnp.sum(grad_second * second_normed, axis=0))
    grad_second_shift = lax.optimization_barrier(jnp.sum(grad_second, axis=0))
    grad_middle = upstream + norm_backward(grad_second, second_normed, second_inv, second_gain.astype(jnp.float32))
    grad_project_bias = lax.optimization_barrier(jnp.sum(grad_middle, axis=0))
    grad_middle_bf = grad_middle.astype(jnp.bfloat16)
    grad_w_project = jnp.dot(attended_flat.T, grad_middle_bf, preferred_element_type=jnp.float32)
    grad_attended = jnp.dot(grad_middle_bf, w_project.T, preferred_element_type=jnp.float32).astype(jnp.bfloat16).reshape(LEN, H, HD)
    grad_queries, grad_keys, grad_values = attend_backward(queries, key_rows, value_rows, logsum, grad_attended)
    grad_queries = grad_queries.reshape(LEN, D)
    grad_keys = grad_keys.reshape(LEN, D)
    grad_values = grad_values.reshape(LEN, D)
    grad_query_bias = lax.optimization_barrier(jnp.sum(grad_queries, axis=0))
    grad_value_bias = lax.optimization_barrier(jnp.sum(grad_values, axis=0))
    grad_packed = jnp.concatenate([grad_queries, grad_keys, grad_values], axis=1).astype(jnp.bfloat16)
    grad_w_heads = jnp.dot(first_act.T, grad_packed, preferred_element_type=jnp.float32)
    grad_first = jnp.dot(grad_packed, w_heads.T, preferred_element_type=jnp.float32)
    grad_first_gain = lax.optimization_barrier(jnp.sum(grad_first * first_normed, axis=0))
    grad_first_shift = lax.optimization_barrier(jnp.sum(grad_first, axis=0))
    grad_tokens = (grad_middle + norm_backward(grad_first, first_normed, first_inv, first_gain.astype(jnp.float32))).astype(jnp.bfloat16)
    grads = (grad_first_gain, grad_first_shift, grad_w_heads, grad_query_bias, grad_value_bias, grad_w_project, grad_project_bias, grad_second_gain, grad_second_shift, grad_w_expand, grad_expand_bias, grad_w_contract, grad_contract_bias)
    return (block_out, grad_tokens, grads)

def reference(tokens, first_gain, first_shift, w_heads, query_bias, value_bias, w_project, project_bias, second_gain, second_shift, w_expand, expand_bias, w_contract, contract_bias, cotangent):
    params = (first_gain, first_shift, w_heads, query_bias, value_bias, w_project, project_bias, second_gain, second_shift, w_expand, expand_bias, w_contract, contract_bias)
    count = tokens.shape[0] // LEN
    zeros = tuple((jnp.zeros(entry.shape, jnp.float32) for entry in params))

    def one_step(carry, pair):
        out_rows, grad_rows, grads = sequence_pass(params, pair[0], pair[1])
        return (tuple((running + fresh for running, fresh in zip(carry, grads))), (out_rows, grad_rows))
    totals, stacked = lax.scan(one_step, zeros, (tokens.reshape(count, LEN, D), cotangent.reshape(count, LEN, D)))
    return (stacked[0].reshape(count * LEN, D), stacked[1].reshape(count * LEN, D), totals[0], totals[1], totals[2], totals[3], totals[4], totals[5], totals[6], totals[7], totals[8], totals[9], totals[10], totals[11], totals[12])
```

```python
import jax
import jax.numpy as jnp
from jax import lax
from jax.sharding import PartitionSpec as P

H = 25
HD = 64
LEN = 512

EPS = 1e-05
TANH_COEF = 0.7978845608028654
CUBIC = 0.044715
F32 = jnp.float32
BF16 = jnp.bfloat16


def norm_forward(row_block, norm_gain, norm_shift):
    centre = jnp.mean(row_block, axis=-1, keepdims=True)
    centred = row_block - centre
    spread = jnp.mean(centred * centred, axis=-1, keepdims=True)
    inverse = lax.rsqrt(spread + EPS)
    normed = centred * inverse
    return (normed * norm_gain + norm_shift, normed, inverse)


def norm_backward(incoming, normed, inverse, norm_gain):
    weighted = incoming * norm_gain
    first_mean = jnp.mean(weighted, axis=-1, keepdims=True)
    second_mean = jnp.mean(weighted * normed, axis=-1, keepdims=True)
    return inverse * (weighted - first_mean - normed * second_mean)


def gelu_parts(expanded):
    argument = TANH_COEF * (expanded + CUBIC * expanded * expanded * expanded)
    tangent = jnp.tanh(argument)
    gelu_value = 0.5 * expanded * (1.0 + tangent)
    gelu_slope = 0.5 * (1.0 + tangent) + 0.5 * expanded * (1.0 - tangent * tangent) * TANH_COEF * (
        1.0 + 3.0 * CUBIC * expanded * expanded
    )
    return (gelu_value, gelu_slope)


def single_scores(query_head, key_head):
    length = query_head.shape[0]
    causal = lax.broadcasted_iota(jnp.int32, (length, length), 0) >= lax.broadcasted_iota(
        jnp.int32, (length, length), 1
    )
    scores = jnp.einsum(
        "qd,kd->qk", query_head, key_head, preferred_element_type=jnp.float32
    ) * HD ** (-0.5)
    return jnp.where(causal, scores, -jnp.inf)


def head_forward(triple):
    query_head, key_head, value_head = triple
    scores = single_scores(query_head, key_head)
    highest = jnp.max(scores, axis=-1, keepdims=True)
    logsum = highest + jnp.log(jnp.sum(jnp.exp(scores - highest), axis=-1, keepdims=True))
    weights = jnp.exp(scores - logsum).astype(jnp.bfloat16)
    attended = jnp.einsum("qk,kd->qd", weights, value_head, preferred_element_type=jnp.float32)
    return (attended.astype(jnp.bfloat16), logsum)


def head_backward(group):
    query_head, key_head, value_head, logsum, grad_head = group
    factor = HD ** (-0.5)
    scores = single_scores(query_head, key_head)
    probs = jnp.exp(scores - logsum)
    weights = probs.astype(jnp.bfloat16)
    grad_values = jnp.einsum("qk,qd->kd", weights, grad_head, preferred_element_type=jnp.float32)
    grad_probs = jnp.einsum("qd,kd->qk", grad_head, value_head, preferred_element_type=jnp.float32)
    rowdot = jnp.sum(probs * grad_probs, axis=-1, keepdims=True)
    grad_scores = (probs * (grad_probs - rowdot)).astype(jnp.bfloat16)
    grad_queries = (
        jnp.einsum("qk,kd->qd", grad_scores, key_head, preferred_element_type=jnp.float32) * factor
    )
    grad_keys = (
        jnp.einsum("qk,qd->kd", grad_scores, query_head, preferred_element_type=jnp.float32)
        * factor
    )
    return (grad_queries, grad_keys, grad_values)


def attend_forward(triple):
    queries, key_rows, value_rows = triple
    heads_first = tuple((jnp.transpose(entry, (1, 0, 2)) for entry in (queries, key_rows, value_rows)))
    attended, logsum = lax.map(head_forward, heads_first)
    return (jnp.transpose(attended, (1, 0, 2)), logsum)


def attend_backward(group):
    queries, key_rows, value_rows, logsum, grad_att = group
    heads_first = tuple((jnp.transpose(entry, (1, 0, 2)) for entry in (queries, key_rows, value_rows)))
    grad_first_heads = jnp.transpose(grad_att, (1, 0, 2))
    grad_queries, grad_keys, grad_values = lax.map(
        head_backward, (heads_first[0], heads_first[1], heads_first[2], logsum, grad_first_heads)
    )
    return (
        jnp.transpose(grad_queries, (1, 0, 2)),
        jnp.transpose(grad_keys, (1, 0, 2)),
        jnp.transpose(grad_values, (1, 0, 2)),
    )


def swap_group(x):
    return lax.ppermute(x, "grp", [(0, 1), (1, 0)])


def exchange(x, bit, count):
    return lax.ppermute(x, "rep", [(i, i ^ (1 << bit)) for i in range(count)])


def colour_orders(count):
    bits = list(range(count.bit_length() - 1))
    if len(bits) < 3:
        return [bits]
    first, second, third = bits[0], bits[1], bits[2]
    rest = bits[3:]
    return [
        [first, second, third] + rest,
        [second, first, third] + rest,
        [third, first, second] + rest,
    ]


def xor_places(order, rank):
    count = 1 << len(order)
    masks = []
    for place in range(count):
        mask = 0
        for depth, bit in enumerate(order):
            if place >> (len(order) - 1 - depth) & 1:
                mask |= 1 << bit
        masks.append(mask)
    return jnp.bitwise_xor(jnp.array(masks, jnp.int32), rank)


def halve(buf, order, count):
    for depth, bit in enumerate(order):
        half = buf.shape[0] // 2
        arrived = exchange(buf[half:], bit, count)
        total = buf[:half].astype(F32) + arrived.astype(F32)
        buf = total if depth == len(order) - 1 else total.astype(BF16)
    return buf[0]


def scatter_sum(transposed, rank, count):
    columns, rows = transposed.shape
    chunks = transposed.reshape(count, columns // count, rows)
    orders = colour_orders(count)
    cuts = [rows * i // len(orders) // 128 * 128 for i in range(len(orders))] + [rows]
    parts = []
    for i, order in enumerate(orders):
        lanes = chunks[:, :, cuts[i] : cuts[i + 1]]
        parts.append(halve(jnp.take(lanes, xor_places(order, rank), axis=0), order, count))
    return jnp.concatenate(parts, axis=1).T


def solution(mesh):
    count = mesh.shape["rep"]
    assert mesh.shape["grp"] == 2

    def weight_sum(rows_own, rows_away, cols, cols_away, rank):
        total = jnp.einsum("tc,td->cd", cols, rows_own, preferred_element_type=F32) + jnp.einsum(
            "tc,td->cd", cols_away, rows_away, preferred_element_type=F32
        )
        return scatter_sum(total.astype(BF16), rank, count)

    def per_device(
        tokens,
        first_gain,
        first_shift,
        w_heads,
        query_bias,
        value_bias,
        w_project,
        project_bias,
        second_gain,
        second_shift,
        w_expand,
        expand_bias,
        w_contract,
        contract_bias,
        cotangent,
    ):
        width = tokens.shape[1]
        total_rows = tokens.shape[0]
        seqs = total_rows // LEN
        side = lax.axis_index("grp")
        rank = lax.axis_index("rep")

        def gather(x):
            return lax.all_gather(x, "grp", axis=0, tiled=True)

        def half_of(x, which, axis=1):
            size = x.shape[axis] // 2
            return lax.dynamic_slice_in_dim(x, which * size, size, axis)

        smalls = (
            first_gain,
            first_shift,
            query_bias,
            value_bias,
            project_bias,
            second_gain,
            second_shift,
            contract_bias,
            expand_bias,
        )
        own_small = jnp.concatenate(smalls)
        away_small = swap_group(own_small)
        low = jnp.where(side == 0, own_small, away_small).astype(F32)
        high = jnp.where(side == 0, away_small, own_small).astype(F32)
        full_small = []
        at = 0
        for entry in smalls:
            n = entry.shape[0]
            full_small.append(jnp.concatenate([low[at : at + n], high[at : at + n]]))
            at += n
        (
            gain_one,
            shift_one,
            query_full,
            value_full,
            project_shift,
            gain_two,
            shift_two,
            contract_shift,
            expand_shift,
        ) = full_small
        heads_full = gather(w_heads)
        project_full = gather(w_project)
        expand_full = gather(w_expand)
        contract_full = gather(w_contract)
        cot_away = swap_group(cotangent)

        inputs = tokens.astype(F32)
        first_out, first_normed, first_inv = norm_forward(inputs, gain_one, shift_one)
        first_act = first_out.astype(BF16)
        packed = jnp.dot(first_act, heads_full, preferred_element_type=F32)
        queries = (packed[:, :width] + query_full).astype(BF16).reshape(seqs, LEN, H, HD)
        key_rows = packed[:, width : 2 * width].astype(BF16).reshape(seqs, LEN, H, HD)
        value_rows = (packed[:, 2 * width :] + value_full).astype(BF16).reshape(seqs, LEN, H, HD)
        attended, logsum = lax.map(attend_forward, (queries, key_rows, value_rows))
        attended_flat = attended.reshape(total_rows, width)
        middle = (
            inputs + jnp.dot(attended_flat, project_full, preferred_element_type=F32) + project_shift
        )
        second_out, second_normed, second_inv = norm_forward(middle, gain_two, shift_two)
        second_act = second_out.astype(BF16)
        expanded = jnp.dot(second_act, expand_full, preferred_element_type=F32) + expand_shift
        gelu_value, gelu_slope = gelu_parts(expanded)
        activated = gelu_value.astype(BF16)

        def rows_pair(x):
            return half_of(x, side), swap_group(half_of(x, 1 - side))

        upstream = cotangent.astype(F32)
        act_own, act_away = rows_pair(activated)
        out_w_contract = weight_sum(act_own, act_away, cotangent, cot_away, rank)

        grad_expanded = (
            jnp.einsum("td,fd->tf", cotangent, contract_full, preferred_element_type=F32) * gelu_slope
        )
        grad_expanded_bf = grad_expanded.astype(BF16)
        second_own, second_away = rows_pair(second_act)
        out_w_expand = weight_sum(
            second_own, second_away, grad_expanded_bf, swap_group(grad_expanded_bf), rank
        )
        grad_second = jnp.einsum(
            "tf,df->td", grad_expanded_bf, expand_full, preferred_element_type=F32
        )
        grad_middle = upstream + norm_backward(grad_second, second_normed, second_inv, gain_two)
        grad_middle_bf = grad_middle.astype(BF16)
        att_own, att_away = rows_pair(attended_flat)
        out_w_project = weight_sum(
            att_own, att_away, grad_middle_bf, swap_group(grad_middle_bf), rank
        )
        grad_attended = (
            jnp.einsum("td,ed->te", grad_middle_bf, project_full, preferred_element_type=F32)
            .astype(BF16)
            .reshape(seqs, LEN, H, HD)
        )
        grad_queries, grad_keys, grad_values = lax.map(
            attend_backward, (queries, key_rows, value_rows, logsum, grad_attended)
        )
        grad_queries = grad_queries.reshape(total_rows, width)
        grad_keys = grad_keys.reshape(total_rows, width)
        grad_values = grad_values.reshape(total_rows, width)
        grad_packed = jnp.concatenate([grad_queries, grad_keys, grad_values], axis=1).astype(BF16)
        first_own, first_away = rows_pair(first_act)
        out_w_heads = weight_sum(first_own, first_away, grad_packed, swap_group(grad_packed), rank)
        block_out = (
            middle
            + jnp.dot(activated, contract_full, preferred_element_type=F32)
            + contract_shift
        ).astype(BF16)
        grad_first = jnp.einsum("tc,dc->td", grad_packed, heads_full, preferred_element_type=F32)
        grad_tokens = (
            grad_middle + norm_backward(grad_first, first_normed, first_inv, gain_one)
        ).astype(BF16)

        sums = (
            jnp.sum(grad_first * first_normed, axis=0),
            jnp.sum(grad_first, axis=0),
            jnp.sum(grad_queries, axis=0),
            jnp.sum(grad_values, axis=0),
            jnp.sum(grad_middle, axis=0),
            jnp.sum(grad_second * second_normed, axis=0),
            jnp.sum(grad_second, axis=0),
            jnp.sum(upstream, axis=0),
            jnp.sum(grad_expanded, axis=0),
        )
        mine = jnp.concatenate([half_of(x, side, 0) for x in sums])
        theirs = jnp.concatenate([half_of(x, 1 - side, 0) for x in sums])
        vector = mine + swap_group(theirs)
        for bit in range(count.bit_length() - 1):
            vector = vector + exchange(vector, bit, count)
        finals = []
        at = 0
        for entry in sums:
            n = entry.shape[0] // 2
            finals.append(vector[at : at + n])
            at += n
        return (
            block_out,
            grad_tokens,
            finals[0],
            finals[1],
            out_w_heads,
            finals[2],
            finals[3],
            out_w_project,
            finals[4],
            finals[5],
            finals[6],
            out_w_expand,
            finals[8],
            out_w_contract,
            finals[7],
        )

    placed = (
        P(("rep", "grp"), None),
        P("grp"),
        P("grp"),
        P("grp", None),
        P("grp"),
        P("grp"),
        P("grp", None),
        P("grp"),
        P("grp"),
        P("grp"),
        P("grp", None),
        P("grp"),
        P("grp", None),
        P("grp"),
        P(("rep", "grp"), None),
    )
    return jax.shard_map(
        per_device,
        mesh=mesh,
        in_specs=placed,
        out_specs=(
            P(("rep", "grp"), None),
            P(("rep", "grp"), None),
            P("grp"),
            P("grp"),
            P("grp", "rep"),
            P("grp"),
            P("grp"),
            P("grp", "rep"),
            P("grp"),
            P("grp"),
            P("grp"),
            P("grp", "rep"),
            P("grp"),
            P("grp", "rep"),
            P("grp"),
        ),
        check_vma=False,
    )
```

```python
import functools

import jax
import jax.numpy as jnp
from jax import lax
from jax.experimental import pallas as pl
from jax.experimental.pallas import tpu as pltpu
from jax.sharding import PartitionSpec as P

H = 25
HD = 64
LEN = 512

EPS = 1e-05
TANH_COEF = 0.7978845608028654
CUBIC = 0.044715
F32 = jnp.float32
BF16 = jnp.bfloat16


def norm_forward(row_block, norm_gain, norm_shift):
    centre = jnp.mean(row_block, axis=-1, keepdims=True)
    centred = row_block - centre
    spread = jnp.mean(centred * centred, axis=-1, keepdims=True)
    inverse = lax.rsqrt(spread + EPS)
    normed = centred * inverse
    return (normed * norm_gain + norm_shift, normed, inverse)


def norm_backward(incoming, normed, inverse, norm_gain):
    weighted = incoming * norm_gain
    first_mean = jnp.mean(weighted, axis=-1, keepdims=True)
    second_mean = jnp.mean(weighted * normed, axis=-1, keepdims=True)
    return inverse * (weighted - first_mean - normed * second_mean)


def gelu_parts(expanded):
    argument = TANH_COEF * (expanded + CUBIC * expanded * expanded * expanded)
    tangent = jnp.tanh(argument)
    gelu_value = 0.5 * expanded * (1.0 + tangent)
    gelu_slope = 0.5 * (1.0 + tangent) + 0.5 * expanded * (1.0 - tangent * tangent) * TANH_COEF * (
        1.0 + 3.0 * CUBIC * expanded * expanded
    )
    return (gelu_value, gelu_slope)


def swap_group(x):
    return lax.ppermute(x, "grp", [(0, 1), (1, 0)])


def exchange(x, bit, count):
    return lax.ppermute(x, "rep", [(i, i ^ (1 << bit)) for i in range(count)])


def colour_orders(count):
    bits = list(range(count.bit_length() - 1))
    first, second, third = bits[0], bits[1], bits[2]
    rest = bits[3:]
    return [
        [first, second, third] + rest,
        [second, first, third] + rest,
        [third, first, second] + rest,
    ]


def colour_cuts(lanes):
    return [0, lanes // 384 * 128, lanes // 384 * 256, lanes]


def round_up(n, k):
    return -(-n // k) * k


def spread_kernel(meta, rank_ref, lo_ref, la_ref, ro_ref, ra_ref, *refs):
    count, chunk, group, orders, cuts, base, aliased = meta
    refs = refs[6:] if aliased else refs
    keeps, sends, stages, sem = refs[0:6:2], refs[1:6:2], refs[6:9], refs[9]
    step = pl.program_id(0)
    rank = rank_ref[0]
    padded = round_up(chunk, 16)
    half = count // 2
    right_own, right_away = ro_ref[...], ra_ref[...]

    def copy(k, slot, place, wait):
        src = stages[k].at[slot]
        rows = pl.ds(base, padded)
        if wait:
            pltpu.make_async_copy(src, keeps[k].at[0, rows, :], sem.at[k, slot]).wait()
            return

        @pl.when(place < half)
        def _():
            pltpu.make_async_copy(src, keeps[k].at[place, rows, :], sem.at[k, slot]).start()

        @pl.when(place >= half)
        def _():
            pltpu.make_async_copy(src, sends[k].at[place - half, rows, :], sem.at[k, slot]).start()

    for s in range(group):
        slot = s % 2 if group > 1 else lax.rem(step, 2)
        low = s * chunk // 16 * 16
        high = round_up((s + 1) * chunk, 16)
        off = s * chunk - low
        total = jnp.dot(lo_ref[low:high, :], right_own, preferred_element_type=F32)
        total += jnp.dot(la_ref[low:high, :], right_away, preferred_element_type=F32)
        if off or high - low != padded:
            total = total[off : off + chunk]
        total = total.astype(BF16)
        index = step * group + s
        mixed = jnp.bitwise_xor(index, rank)

        def release():
            for k in range(3):
                copy(k, slot, None, True)

        if group > 1 and s >= 2:
            release()
        elif group > 1:
            pl.when(step > 0)(release)
        else:
            pl.when(step > 1)(release)
        for k, order in enumerate(orders):
            place = jnp.int32(0)
            for depth, bit in enumerate(order):
                place += ((mixed >> bit) & 1) << (len(order) - 1 - depth)
            stages[k][slot, : total.shape[0], :] = total[:, cuts[k] : cuts[k + 1]]
            copy(k, slot, place, False)

    @pl.when(step == pl.num_programs(0) - 1)
    def _():
        for slot in range(2):
            for k in range(3):
                copy(k, slot, None, True)


def spread(rank, left_own, left_away, right_own, right_away, count, rows_total=None, base=0, into=None):
    columns, tokens = left_own.shape
    lanes = right_own.shape[1]
    chunk = columns // count
    group = 1
    while group * chunk % 16:
        group *= 2
    padded = round_up(chunk, 16)
    rows_total = rows_total or padded
    orders = colour_orders(count)
    cuts = colour_cuts(lanes)
    widths = [cuts[k + 1] - cuts[k] for k in range(3)]
    meta = (count, chunk, group, orders, cuts, base, into is not None)
    outs = [jax.ShapeDtypeStruct((count // 2, rows_total, widths[i // 2]), BF16) for i in range(6)]
    left = pl.BlockSpec((group * chunk, tokens), lambda i, *_: (i, 0))
    whole = pl.BlockSpec((tokens, lanes), lambda i, *_: (0, 0))
    anywhere = pl.BlockSpec(memory_space=pl.ANY)
    extra = list(into) if into is not None else []
    return pl.pallas_call(
        functools.partial(spread_kernel, meta),
        grid_spec=pltpu.PrefetchScalarGridSpec(
            num_scalar_prefetch=1,
            grid=(count // group,),
            in_specs=[left, left, whole, whole] + [anywhere] * len(extra),
            out_specs=[anywhere] * 6,
            scratch_shapes=[pltpu.VMEM((2, padded, w), BF16) for w in widths]
            + [pltpu.SemaphoreType.DMA((3, 2))],
        ),
        out_shape=outs,
        input_output_aliases={5 + i: i for i in range(len(extra))},
        name="spread",
    )(rank, left_own, left_away, right_own, right_away, *extra)


def merge_kernel(*refs):
    for k in range(3):
        keep_low, keep_high, came_low, came_high = refs[4 * k : 4 * k + 4]
        keep, send = refs[12 + 2 * k], refs[13 + 2 * k]
        keep[...] = (keep_low[...].astype(F32) + came_low[...].astype(F32)).astype(BF16)
        send[...] = (keep_high[...].astype(F32) + came_high[...].astype(F32)).astype(BF16)


def merge(keeps, arrived):
    half = keeps[0].shape[0] // 2
    ins, specs, outs, out_specs = [], [], [], []
    for keep, came in zip(keeps, arrived):
        shape = (1,) + keep.shape[1:]
        low = pl.BlockSpec(shape, lambda i: (i, 0, 0))
        high = pl.BlockSpec(shape, lambda i, half=half: (i + half, 0, 0))
        ins += [keep, keep, came, came]
        specs += [low, high, low, high]
        outs += [jax.ShapeDtypeStruct((half,) + keep.shape[1:], BF16)] * 2
        out_specs += [low, low]
    res = pl.pallas_call(
        merge_kernel, grid=(half,), in_specs=specs, out_specs=out_specs, out_shape=outs, name="merge"
    )(*ins)
    return res[0::2], res[1::2]


def finish_kernel(cuts, members, *refs):
    outs = refs[6:]
    for k in range(3):
        total = refs[2 * k][0].astype(F32) + refs[2 * k + 1][0].astype(F32)
        for (base, chunk), out in zip(members, outs):
            padded = round_up(chunk, 16)
            turned = total[base : base + padded].T
            out[cuts[k] : cuts[k + 1], :] = turned[:, :chunk]


def finish(keeps, arrived, lanes, members):
    cuts = colour_cuts(lanes)
    ins = []
    for keep, came in zip(keeps, arrived):
        ins += [keep, came]
    return pl.pallas_call(
        functools.partial(finish_kernel, cuts, members),
        out_shape=[jax.ShapeDtypeStruct((lanes, chunk), F32) for _, chunk in members],
        name="finish",
    )(*ins)


def reduce_chunks(buffers, count, lanes, members):
    orders = colour_orders(count)
    keeps, sends = buffers[0::2], buffers[1::2]
    for depth in range(len(orders[0])):
        arrived = [exchange(sends[k], orders[k][depth], count) for k in range(3)]
        if depth < len(orders[0]) - 1:
            keeps, sends = merge(keeps, arrived)
    return finish(keeps, arrived, lanes, members)


QB=256

NT = (((1,), (1,)), ((), ()))

def lane_ids(shape):
    return lax.broadcasted_iota(jnp.int32, shape, len(shape)-1)

def pair_of(left, right):
    return jnp.concatenate([left[:, HD:], right[:, :HD]], axis=1)

def causal_fill(scores, fill):
    rows, cols = scores.shape
    shift = cols - rows
    keep = lax.broadcasted_iota(jnp.int32, (rows, rows), 0) >= lax.broadcasted_iota(jnp.int32, (rows, rows), 1)
    diag = jnp.where(keep, scores[:, shift:], fill)
    return diag if shift == 0 else jnp.concatenate([scores[:, :shift], diag], axis=1)

def attend_kernel(q_ref, ka_ref, kb_ref, v_ref, o_ref, lse_ref):
    p = pl.program_id(1)
    lanes = lane_ids((LEN, 2 * HD))
    q = q_ref[...] * BF16(HD ** -0.5)
    k = pair_of(ka_ref[...], kb_ref[...])
    v = v_ref[...]
    for h in range(2):
        qh = jnp.where((lanes < HD) == (h == 0), q, BF16(0))
        for at in range(0, LEN, QB):
            end = at + QB
            s = lax.dot_general(qh[at:end], k[:end], NT, preferred_element_type=F32)
            s = causal_fill(s, -jnp.inf)
            m = jnp.max(s, axis=1, keepdims=True)
            e = jnp.exp(s - m)
            l = jnp.sum(e, axis=1, keepdims=True)
            o = jnp.dot(e.astype(BF16), v[:end], preferred_element_type=F32) / l
            ln = lanes[at:end]
            if h == 0:
                o_ref[at:end, :] = o.astype(BF16)
            else:
                o_ref[at:end, :] = jnp.where(ln < HD, o_ref[at:end, :], o.astype(BF16))
            lse_ref[at:end, :] = jnp.where(ln == 2 * p + h, m + jnp.log(l), lse_ref[at:end, :])

def attend(packed):
    rows = packed.shape[0]
    width = packed.shape[1] // 3
    seqs = rows // LEN
    pairs = (H + 1) // 2
    kb, vb = width // (2 * HD), 2 * width // (2 * HD)
    blk = lambda f: pl.BlockSpec((LEN, 2 * HD), f)
    return pl.pallas_call(
        attend_kernel,
        grid=(seqs, pairs),
        in_specs=[blk(lambda s, p: (s, p)), blk(lambda s, p: (s, p + kb)), blk(lambda s, p: (s, p + kb + 1)), blk(lambda s, p: (s, p + vb))],
        out_specs=[blk(lambda s, p: (s, p)), blk(lambda s, p: (s, 0))],
        out_shape=[jax.ShapeDtypeStruct((rows, width), BF16), jax.ShapeDtypeStruct((rows, 2 * HD), F32)],
        name="attend",
    )(packed, packed, packed, packed)

def attend_back_kernel(q_ref, ka_ref, kb_ref, v_ref, do_ref, o_ref, lse_ref, out_ref, dq_ref):
    p = pl.program_id(1)
    lanes = lane_ids((LEN, 2 * HD))
    low = lanes < HD
    q = q_ref[...] * BF16(HD ** -0.5)
    k = pair_of(ka_ref[...], kb_ref[...])
    real = lanes + 2 * HD * p < H * HD
    v = jnp.where(real, v_ref[...], BF16(0))
    dot_t = do_ref[...]
    do = jnp.where(real, dot_t.T, BF16(0))
    o = jnp.where(real, o_ref[...], BF16(0))
    prod = do.astype(F32) * o.astype(F32)
    lse = lse_ref[...]
    q_t = q.T
    for h in range(2):
        mine = low if h == 0 else jnp.logical_not(low)
        qh = jnp.where(mine, q, BF16(0))
        doh = jnp.where(mine, do, BF16(0))
        delta = jnp.sum(jnp.where(mine, prod, 0.0), axis=1, keepdims=True)
        norm = jnp.sum(jnp.where(lanes == 2 * p + h, lse, 0.0), axis=1, keepdims=True)
        rows = slice(h * HD, (h + 1) * HD)
        dk = None
        for at in range(LEN - QB, -1, -QB):
            end = at + QB
            s = lax.dot_general(qh[at:end], k[:end], NT, preferred_element_type=F32)
            w = causal_fill(jnp.exp(s - norm[at:end]), 0.0)
            wb = w.astype(BF16)
            dp = lax.dot_general(doh[at:end], v[:end], NT, preferred_element_type=F32)
            ds = (w * (dp - delta[at:end])).astype(BF16)
            dq = jnp.dot(ds, k[:end], preferred_element_type=F32) * HD ** -0.5
            if h == 0:
                dq_ref[at:end, :] = dq.astype(BF16)
            else:
                dq_ref[at:end, :] = jnp.where(low[at:end], dq_ref[at:end, :], dq.astype(BF16))
            dk_part = jnp.dot(q_t[rows, at:end], ds, preferred_element_type=F32)
            dv_part = jnp.dot(dot_t[rows, at:end], wb, preferred_element_type=F32)
            if dk is None:
                dk, dv = dk_part, dv_part
            else:
                dk = jnp.concatenate([dk[:, :end] + dk_part, dk[:, end:]], axis=1)
                dv = jnp.concatenate([dv[:, :end] + dv_part, dv[:, end:]], axis=1)
        out_ref[1, rows, :] = dk.astype(BF16)
        out_ref[2, rows, :] = dv.astype(BF16)
    out_ref[0, :, :] = dq_ref[...].T

def attend_back(packed, grad_t, attended, lse):
    rows = packed.shape[0]
    width = packed.shape[1] // 3
    seqs = rows // LEN
    pairs = (H + 1) // 2
    kb, vb = width // (2 * HD), 2 * width // (2 * HD)
    blk = lambda f: pl.BlockSpec((LEN, 2 * HD), f)
    out = pl.pallas_call(
        attend_back_kernel,
        grid=(seqs, pairs),
        in_specs=[blk(lambda s, p: (s, p)), blk(lambda s, p: (s, p + kb)), blk(lambda s, p: (s, p + kb + 1)), blk(lambda s, p: (s, p + vb)),
                  pl.BlockSpec((2 * HD, LEN), lambda s, p: (p, s)), blk(lambda s, p: (s, p)), blk(lambda s, p: (s, 0))],
        out_specs=pl.BlockSpec((3, 2 * HD, LEN), lambda s, p: (0, p, s)),
        out_shape=jax.ShapeDtypeStruct((3, width, rows), BF16),
        scratch_shapes=[pltpu.VMEM((LEN, 2 * HD), BF16)],
        name="attend_back",
    )(packed, packed, packed, packed, grad_t, attended, lse)
    return out.reshape(3 * width, rows)


def solution(mesh):
    count = mesh.shape["rep"]
    assert mesh.shape["grp"] == 2

    def per_device(
        tokens,
        first_gain,
        first_shift,
        w_heads,
        query_bias,
        value_bias,
        w_project,
        project_bias,
        second_gain,
        second_shift,
        w_expand,
        expand_bias,
        w_contract,
        contract_bias,
        cotangent,
    ):
        width = tokens.shape[1]
        total_rows = tokens.shape[0]
        seqs = total_rows // LEN
        side = lax.axis_index("grp")
        rank = jnp.reshape(lax.axis_index("rep"), (1,))

        def gather(x):
            return lax.all_gather(x, "grp", axis=0, tiled=True)

        def half_of(x, which, axis=1):
            size = x.shape[axis] // 2
            return lax.dynamic_slice_in_dim(x, which * size, size, axis)

        smalls = (
            first_gain,
            first_shift,
            query_bias,
            value_bias,
            project_bias,
            second_gain,
            second_shift,
            contract_bias,
            expand_bias,
        )
        own_small = jnp.concatenate(smalls)
        away_small = swap_group(own_small)
        low = jnp.where(side == 0, own_small, away_small).astype(F32)
        high = jnp.where(side == 0, away_small, own_small).astype(F32)
        full_small = []
        at = 0
        for entry in smalls:
            n = entry.shape[0]
            full_small.append(jnp.concatenate([low[at : at + n], high[at : at + n]]))
            at += n
        (
            gain_one,
            shift_one,
            query_full,
            value_full,
            project_shift,
            gain_two,
            shift_two,
            contract_shift,
            expand_shift,
        ) = full_small
        heads_full = gather(w_heads)
        project_full = gather(w_project)
        expand_full = gather(w_expand)
        contract_full = gather(w_contract)
        cot_away = swap_group(cotangent)

        inputs = tokens.astype(F32)
        first_out, first_normed, first_inv = norm_forward(inputs, gain_one, shift_one)
        first_act = first_out.astype(BF16)
        packed = jnp.dot(first_act, heads_full, preferred_element_type=F32)
        packed = (packed + jnp.concatenate([query_full, jnp.zeros_like(query_full), value_full])).astype(BF16)
        attended_flat, logsum = attend(packed)
        middle = (
            inputs + jnp.dot(attended_flat, project_full, preferred_element_type=F32) + project_shift
        )
        second_out, second_normed, second_inv = norm_forward(middle, gain_two, shift_two)
        second_act = second_out.astype(BF16)
        expanded = jnp.dot(second_act, expand_full, preferred_element_type=F32) + expand_shift
        gelu_value, gelu_slope = gelu_parts(expanded)
        activated = gelu_value.astype(BF16)

        def rows_pair(x):
            return half_of(x, side), swap_group(half_of(x, 1 - side))

        upstream = cotangent.astype(F32)
        act_own, act_away = rows_pair(activated)
        chunk_c = width // count
        (out_w_contract,) = reduce_chunks(
            spread(rank, cotangent.T, cot_away.T, act_own, act_away, count), count, act_own.shape[1], [(0, chunk_c)]
        )

        grad_expanded = (
            jnp.einsum("td,fd->tf", cotangent, contract_full, preferred_element_type=F32) * gelu_slope
        )
        grad_expanded_bf = grad_expanded.astype(BF16)
        second_own, second_away = rows_pair(second_act)
        ge_t = grad_expanded_bf.T
        grad_second = jnp.einsum(
            "tf,df->td", grad_expanded_bf, expand_full, preferred_element_type=F32
        )
        grad_middle = upstream + norm_backward(grad_second, second_normed, second_inv, gain_two)
        grad_middle_bf = grad_middle.astype(BF16)
        att_own, att_away = rows_pair(attended_flat)
        gm_t = grad_middle_bf.T
        chunk_e = ge_t.shape[0] // count
        pad_e = round_up(chunk_e, 16)
        both = pad_e + round_up(chunk_c, 16)
        buffers = spread(rank, ge_t, swap_group(ge_t), second_own, second_away, count, both, 0)
        buffers = spread(rank, gm_t, swap_group(gm_t), att_own, att_away, count, both, pad_e, buffers)
        out_w_expand, out_w_project = reduce_chunks(
            buffers, count, att_own.shape[1], [(0, chunk_e), (pad_e, chunk_c)]
        )
        grad_att_t = jnp.einsum("td,ed->et", grad_middle_bf, project_full, preferred_element_type=F32).astype(BF16)
        gp_t = attend_back(packed, grad_att_t, attended_flat, logsum)
        first_own, first_away = rows_pair(first_act)
        (out_w_heads,) = reduce_chunks(
            spread(rank, gp_t, swap_group(gp_t), first_own, first_away, count), count, first_own.shape[1], [(0, gp_t.shape[0] // count)]
        )
        grad_packed = gp_t.T
        grad_queries = grad_packed[:, :width].astype(F32)
        grad_values = grad_packed[:, 2 * width :].astype(F32)
        block_out = (
            middle
            + jnp.dot(activated, contract_full, preferred_element_type=F32)
            + contract_shift
        ).astype(BF16)
        grad_first = jnp.einsum("tc,dc->td", grad_packed, heads_full, preferred_element_type=F32)
        grad_tokens = (
            grad_middle + norm_backward(grad_first, first_normed, first_inv, gain_one)
        ).astype(BF16)

        sums = (
            jnp.sum(grad_first * first_normed, axis=0),
            jnp.sum(grad_first, axis=0),
            jnp.sum(grad_queries, axis=0),
            jnp.sum(grad_values, axis=0),
            jnp.sum(grad_middle, axis=0),
            jnp.sum(grad_second * second_normed, axis=0),
            jnp.sum(grad_second, axis=0),
            jnp.sum(upstream, axis=0),
            jnp.sum(grad_expanded, axis=0),
        )
        mine = jnp.concatenate([half_of(x, side, 0) for x in sums])
        theirs = jnp.concatenate([half_of(x, 1 - side, 0) for x in sums])
        vector = mine + swap_group(theirs)
        for bit in range(count.bit_length() - 1):
            vector = vector + exchange(vector, bit, count)
        finals = []
        at = 0
        for entry in sums:
            n = entry.shape[0] // 2
            finals.append(vector[at : at + n])
            at += n
        return (
            block_out,
            grad_tokens,
            finals[0],
            finals[1],
            out_w_heads,
            finals[2],
            finals[3],
            out_w_project,
            finals[4],
            finals[5],
            finals[6],
            out_w_expand,
            finals[8],
            out_w_contract,
            finals[7],
        )

    placed = (
        P(("rep", "grp"), None),
        P("grp"),
        P("grp"),
        P("grp", None),
        P("grp"),
        P("grp"),
        P("grp", None),
        P("grp"),
        P("grp"),
        P("grp"),
        P("grp", None),
        P("grp"),
        P("grp", None),
        P("grp"),
        P(("rep", "grp"), None),
    )
    return jax.shard_map(
        per_device,
        mesh=mesh,
        in_specs=placed,
        out_specs=(
            P(("rep", "grp"), None),
            P(("rep", "grp"), None),
            P("grp"),
            P("grp"),
            P("grp", "rep"),
            P("grp"),
            P("grp"),
            P("grp", "rep"),
            P("grp"),
            P("grp"),
            P("grp"),
            P("grp", "rep"),
            P("grp"),
            P("grp", "rep"),
            P("grp"),
        ),
        check_vma=False,
    )
```

```python
import functools
import types

import jax
import jax.numpy as jnp
from jax import lax
from jax.experimental import pallas as pl
from jax.experimental.pallas import tpu as pltpu
from jax.sharding import PartitionSpec as P


HD = 64
LEN = 512
QB = 256
EPS = 1e-05
TANH_COEF = 0.7978845608028654
CUBIC = 0.044715
F32 = jnp.float32
BF16 = jnp.bfloat16
NT = (((1,), (1,)), ((), ()))
VMEM_LIMIT = 60 * 1024 * 1024


def shape_of(shape, dtype):
    return jax.ShapeDtypeStruct(shape, dtype)


def params():
    return pltpu.CompilerParams(vmem_limit_bytes=VMEM_LIMIT)


def cost(flops, moved):
    return pl.CostEstimate(flops=int(flops), bytes_accessed=int(moved), transcendentals=0)


def round_up(n, k):
    return -(-n // k) * k


def swap_group(x):
    return lax.ppermute(x, "grp", [(0, 1), (1, 0)])


def exchange(x, mask, count):
    return lax.ppermute(x, "rep", [(i, i ^ mask) for i in range(count)])


def row_sums(x):
    ones = jnp.ones((8, x.shape[1]), BF16)
    return lax.dot_general(ones, x, NT, preferred_element_type=F32)


def joined_dot(left_one, left_two, right_one, right_two):
    missing = left_one.shape[1] - right_one.shape[0]
    rights = [right_one, right_two]
    if missing:
        fill = jnp.zeros((missing, right_one.shape[1]), right_one.dtype)
        rights = [right_one, fill, right_two, fill]
    left = jnp.concatenate([left_one, left_two], axis=1)
    return jnp.dot(left, jnp.concatenate(rights, axis=0), preferred_element_type=F32)


def stream(step, steps, sources, buffers, sem):
    @pl.when(step == 0)
    def _():
        for i in range(steps):
            for j, (source, buffer) in enumerate(zip(sources, buffers)):
                pltpu.make_async_copy(source(i), buffer.at[i], sem.at[j, i]).start()

    for j, (source, buffer) in enumerate(zip(sources, buffers)):
        pltpu.make_async_copy(source(0), buffer.at[step], sem.at[j, step]).wait()


ANYWHERE = pl.BlockSpec(memory_space=pl.ANY)


def store_pair(side, value, own_ref, away_ref):
    half = value.shape[1] // 2
    fill = jnp.zeros((value.shape[0], own_ref.shape[1] - half), value.dtype)
    low = jnp.concatenate([value[:, :half], fill], axis=1)
    high = jnp.concatenate([value[:, half:], fill], axis=1)

    @pl.when(side == 0)
    def _():
        own_ref[...] = low
        away_ref[...] = high

    @pl.when(side == 1)
    def _():
        own_ref[...] = high
        away_ref[...] = low


def gather_kernel(*refs):
    out = refs[-1]
    out[...] = jnp.zeros_like(out)
    for i, ref in enumerate(refs[:-1]):
        out[i : i + 1, : ref.shape[0]] = ref[...].astype(F32).reshape(1, ref.shape[0])


def gather_smalls(smalls):
    widest = max(x.shape[0] for x in smalls)
    return pl.pallas_call(gather_kernel, out_shape=shape_of((16, widest), F32), name="gather")(*smalls)


def unpack_kernel(side_ref, own_ref, away_ref, rows_ref, cols_ref, packed_ref):
    half = rows_ref.shape[1] // 2
    first = side_ref[0] == 0
    own, away = own_ref[0:8, :half], away_ref[0:8, :half]
    low = jnp.where(first, own, away)
    high = jnp.where(first, away, own)
    rows = jnp.concatenate([low, high], axis=1)
    rows_ref[...] = rows
    cols_ref[...] = jnp.concatenate([rows, jnp.zeros((120, 2 * half), F32)], axis=0).T
    packed_ref[...] = jnp.concatenate([rows[2:3], jnp.zeros((1, 2 * half), F32), rows[3:4]], axis=1)


def unpack_smalls(side, own, away, width):
    vmem = pl.BlockSpec(memory_space=pltpu.VMEM)
    return pl.pallas_call(
        unpack_kernel,
        in_specs=[pl.BlockSpec(memory_space=pltpu.SMEM), vmem, vmem],
        out_shape=[shape_of((8, width), F32), shape_of((width, 128), F32), shape_of((1, 3 * width), F32)],
        name="unpack",
    )(side, own, away)


def collect_kernel(side_ref, pack_ref, eb_ref, *refs):
    rows, (mine_ref, theirs_ref) = refs[:-2], refs[-2:]
    width = rows[0].shape[1]
    half = width // 2
    first = side_ref[0] == 0
    pack = pack_ref[0:1, :]
    full = [r[0:1, :] for r in rows[:2]] + [pack[:, :width], pack[:, 2 * width :]]
    full += [r[0:1, :] for r in rows[2:]]
    full = jnp.concatenate(full, axis=0)
    low, high = full[:, :half], full[:, half:]
    mine_ref[...] = jnp.zeros_like(mine_ref)
    theirs_ref[...] = jnp.zeros_like(theirs_ref)
    mine_ref[0:8, :half] = jnp.where(first, low, high)
    theirs_ref[0:8, :half] = jnp.where(first, high, low)
    units = mine_ref.shape[1]
    low, high = eb_ref[0:1, :units], eb_ref[0:1, units:]
    mine_ref[8:9, :] = jnp.where(first, low, high)
    theirs_ref[8:9, :] = jnp.where(first, high, low)


def collect(side, pack, eb, rows):
    vmem = pl.BlockSpec(memory_space=pltpu.VMEM)
    out = shape_of((16, eb.shape[1] // 2), F32)
    return pl.pallas_call(
        collect_kernel,
        in_specs=[pl.BlockSpec(memory_space=pltpu.SMEM)] + [vmem] * (2 + len(rows)),
        out_shape=[out, out],
        name="collect",
    )(side, pack, eb, *rows)


def add_kernel(a_ref, b_ref, out_ref):
    out_ref[...] = a_ref[...] + b_ref[...]


def add(a, b):
    return pl.pallas_call(add_kernel, out_shape=shape_of(a.shape, a.dtype), name="add")(a, b)


def divide_kernel(a_ref, b_ref, *outs):
    total = a_ref[...] + b_ref[...]
    for i, out in enumerate(outs):
        out[...] = total[i : i + 1, : out.shape[0]].reshape(out.shape[0])


def divide(a, b, sizes):
    return pl.pallas_call(
        divide_kernel, out_shape=[shape_of((n,), F32) for n in sizes], name="divide"
    )(a, b)


def prep_kernel(side_ref, x_ref, c_ref, cols_ref, own_ref, away_ref, cot_ref, sum_ref, act_ref):
    x = x_ref[...].astype(F32)
    half = x.shape[0] // 2
    side = side_ref[0]
    centred = x - jnp.mean(x, axis=0, keepdims=True)
    inverse = lax.rsqrt(jnp.mean(centred * centred, axis=0, keepdims=True) + EPS)
    act_ref[...] = (centred * inverse * cols_ref[:, 0:1] + cols_ref[:, 1:2]).astype(BF16)
    for ref, which in ((own_ref, side), (away_ref, 1 - side)):
        ref[:, :half] = act_ref[pl.ds(pl.multiple_of(which * half, 16), half), :].T
        ref[:, half:] = jnp.zeros((ref.shape[0], ref.shape[1] - half), BF16)
    cot = c_ref[...].T
    cot_ref[...] = cot
    part = jnp.sum(cot.astype(F32), axis=0, keepdims=True)
    part = jnp.broadcast_to(part, sum_ref.shape)

    @pl.when(pl.program_id(0) == 0)
    def _():
        sum_ref[...] = part

    @pl.when(pl.program_id(0) > 0)
    def _():
        sum_ref[...] += part


def prep(side, tok_t, cot_t, cols):
    width, rows = tok_t.shape
    block = min(256, rows)
    half = round_up(width // 2, 128)
    nat = pl.BlockSpec((block, width), lambda i, *_: (i, 0))
    turned = pl.BlockSpec((width, block), lambda i, *_: (0, i))
    pair = pl.BlockSpec((block, half), lambda i, *_: (i, 0))
    return pl.pallas_call(
        prep_kernel,
        grid_spec=pltpu.PrefetchScalarGridSpec(
            num_scalar_prefetch=1,
            grid=(rows // block,),
            in_specs=[turned, turned, pl.BlockSpec((width, 128), lambda i, *_: (0, 0))],
            out_specs=[pair, pair, nat, pl.BlockSpec((8, width), lambda i, *_: (0, 0))],
            scratch_shapes=[pltpu.VMEM((width, block), BF16)],
        ),
        out_shape=[
            shape_of((rows, half), BF16),
            shape_of((rows, half), BF16),
            shape_of((rows, width), BF16),
            shape_of((8, width), F32),
        ],
        compiler_params=params(),
        cost_estimate=cost(0, 8 * rows * width),
        name="prep",
    )(side, tok_t, cot_t, cols)


def heads_kernel(own_ref, away_ref, wo_ref, wa_ref, bias_ref, out_ref):
    total = joined_dot(own_ref[...], away_ref[...], wo_ref[...], wa_ref[...])
    out_ref[...] = (total + bias_ref[...]).astype(BF16)


def heads_project(own, away, w_own, w_away, bias):
    rows, wide = own.shape
    half, columns = w_own.shape
    tile = 1280
    left = pl.BlockSpec((rows, wide), lambda i: (0, 0))
    right = pl.BlockSpec((half, tile), lambda i: (0, i))
    return pl.pallas_call(
        heads_kernel,
        grid=(pl.cdiv(columns, tile),),
        in_specs=[left, left, right, right, pl.BlockSpec((1, tile), lambda i: (0, i))],
        out_specs=pl.BlockSpec((rows, tile), lambda i: (0, i)),
        out_shape=shape_of((rows, columns), BF16),
        compiler_params=params(),
        cost_estimate=cost(4 * rows * half * columns, 4 * half * columns + 2 * rows * columns),
        name="heads",
    )(own, away, w_own, w_away, bias)


def lane_ids(shape):
    return lax.broadcasted_iota(jnp.int32, shape, len(shape) - 1)


def pair_of(left, right):
    return jnp.concatenate([left[:, HD:], right[:, :HD]], axis=1)


def causal_fill(scores, fill):
    rows, cols = scores.shape
    shift = cols - rows
    keep = lax.broadcasted_iota(jnp.int32, (rows, rows), 0) >= lax.broadcasted_iota(
        jnp.int32, (rows, rows), 1
    )
    diag = jnp.where(keep, scores[:, shift:], fill)
    return diag if shift == 0 else jnp.concatenate([scores[:, :shift], diag], axis=1)


def attend_kernel(q_ref, ka_ref, kb_ref, v_ref, o_ref, lse_ref):
    p = pl.program_id(1)
    lanes = lane_ids((LEN, 2 * HD))
    q = q_ref[...] * BF16(HD**-0.5)
    k = pair_of(ka_ref[...], kb_ref[...])
    v = jnp.concatenate([v_ref[...], jnp.ones((LEN, 2 * HD), BF16)], axis=1)
    for at in range(0, LEN, QB):
        end = at + QB
        low = lanes[at:end] < HD
        parts = []
        for h in range(2):
            qh = jnp.where(low == (h == 0), q[at:end], BF16(0))
            s = lax.dot_general(qh, k[:end], NT, preferred_element_type=F32)
            s = causal_fill(s, -jnp.inf)
            m = jnp.max(s, axis=1, keepdims=True)
            e = jnp.exp(s - m)
            both = jnp.dot(e.astype(BF16), v[:end], preferred_element_type=F32)
            parts.append((m, both[:, : 2 * HD], both[:, 2 * HD :]))
        out = jnp.where(low, parts[0][1], parts[1][1])
        sums = jnp.where(low, parts[0][2], parts[1][2])
        o_ref[at:end, :] = (out / sums).astype(BF16)
        ln = lanes[at:end]
        for h in range(2):
            value = parts[h][0] + jnp.log(parts[h][2])
            lse_ref[at:end, :] = jnp.where(ln == 2 * p + h, value, lse_ref[at:end, :])


def attend(packed):
    rows = packed.shape[0]
    width = packed.shape[1] // 3
    seqs = rows // LEN
    pairs = pl.cdiv(width, 2 * HD)
    kb, vb = width // (2 * HD), 2 * width // (2 * HD)

    def blk(f):
        return pl.BlockSpec((LEN, 2 * HD), f)

    return pl.pallas_call(
        attend_kernel,
        grid=(seqs, pairs),
        in_specs=[
            blk(lambda s, p: (s, p)),
            blk(lambda s, p: (s, p + kb)),
            blk(lambda s, p: (s, p + kb + 1)),
            blk(lambda s, p: (s, p + vb)),
        ],
        out_specs=[blk(lambda s, p: (s, p)), blk(lambda s, p: (s, 0))],
        out_shape=[shape_of((rows, width), BF16), shape_of((rows, 2 * HD), F32)],
        cost_estimate=cost(rows * LEN * width * 12, 8 * rows * width),
        name="attend",
    )(packed, packed, packed, packed)


def attend_back_kernel(width, q_ref, ka_ref, kb_ref, v_ref, do_ref, o_ref, lse_ref, out_ref, dq_ref):
    p = pl.program_id(1)
    lanes = lane_ids((LEN, 2 * HD))
    low = lanes < HD
    q = q_ref[...] * BF16(HD**-0.5)
    k = pair_of(ka_ref[...], kb_ref[...])
    real = lanes + 2 * HD * p < width
    v = jnp.where(real, v_ref[...], BF16(0))
    dot_t = do_ref[...]
    do = jnp.where(real, dot_t.T, BF16(0))
    o = jnp.where(real, o_ref[...], BF16(0))
    prod = do.astype(F32) * o.astype(F32)
    lse = lse_ref[...]
    q_t = q.T
    for h in range(2):
        mine = low if h == 0 else jnp.logical_not(low)
        qh = jnp.where(mine, q, BF16(0))
        doh = jnp.where(mine, do, BF16(0))
        delta = jnp.sum(jnp.where(mine, prod, 0.0), axis=1, keepdims=True)
        norm = jnp.sum(jnp.where(lanes == 2 * p + h, lse, 0.0), axis=1, keepdims=True)
        rows = slice(h * HD, (h + 1) * HD)
        dk = None
        for at in range(LEN - QB, -1, -QB):
            end = at + QB
            s = lax.dot_general(qh[at:end], k[:end], NT, preferred_element_type=F32)
            w = causal_fill(jnp.exp(s - norm[at:end]), 0.0)
            wb = w.astype(BF16)
            dp = lax.dot_general(doh[at:end], v[:end], NT, preferred_element_type=F32)
            ds = (w * (dp - delta[at:end])).astype(BF16)
            dq = jnp.dot(ds, k[:end], preferred_element_type=F32) * HD**-0.5
            if h == 0:
                dq_ref[at:end, :] = dq.astype(BF16)
            else:
                dq_ref[at:end, :] = jnp.where(low[at:end], dq_ref[at:end, :], dq.astype(BF16))
            dk_part = jnp.dot(q_t[rows, at:end], ds, preferred_element_type=F32)
            dv_part = jnp.dot(dot_t[rows, at:end], wb, preferred_element_type=F32)
            if dk is None:
                dk, dv = dk_part, dv_part
            else:
                dk = jnp.concatenate([dk[:, :end] + dk_part, dk[:, end:]], axis=1)
                dv = jnp.concatenate([dv[:, :end] + dv_part, dv[:, end:]], axis=1)
        out_ref[1, rows, :] = dk.astype(BF16)
        out_ref[2, rows, :] = dv.astype(BF16)
    out_ref[0, :, :] = dq_ref[...].T


def attend_back(packed, grad_t, attended, lse):
    rows = packed.shape[0]
    width = packed.shape[1] // 3
    seqs = rows // LEN
    pairs = pl.cdiv(width, 2 * HD)
    kb, vb = width // (2 * HD), 2 * width // (2 * HD)

    def blk(f):
        return pl.BlockSpec((LEN, 2 * HD), f)

    out = pl.pallas_call(
        functools.partial(attend_back_kernel, width),
        grid=(seqs, pairs),
        in_specs=[
            blk(lambda s, p: (s, p)),
            blk(lambda s, p: (s, p + kb)),
            blk(lambda s, p: (s, p + kb + 1)),
            blk(lambda s, p: (s, p + vb)),
            pl.BlockSpec((2 * HD, LEN), lambda s, p: (p, s)),
            blk(lambda s, p: (s, p)),
            blk(lambda s, p: (s, 0)),
        ],
        out_specs=pl.BlockSpec((3, 2 * HD, LEN), lambda s, p: (0, p, s)),
        out_shape=shape_of((3, width, rows), BF16),
        scratch_shapes=[pltpu.VMEM((LEN, 2 * HD), BF16)],
        cost_estimate=cost(rows * LEN * width * 12, 14 * rows * width),
        name="aback",
    )(packed, packed, packed, packed, grad_t, attended, lse)
    return out.reshape(3 * width, rows)


def project_kernel(
    side_ref, att_ref, x_ref, wo_ref, wa_ref, rows_ref,
    ao_ref, aa_ref, mid_ref, so_ref, sa_ref, n_ref, inv_ref,
):
    side = side_ref[0]
    store_pair(side, att_ref[...], ao_ref, aa_ref)
    mid = joined_dot(ao_ref[...], aa_ref[...], wo_ref[...], wa_ref[...])
    mid += x_ref[...].T.astype(F32) + rows_ref[4:5, :]
    mid_ref[...] = mid.T
    centred = mid - jnp.mean(mid, axis=1, keepdims=True)
    inverse = lax.rsqrt(jnp.mean(centred * centred, axis=1, keepdims=True) + EPS)
    normed = centred * inverse
    act = (normed * rows_ref[5:6, :] + rows_ref[6:7, :]).astype(BF16)
    store_pair(side, act, so_ref, sa_ref)
    n_ref[...] = normed.astype(BF16).T
    inv_ref[...] = jnp.broadcast_to(inverse, (inverse.shape[0], 128)).T[:8]


def project(side, attended, tok_t, w_own, w_away, small_rows):
    width, rows = tok_t.shape
    half = width // 2
    wide = round_up(half, 128)
    block = min(256, rows)
    nat = pl.BlockSpec((block, width), lambda i, *_: (i, 0))
    pair = pl.BlockSpec((block, wide), lambda i, *_: (i, 0))
    whole = pl.BlockSpec((half, width), lambda i, *_: (0, 0))
    turned = pl.BlockSpec((width, block), lambda i, *_: (0, i))
    return pl.pallas_call(
        project_kernel,
        grid_spec=pltpu.PrefetchScalarGridSpec(
            num_scalar_prefetch=1,
            grid=(rows // block,),
            in_specs=[nat, turned, whole, whole, pl.BlockSpec((8, width), lambda i, *_: (0, 0))],
            out_specs=[
                pair, pair, turned, pair, pair, turned,
                pl.BlockSpec((8, block), lambda i, *_: (0, i)),
            ],
        ),
        out_shape=[
            shape_of((rows, wide), BF16),
            shape_of((rows, wide), BF16),
            shape_of((width, rows), F32),
            shape_of((rows, wide), BF16),
            shape_of((rows, wide), BF16),
            shape_of((width, rows), BF16),
            shape_of((8, rows), F32),
        ],
        compiler_params=params(),
        cost_estimate=cost(4 * rows * half * width, 4 * half * width + 14 * rows * width),
        name="project",
    )(side, attended, tok_t, w_own, w_away, small_rows)


def hidden_kernel(start_ref, so_ref, sa_ref, wo_ref, wa_ref, bias_ref, act_ref, slope_ref):
    rows = so_ref.shape[0] // 2
    wo, wa = wo_ref[...], wa_ref[...]
    for at in range(0, so_ref.shape[0], rows):
        part = slice(at, at + rows)
        v = joined_dot(so_ref[part, :], sa_ref[part, :], wo, wa)
        v += bias_ref[8:9, :]
        square = v * v
        t = jnp.tanh(TANH_COEF * v * (1.0 + CUBIC * square))
        grown = 0.5 * (1.0 + t)
        act_ref[part, :] = (v * grown).astype(BF16)
        slope = grown * (1.0 + v * (1.0 - t) * (TANH_COEF + 3.0 * TANH_COEF * CUBIC * square))
        slope_ref[part, :] = slope.astype(BF16)


def hidden(start, own, away, w_own, w_away, bias, units):
    rows, wide = own.shape
    half = w_own.shape[0]
    tile = 640
    resident = pl.BlockSpec((rows, wide), lambda i, s: (0, 0))
    right = pl.BlockSpec((half, tile), lambda i, s: (0, s[0] + i))
    out = pl.BlockSpec((rows, tile), lambda i, s: (0, i))
    return pl.pallas_call(
        hidden_kernel,
        grid_spec=pltpu.PrefetchScalarGridSpec(
            num_scalar_prefetch=1,
            grid=(units // tile,),
            in_specs=[resident, resident, right, right, pl.BlockSpec((16, tile), lambda i, s: (0, i))],
            out_specs=[out, out],
        ),
        out_shape=[shape_of((rows, units), BF16)] * 2,
        compiler_params=params(),
        cost_estimate=cost(4 * rows * units * half, 4 * units * half + 4 * rows * units),
        name="hidden",
    )(start, own, away, w_own, w_away, bias)


def hidden_back_kernel(meta_ref, cot_ref, w1_ref, w2_ref, s1_ref, s2_ref, ge_ref, sum_ref):
    def part(w_ref, slope_ref):
        ge = jnp.dot(cot_ref[...], w_ref[...], preferred_element_type=F32) * slope_ref[...].astype(F32)
        ge_ref[...] = ge.astype(BF16).T
        sum_ref[...] = jnp.broadcast_to(jnp.sum(ge, axis=0, keepdims=True), sum_ref.shape)

    first = pl.program_id(0) < pl.num_programs(0) // 2
    pl.when(first)(lambda: part(w1_ref, s1_ref))
    pl.when(jnp.logical_not(first))(lambda: part(w2_ref, s2_ref))


def hidden_back(meta, cot, w_first_t, w_second_t, slope_first, slope_second):
    width, units = w_first_t.shape
    rows = cot.shape[0]
    tile = 640
    steps = units // tile
    first = lambda i: jnp.minimum(i, steps - 1)
    second = lambda i: jnp.maximum(i - steps, 0)
    place = lambda i, m: jnp.where(i < steps, (1 - m[0]) * steps + i, m[0] * steps + i - steps)
    return pl.pallas_call(
        hidden_back_kernel,
        grid_spec=pltpu.PrefetchScalarGridSpec(
            num_scalar_prefetch=1,
            grid=(2 * steps,),
            in_specs=[
                pl.BlockSpec((rows, width), lambda i, m: (0, 0)),
                pl.BlockSpec((width, tile), lambda i, m: (0, first(i))),
                pl.BlockSpec((width, tile), lambda i, m: (0, second(i))),
                pl.BlockSpec((rows, tile), lambda i, m: (0, first(i))),
                pl.BlockSpec((rows, tile), lambda i, m: (0, second(i))),
            ],
            out_specs=[
                pl.BlockSpec((tile, rows), lambda i, m: (place(i, m), 0)),
                pl.BlockSpec((8, tile), lambda i, m: (0, place(i, m))),
            ],
        ),
        out_shape=[shape_of((2 * units, rows), BF16), shape_of((8, 2 * units), F32)],
        compiler_params=params(),
        cost_estimate=cost(4 * rows * units * width, 4 * units * width + 8 * rows * units),
        name="hback",
    )(meta, cot, w_first_t, w_second_t, slope_first, slope_second)


ROWS = 160


def middle_kernel(
    meta_ref, g_ref, wo_hbm, wa_hbm, n_hbm, inv_ref, gain_ref, cot_hbm, po_hbm, pa_hbm,
    gm_ref, gmb_ref, ga_ref, s_gain_ref, s_shift_ref, s_bias_ref,
    acc_ref, prod_ref, wo_buf, wa_buf, n_ref, cot_ref, po_ref, pa_ref, sem, sem_late,
):
    side = meta_ref[0]
    width = acc_ref.shape[0]
    half = width // 2
    i = pl.program_id(0)
    steps, tile, _ = wo_buf.shape
    rows = lambda ref: lambda i: ref.at[pl.ds(i * tile, tile), :]
    stream(i, steps, (rows(wo_hbm), rows(wa_hbm)), (wo_buf, wa_buf), sem)
    late = [
        pltpu.make_async_copy(src, dst, sem_late.at[j])
        for j, (src, dst) in enumerate(
            ((n_hbm, n_ref), (cot_hbm, cot_ref), (po_hbm, po_ref), (pa_hbm, pa_ref))
        )
    ]

    @pl.when(i == 0)
    def _():
        for c in late:
            c.start()

    left = jnp.concatenate([wo_buf[i], wa_buf[i]], axis=0)
    total = jnp.dot(left, g_ref[...], preferred_element_type=F32)
    acc_ref[pl.ds(pl.multiple_of(side * half + i * tile, 8), tile), :] = total[:tile]
    acc_ref[pl.ds(pl.multiple_of((1 - side) * half + i * tile, 8), tile), :] = total[tile:]

    @pl.when(i == steps - 1)
    def _():
        for c in late:
            c.wait()
        tokens = acc_ref.shape[1]
        inverse = inv_ref[0:1, :]

        def first(j, sums):
            at = pl.ds(j * ROWS, ROWS)
            e, n = acc_ref[at, :], n_ref[at, :].astype(F32)
            w = e * gain_ref[at, 5:6]
            gmb_ref[at, :] = e.astype(BF16)
            prod_ref[at, :] = (e * n).astype(BF16)
            return (
                sums[0] + jnp.sum(w, axis=0, keepdims=True),
                sums[1] + jnp.sum(w * n, axis=0, keepdims=True),
            )

        zero = jnp.zeros((1, tokens), F32)
        one, two = lax.fori_loop(0, width // ROWS, first, (zero, zero))
        one, two = one / width, two / width
        s_gain_ref[...] = row_sums(prod_ref[...])
        s_shift_ref[...] = row_sums(gmb_ref[...])

        def second(j, _):
            at = pl.ds(j * ROWS, ROWS)
            n = n_ref[at, :].astype(F32)
            back = inverse * (acc_ref[at, :] * gain_ref[at, 5:6] - one - n * two)
            g = cot_ref[at, :].astype(F32) + back
            gm_ref[at, :] = g
            gmb_ref[at, :] = g.astype(BF16)
            return 0

        lax.fori_loop(0, width // ROWS, second, 0)
        g = gmb_ref[...]
        s_bias_ref[...] = row_sums(g)
        for which, p_ref in ((side, po_ref), (1 - side, pa_ref)):
            ga_ref[pl.ds(pl.multiple_of(which * half, 16), half), :] = jnp.dot(
                p_ref[...], g, preferred_element_type=F32
            ).astype(BF16)


def middle_back(meta, ge, w_own, w_away, normed_t, inv_t, cols, cot_t, p_own, p_away):
    units, rows = ge.shape
    half = w_own.shape[0]
    width = 2 * half
    tile = 200
    steps = half // tile
    once = pl.Buffered(1)
    const = lambda shape: pl.BlockSpec(shape, lambda i, m: (0, 0), pipeline_mode=once)
    out = lambda shape: pl.BlockSpec(shape, lambda i, m: (0, 0))
    small = shape_of((8, width), F32)
    return pl.pallas_call(
        middle_kernel,
        grid_spec=pltpu.PrefetchScalarGridSpec(
            num_scalar_prefetch=1,
            grid=(steps,),
            in_specs=[
                const((units, rows)), ANYWHERE, ANYWHERE, ANYWHERE,
                const((8, rows)), const((width, 128)), ANYWHERE, ANYWHERE, ANYWHERE,
            ],
            out_specs=[out((width, rows))] * 3 + [out((8, width))] * 3,
            scratch_shapes=[
                pltpu.VMEM((width, rows), F32),
                pltpu.VMEM((width, rows), BF16),
                pltpu.VMEM((steps, tile, units), BF16),
                pltpu.VMEM((steps, tile, units), BF16),
                pltpu.VMEM((width, rows), BF16),
                pltpu.VMEM((width, rows), BF16),
                pltpu.VMEM((half, width), BF16),
                pltpu.VMEM((half, width), BF16),
                pltpu.SemaphoreType.DMA((2, steps)),
                pltpu.SemaphoreType.DMA((4,)),
            ],
        ),
        out_shape=[
            shape_of((width, rows), F32),
            shape_of((width, rows), BF16),
            shape_of((width, rows), BF16),
            small, small, small,
        ],
        compiler_params=params(),
        cost_estimate=cost(
            2 * rows * units * width + 2 * rows * width * width, 2 * units * width + 12 * rows * width
        ),
        name="middle",
    )(meta, ge, w_own, w_away, normed_t, inv_t, cols, cot_t, p_own, p_away)


def first_kernel(
    meta_ref, gp_ref, wo_hbm, wa_hbm, tok_hbm, gain_ref, gm_hbm,
    out_ref, s_gain_ref, s_shift_ref, s_pack_ref,
    acc_ref, prod_ref, e_ref, wo_buf, wa_buf, tok_ref, gm_ref, sem, sem_late,
):
    side = meta_ref[0]
    width = acc_ref.shape[0]
    half = width // 2
    i = pl.program_id(0)
    steps, tile, _ = wo_buf.shape
    rows = lambda ref: lambda i: ref.at[pl.ds(i * tile, tile), :]
    stream(i, steps, (rows(wo_hbm), rows(wa_hbm)), (wo_buf, wa_buf), sem)
    late = [
        pltpu.make_async_copy(src, dst, sem_late.at[j])
        for j, (src, dst) in enumerate(((tok_hbm, tok_ref), (gm_hbm, gm_ref)))
    ]

    @pl.when(i == 0)
    def _():
        for c in late:
            c.start()

    g = gp_ref[...]
    total = jnp.dot(
        jnp.concatenate([wo_buf[i], wa_buf[i]], axis=0), g, preferred_element_type=F32
    )
    acc_ref[pl.ds(pl.multiple_of(side * half + i * tile, 8), tile), :] = total[:tile]
    acc_ref[pl.ds(pl.multiple_of((1 - side) * half + i * tile, 8), tile), :] = total[tile:]

    @pl.when(i == 0)
    def _():
        s_pack_ref[...] = row_sums(g)

    @pl.when(i == pl.num_programs(0) - 1)
    def _():
        for c in late:
            c.wait()
        tokens = acc_ref.shape[1]
        zero = jnp.zeros((1, tokens), F32)
        loops = width // ROWS

        def total(j, s):
            return s + jnp.sum(tok_ref[pl.ds(j * ROWS, ROWS), :].astype(F32), axis=0, keepdims=True)

        mean = lax.fori_loop(0, loops, total, zero) / width

        def spread_of(j, s):
            c = tok_ref[pl.ds(j * ROWS, ROWS), :].astype(F32) - mean
            return s + jnp.sum(c * c, axis=0, keepdims=True)

        inverse = lax.rsqrt(lax.fori_loop(0, loops, spread_of, zero) / width + EPS)

        def first(j, sums):
            at = pl.ds(j * ROWS, ROWS)
            e = acc_ref[at, :]
            n = (tok_ref[at, :].astype(F32) - mean) * inverse
            w = e * gain_ref[at, 0:1]
            e_ref[at, :] = e.astype(BF16)
            prod_ref[at, :] = (e * n).astype(BF16)
            return (
                sums[0] + jnp.sum(w, axis=0, keepdims=True),
                sums[1] + jnp.sum(w * n, axis=0, keepdims=True),
            )

        one, two = lax.fori_loop(0, loops, first, (zero, zero))
        one, two = one / width, two / width
        s_gain_ref[...] = row_sums(prod_ref[...])
        s_shift_ref[...] = row_sums(e_ref[...])

        def second(j, _):
            at = pl.ds(j * ROWS, ROWS)
            n = (tok_ref[at, :].astype(F32) - mean) * inverse
            back = inverse * (acc_ref[at, :] * gain_ref[at, 0:1] - one - n * two)
            out_ref[at, :] = (gm_ref[at, :] + back).astype(BF16)
            return 0

        lax.fori_loop(0, loops, second, 0)


def first_back(meta, gp_t, w_own, w_away, tok_t, cols, gm_t):
    columns, rows = gp_t.shape
    half = w_own.shape[0]
    width = 2 * half
    tile = 200
    steps = half // tile
    const = lambda shape: pl.BlockSpec(shape, lambda i, m: (0, 0))
    return pl.pallas_call(
        first_kernel,
        grid_spec=pltpu.PrefetchScalarGridSpec(
            num_scalar_prefetch=1,
            grid=(steps,),
            in_specs=[
                const((columns, rows)), ANYWHERE, ANYWHERE, ANYWHERE, const((width, 128)), ANYWHERE,
            ],
            out_specs=[const((width, rows)), const((8, width)), const((8, width)), const((8, columns))],
            scratch_shapes=[
                pltpu.VMEM((width, rows), F32),
                pltpu.VMEM((width, rows), BF16),
                pltpu.VMEM((width, rows), BF16),
                pltpu.VMEM((steps, tile, columns), BF16),
                pltpu.VMEM((steps, tile, columns), BF16),
                pltpu.VMEM((width, rows), BF16),
                pltpu.VMEM((width, rows), F32),
                pltpu.SemaphoreType.DMA((2, steps)),
                pltpu.SemaphoreType.DMA((2,)),
            ],
        ),
        out_shape=[
            shape_of((width, rows), BF16),
            shape_of((8, width), F32),
            shape_of((8, width), F32),
            shape_of((8, columns), F32),
        ],
        compiler_params=params(),
        cost_estimate=cost(4 * rows * half * columns, 4 * half * columns + 2 * rows * columns + 10 * rows * width),
        name="first",
    )(meta, gp_t, w_own, w_away, tok_t, cols, gm_t)


def output_kernel(a1_ref, a2_ref, w1_hbm, w2_hbm, mid_ref, cols_ref, out_ref, w1_buf, w2_buf, sem):
    i = pl.program_id(0)
    steps, tile, _ = w1_buf.shape
    rows = lambda ref: lambda i: ref.at[pl.ds(i * tile, tile), :]
    stream(i, steps, (rows(w1_hbm), rows(w2_hbm)), (w1_buf, w2_buf), sem)
    weights = jnp.concatenate([w1_buf[i], w2_buf[i]], axis=1)
    acts = jnp.concatenate([a1_ref[...], a2_ref[...]], axis=1)
    total = lax.dot_general(weights, acts, NT, preferred_element_type=F32)
    out_ref[...] = (total + mid_ref[...] + cols_ref[:, 7:8]).astype(BF16)


def block_output(act_first, act_second, w_away_t, w_own_t, middle_t, cols):
    rows, units = act_first.shape
    width = w_own_t.shape[0]
    tile = 400
    left = pl.BlockSpec((rows, units), lambda i: (0, 0))
    steps = width // tile
    part = pl.BlockSpec((tile, rows), lambda i: (i, 0))
    return pl.pallas_call(
        output_kernel,
        grid=(width // tile,),
        in_specs=[left, left, ANYWHERE, ANYWHERE, part, pl.BlockSpec((tile, 128), lambda i: (i, 0))],
        out_specs=part,
        scratch_shapes=[pltpu.VMEM((steps, tile, units), BF16)] * 2 + [pltpu.SemaphoreType.DMA((2, steps))],
        out_shape=shape_of((width, rows), BF16),
        compiler_params=params(),
        cost_estimate=cost(4 * rows * units * width, 4 * units * width + 4 * rows * units + 6 * rows * width),
        name="output",
    )(act_first, act_second, w_away_t, w_own_t, middle_t, cols)


class Group:
    def __init__(self, count, lanes, chunks, plan):
        self.count, self.lanes, self.chunks = count, lanes, chunks
        shares, orders = plan
        bits = count.bit_length() - 1
        self.orders = [list(order) + list(range(len(order), bits)) for order in orders]
        tiles = lanes // 128
        one, two = (round(tiles * share) for share in shares)
        self.cuts = [0, one * 128, (one + two) * 128, tiles * 128]
        self.widths = [self.cuts[k + 1] - self.cuts[k] for k in range(3)]
        self.left_over = lanes % 128
        self.pieces = self.widths[2] // self.left_over if self.left_over else 0

    def padded(self, which):
        return round_up(self.chunks[which], 16)

    def each(self, which):
        return pl.cdiv(self.chunks[which], self.pieces)

    def packed(self, which):
        return round_up(self.each(which), 16) if self.left_over else 0

    def rows(self, k, which):
        return self.padded(which) + (self.packed(which) if k == 2 else 0)

    def base(self, k, which):
        return sum(self.rows(k, w) for w in range(which))

    def total_rows(self, k):
        return self.base(k, len(self.chunks))


SLOTS = 4


def spread_kernel(spec, meta_ref, lo_ref, la_ref, ro_ref, ra_ref, *refs):
    group, which, batch, n_into = spec
    refs = refs[n_into:]
    keeps, sends, stages, sem = refs[:3], refs[3:6], refs[6:9], refs[9]
    count, chunk = group.count, group.chunks[which]
    step, steps = pl.program_id(0), pl.num_programs(0)
    rank, first = meta_ref[0], meta_ref[1]
    padded = group.padded(which)
    half = count // 2

    def rows_of(k):
        return pl.ds(group.base(k, which), group.rows(k, which))

    def wait_slot(slot):
        for k in range(3):
            pltpu.make_async_copy(
                stages[k].at[slot], keeps[k].at[0, rows_of(k), :], sem.at[k, slot]
            ).wait()

    lanes = group.lanes
    total = joined_dot(lo_ref[...], la_ref[...], ro_ref[:, :lanes], ra_ref[:, :lanes])
    for s in range(batch):
        index = step * batch + s
        slot = s % SLOTS if batch % SLOTS == 0 else lax.rem(index, SLOTS)
        if s >= SLOTS:
            wait_slot(slot)
        else:
            pl.when(index >= SLOTS)(lambda slot=slot: wait_slot(slot))
        mixed = jnp.bitwise_xor(first + index, rank)
        part = total[s * chunk : (s + 1) * chunk]
        for k in range(3):
            low, width = group.cuts[k], group.widths[k]
            stages[k][slot, :chunk, :] = part[:, low : low + width].astype(BF16)
            if k == 2 and group.left_over:
                each, pieces = group.each(which), group.pieces
                extra = part[:, low + width :]
                if pieces * each > chunk:
                    extra = jnp.concatenate(
                        [extra, jnp.zeros((pieces * each - chunk, group.left_over), F32)], axis=0
                    )
                extra = jnp.concatenate([extra[j * each : (j + 1) * each] for j in range(pieces)], axis=1)
                stages[k][slot, padded : padded + each, :] = extra.astype(BF16)
            place = jnp.int32(0)
            order = group.orders[k]
            for depth, bit in enumerate(order):
                place += ((mixed >> bit) & 1) << (len(order) - 1 - depth)

            @pl.when(place < half)
            def _(k=k, slot=slot, place=place):
                pltpu.make_async_copy(
                    stages[k].at[slot], keeps[k].at[place, rows_of(k), :], sem.at[k, slot]
                ).start()

            @pl.when(place >= half)
            def _(k=k, slot=slot, place=place):
                pltpu.make_async_copy(
                    stages[k].at[slot], sends[k].at[place - half, rows_of(k), :], sem.at[k, slot]
                ).start()

    @pl.when(step == steps - 1)
    def _():
        for slot in range(SLOTS):
            wait_slot(slot)


def spread(group, which, meta, lefts, rights, into=None):
    left_own, left_away = lefts
    columns, tokens = left_own.shape
    count, chunk = group.count, group.chunks[which]
    batch = 1
    while batch * chunk % 16:
        batch *= 2
    outs = [shape_of((count // 2, group.total_rows(k), group.widths[k]), BF16) for k in range(3)] * 2
    extra = list(into) if into is not None else []
    spec = (group, which, batch, len(extra))
    anywhere = pl.BlockSpec(memory_space=pl.ANY)
    left = pl.BlockSpec((batch * chunk, tokens), lambda i, *_: (i, 0))
    whole = pl.BlockSpec(rights[0].shape, lambda i, *_: (0, 0))
    return pl.pallas_call(
        functools.partial(spread_kernel, spec),
        grid_spec=pltpu.PrefetchScalarGridSpec(
            num_scalar_prefetch=1,
            grid=(columns // (batch * chunk),),
            in_specs=[left, left, whole, whole] + [anywhere] * len(extra),
            out_specs=[anywhere] * len(outs),
            scratch_shapes=[
                pltpu.VMEM((SLOTS, group.rows(k, which), group.widths[k]), BF16) for k in range(3)
            ]
            + [pltpu.SemaphoreType.DMA((3, SLOTS))],
        ),
        out_shape=outs,
        input_output_aliases={5 + i: i for i in range(len(extra))},
        compiler_params=params(),
        cost_estimate=cost(
            4 * columns * tokens * group.lanes, 4 * columns * tokens + 2 * columns * group.lanes
        ),
        name="spread",
    )(meta, left_own, left_away, *rights, *extra)


def merge_kernel(*refs):
    for k in range(3):
        keep_low, came_low, keep_high, came_high = refs[4 * k : 4 * k + 4]
        keep, send = refs[12 + k], refs[15 + k]
        keep[...] = (keep_low[...].astype(F32) + came_low[...].astype(F32)).astype(BF16)
        send[...] = (keep_high[...].astype(F32) + came_high[...].astype(F32)).astype(BF16)


def merge(keeps, arrived):
    half = keeps[0].shape[0] // 2
    ins, specs, outs, out_specs = [], [], [], []
    moved = 0
    for keep, came in zip(keeps, arrived):
        shape = (1,) + keep.shape[1:]
        low = pl.BlockSpec(shape, lambda i: (i, 0, 0))
        high = pl.BlockSpec(shape, lambda i: (i + half, 0, 0))
        ins += [keep, came, keep, came]
        specs += [low, low, high, high]
        outs.append(shape_of((half,) + keep.shape[1:], BF16))
        out_specs.append(low)
        moved += 6 * keep.size
    return pl.pallas_call(
        merge_kernel,
        grid=(half,),
        in_specs=specs,
        out_specs=out_specs * 2,
        out_shape=outs * 2,
        compiler_params=params(),
        cost_estimate=cost(0, moved),
        name="merge",
    )(*ins)


def finish_kernel(group, *refs):
    outs = refs[6:]
    totals = [refs[2 * k][0].astype(F32) + refs[2 * k + 1][0].astype(F32) for k in range(3)]
    for which, chunk in enumerate(group.chunks):
        out = outs[which]
        for k in range(3):
            base = group.base(k, which)
            out[:, group.cuts[k] : group.cuts[k + 1]] = totals[k][base : base + chunk]
        width = group.left_over
        if width:
            base = group.base(2, which) + group.padded(which)
            rest = totals[2][base : base + group.each(which)]
            rest = jnp.concatenate([rest[:, j * width : (j + 1) * width] for j in range(group.pieces)], axis=0)
            out[:, group.cuts[3] :] = rest[:chunk]


def finish(group, keeps, arrived):
    ins = []
    for keep, came in zip(keeps, arrived):
        ins += [keep, came]
    res = pl.pallas_call(
        functools.partial(finish_kernel, group),
        out_shape=[shape_of((chunk, group.lanes), F32) for chunk in group.chunks],
        compiler_params=params(),
        cost_estimate=cost(0, 8 * sum(group.chunks) * group.lanes),
        name="finish",
    )(*ins)
    return [x.T for x in res]


ORDER = (
    "sc", "hb", "mid", "mc", "e", "p", "ab", "mc", "sh", "me", "mc", "first", "s", "mh", "s", "me",
    "mh", "s", "me", "out", "s", "mc", "s", "mh", "s", "me", "mh",
)

PLANS = (
    ((0.36, 0.36), ((0, 2, 1, 3), (1, 0, 2, 3), (2, 1, 0, 3))),
    ((0.33, 0.33), ((0, 1, 2, 3), (1, 2, 0, 3), (2, 0, 1, 3))),
    ((0.5, 0.33), ((0, 1, 2, 3), (1, 0, 2, 3), (2, 1, 0, 3))),
)


def all_steps(bits):
    steps = list(ORDER)
    for name in ("mc", "me", "mh"):
        steps += [name] * (bits - steps.count(name))
    return steps + ["s"] * (bits + 2 - steps.count("s"))


def solution(mesh):
    count = mesh.shape["rep"]
    assert mesh.shape["grp"] == 2
    bits = count.bit_length() - 1
    assert 1 << bits == count and bits >= 4

    def per_device(
        tokens,
        first_gain,
        first_shift,
        w_heads,
        query_bias,
        value_bias,
        w_project,
        project_bias,
        second_gain,
        second_shift,
        w_expand,
        expand_bias,
        w_contract,
        contract_bias,
        cotangent,
    ):
        width = tokens.shape[1]
        units = w_contract.shape[0]
        side = lax.axis_index("grp")
        rank = lax.axis_index("rep")
        sides = jnp.reshape(side, (1,))

        smalls = (
            first_gain,
            first_shift,
            query_bias,
            value_bias,
            project_bias,
            second_gain,
            second_shift,
            contract_bias,
            expand_bias,
        )
        tok_t, cot_t, contract_own = tokens.T, cotangent.T, w_contract.T
        own_small = gather_smalls(smalls)
        away_small = swap_group(own_small)
        heads_in, _ = lax.optimization_barrier((w_heads, away_small))
        heads_away = swap_group(heads_in)
        small_rows, cols, packed_row = unpack_smalls(sides, own_small, away_small, width)
        first_own, first_out, cot, cot_sum = prep(sides, tok_t, cot_t, cols)
        w_project_in, _ = lax.optimization_barrier((w_project, first_own))
        project_away = swap_group(w_project_in)
        packed = heads_project(first_own, first_out, w_heads, heads_away, packed_row)

        latest = [packed]


        def hold(x):
            return lax.optimization_barrier((x, latest[0]))[0]

        def held(out):
            latest[0] = jax.tree.leaves(out)[0]
            return out

        w_expand_in, _ = lax.optimization_barrier((hold(w_expand), project_away))
        expand_away = swap_group(w_expand_in)
        contract_away = swap_group(hold(contract_own))
        cot_away_t = swap_group(hold(cot_t))
        first_away = swap_group(hold(first_out))

        tiles = units // 640
        start_first = jnp.reshape((1 - side) * tiles, (1,)).astype(jnp.int32)
        start_second = jnp.reshape(side * tiles, (1,)).astype(jnp.int32)

        def do_hidden(start, bias):
            return held(hidden(hold(start), second_own, second_out, w_expand, expand_away, bias, units))

        attended, lse = held(attend(packed))
        att_own, att_out, middle_t, second_own, second_out, normed_t, inv_t = held(project(
            sides, attended, tok_t, w_project, project_away, small_rows
        ))
        act_first, slope_first = do_hidden(start_first, away_small)
        act_away = swap_group(act_first)
        act_second, slope_second = do_hidden(start_second, own_small)

        chunk_d = width // count
        chunk_f = 2 * units // count
        chunk_h = w_heads.shape[1] // count
        groups = {
            "c": Group(count, units, [chunk_d], PLANS[0]),
            "e": Group(count, width // 2, [chunk_f, chunk_d], PLANS[1]),
            "h": Group(count, width // 2, [chunk_h], PLANS[2]),
        }
        meta_all = jnp.stack([rank, jnp.int32(0)]).astype(jnp.int32)
        state, results = {}, {}
        r = types.SimpleNamespace()

        def send(name, buffers):
            group = groups[name]
            state[name] = [list(buffers[:3]), 0, [
                exchange(buffers[3 + k], 1 << group.orders[k][0], count) for k in range(3)
            ]]

        def advance(name):
            group = groups[name]
            keeps, depth, arrived = state[name]
            keeps = [hold(keeps[0])] + keeps[1:]
            if depth == bits - 1:
                results[name] = held(finish(group, keeps, arrived))
                return
            buffers = held(merge(keeps, arrived))
            state[name] = [list(buffers[:3]), depth + 1, [
                exchange(buffers[3 + k], 1 << group.orders[k][depth + 1], count) for k in range(3)
            ]]

        def do_contract():
            send("c", held(spread(
                groups["c"], 0, hold(meta_all), (cot_t, cot_away_t), (act_second, act_away)
            )))

        def do_hidden_back():
            r.ge, r.eb = held(hidden_back(
                hold(sides), cot, contract_away, contract_own, slope_first, slope_second
            ))
            r.ge_away = swap_group(r.ge)
            r.second_away = swap_group(second_out)
            r.att_away = swap_group(att_out)

        def do_middle():
            r.gm_t, r.gmb_t, r.ga_t, r.s_gain2, r.s_shift2, r.s_pb = held(middle_back(
                hold(sides), r.ge, w_expand, expand_away, normed_t, inv_t,
                cols, cot_t, w_project, project_away,
            ))
            r.gmb_away = swap_group(r.gmb_t)

        def do_expand():
            r.buffers = held(spread(
                groups["e"], 0, hold(meta_all), (r.ge, r.ge_away), (second_own, r.second_away)
            ))

        def do_project():
            send("e", held(spread(
                groups["e"], 1, hold(meta_all), (r.gmb_t, r.gmb_away),
                (att_own, r.att_away), r.buffers,
            )))

        def do_attend_back():
            r.gp_t = held(attend_back(hold(packed), r.ga_t, attended, lse))
            r.gp_away = swap_group(r.gp_t)

        def do_heads():
            send("h", held(spread(
                groups["h"], 0, hold(meta_all), (r.gp_t, r.gp_away), (first_own, first_away)
            )))

        def do_first():
            r.grad_tokens_t, r.s_gain1, r.s_shift1, r.s_pack = held(first_back(
                hold(sides), r.gp_t, w_heads, heads_away, tok_t, cols, r.gm_t
            ))

        def do_output():
            r.block_out_t = held(
                block_output(hold(act_first), act_second, contract_away, contract_own, middle_t, cols)
            )

        small = []

        def do_small():
            if not small:
                mine, theirs = held(collect(
                    hold(sides), r.s_pack, r.eb,
                    [r.s_gain1, r.s_shift1, r.s_pb, r.s_gain2, r.s_shift2, cot_sum],
                ))
                small.extend([mine, swap_group(theirs), 0])
                return
            vector, arrived, bit = small
            if bit == bits:
                small[0] = held(divide(hold(vector), arrived, [width // 2] * 8 + [units]))
                return
            vector = held(add(hold(vector), arrived))
            small[:] = [vector, exchange(vector, 1 << (bits - 1 - bit), count), bit + 1]

        steps = {
            "sc": do_contract, "hb": do_hidden_back, "mid": do_middle,
            "e": do_expand, "p": do_project, "ab": do_attend_back,
            "sh": do_heads, "first": do_first, "out": do_output, "s": do_small,
            "mc": lambda: advance("c"), "me": lambda: advance("e"),
            "mh": lambda: advance("h"),
        }
        for name in all_steps(bits):
            steps[name]()
        finals = small[0]
        (out_w_contract,) = results["c"]
        out_w_expand, out_w_project = results["e"]
        (out_w_heads,) = results["h"]
        grad_tokens_t, block_out_t = r.grad_tokens_t, r.block_out_t

        return (
            block_out_t.T,
            grad_tokens_t.T,
            finals[0],
            finals[1],
            out_w_heads,
            finals[2],
            finals[3],
            out_w_project,
            finals[4],
            finals[5],
            finals[6],
            out_w_expand,
            finals[8],
            out_w_contract,
            finals[7],
        )

    placed = (
        P(("rep", "grp"), None),
        P("grp"),
        P("grp"),
        P("grp", None),
        P("grp"),
        P("grp"),
        P("grp", None),
        P("grp"),
        P("grp"),
        P("grp"),
        P("grp", None),
        P("grp"),
        P("grp", None),
        P("grp"),
        P(("rep", "grp"), None),
    )
    return jax.shard_map(
        per_device,
        mesh=mesh,
        in_specs=placed,
        out_specs=(
            P(("rep", "grp"), None),
            P(("rep", "grp"), None),
            P("grp"),
            P("grp"),
            P("grp", "rep"),
            P("grp"),
            P("grp"),
            P("grp", "rep"),
            P("grp"),
            P("grp"),
            P("grp"),
            P("grp", "rep"),
            P("grp"),
            P("grp", "rep"),
            P("grp"),
        ),
        check_vma=False,
    )
```

```python
import functools
import types

import jax
import jax.numpy as jnp
from jax import lax
from jax.experimental import pallas as pl
from jax.experimental.pallas import tpu as pltpu
from jax.sharding import PartitionSpec as P


HD = 64
LEN = 512
QB = 256
EPS = 1e-05
TANH_COEF = 0.7978845608028654
CUBIC = 0.044715
F32 = jnp.float32
BF16 = jnp.bfloat16
NT = (((1,), (1,)), ((), ()))
VMEM_LIMIT = 60 * 1024 * 1024


def shape_of(shape, dtype):
    return jax.ShapeDtypeStruct(shape, dtype)


def params():
    return pltpu.CompilerParams(vmem_limit_bytes=VMEM_LIMIT)


def cost(flops, moved):
    return pl.CostEstimate(flops=int(flops), bytes_accessed=int(moved), transcendentals=0)


def round_up(n, k):
    return -(-n // k) * k


def swap_group(x):
    return lax.ppermute(x, "grp", [(0, 1), (1, 0)])


def exchange(x, mask, count):
    return lax.ppermute(x, "rep", [(i, i ^ mask) for i in range(count)])


def row_sums(x):
    ones = jnp.ones((8, x.shape[1]), BF16)
    return lax.dot_general(ones, x, NT, preferred_element_type=F32)


def joined_dot(left_one, left_two, right_one, right_two):
    missing = left_one.shape[1] - right_one.shape[0]
    rights = [right_one, right_two]
    if missing:
        fill = jnp.zeros((missing, right_one.shape[1]), right_one.dtype)
        rights = [right_one, fill, right_two, fill]
    left = jnp.concatenate([left_one, left_two], axis=1)
    return jnp.dot(left, jnp.concatenate(rights, axis=0), preferred_element_type=F32)


def stream(step, steps, sources, buffers, sem):
    @pl.when(step == 0)
    def _():
        for i in range(steps):
            for j, (source, buffer) in enumerate(zip(sources, buffers)):
                pltpu.make_async_copy(source(i), buffer.at[i], sem.at[j, i]).start()

    for j, (source, buffer) in enumerate(zip(sources, buffers)):
        pltpu.make_async_copy(source(0), buffer.at[step], sem.at[j, step]).wait()


ANYWHERE = pl.BlockSpec(memory_space=pl.ANY)


def store_pair(side, value, own_ref, away_ref):
    half = value.shape[1] // 2
    fill = jnp.zeros((value.shape[0], own_ref.shape[1] - half), value.dtype)
    low = jnp.concatenate([value[:, :half], fill], axis=1)
    high = jnp.concatenate([value[:, half:], fill], axis=1)

    @pl.when(side == 0)
    def _():
        own_ref[...] = low
        away_ref[...] = high

    @pl.when(side == 1)
    def _():
        own_ref[...] = high
        away_ref[...] = low


def gather_kernel(*refs):
    out = refs[-1]
    out[...] = jnp.zeros_like(out)
    for i, ref in enumerate(refs[:-1]):
        out[i : i + 1, : ref.shape[0]] = ref[...].astype(F32).reshape(1, ref.shape[0])


def gather_smalls(smalls):
    widest = max(x.shape[0] for x in smalls)
    return pl.pallas_call(gather_kernel, out_shape=shape_of((16, widest), F32), name="gather")(*smalls)


def unpack_kernel(side_ref, own_ref, away_ref, rows_ref, cols_ref, packed_ref):
    half = rows_ref.shape[1] // 2
    first = side_ref[0] == 0
    own, away = own_ref[0:8, :half], away_ref[0:8, :half]
    low = jnp.where(first, own, away)
    high = jnp.where(first, away, own)
    rows = jnp.concatenate([low, high], axis=1)
    rows_ref[...] = rows
    cols_ref[...] = jnp.concatenate([rows, jnp.zeros((120, 2 * half), F32)], axis=0).T
    packed_ref[...] = jnp.concatenate([rows[2:3], jnp.zeros((1, 2 * half), F32), rows[3:4]], axis=1)


def unpack_smalls(side, own, away, width):
    vmem = pl.BlockSpec(memory_space=pltpu.VMEM)
    return pl.pallas_call(
        unpack_kernel,
        in_specs=[pl.BlockSpec(memory_space=pltpu.SMEM), vmem, vmem],
        out_shape=[shape_of((8, width), F32), shape_of((width, 128), F32), shape_of((1, 3 * width), F32)],
        name="unpack",
    )(side, own, away)


def collect_kernel(side_ref, pack_ref, eb_ref, *refs):
    rows, (mine_ref, theirs_ref) = refs[:-2], refs[-2:]
    width = rows[0].shape[1]
    half = width // 2
    first = side_ref[0] == 0
    pack = pack_ref[0:1, :]
    full = [r[0:1, :] for r in rows[:2]] + [pack[:, :width], pack[:, 2 * width :]]
    full += [r[0:1, :] for r in rows[2:]]
    full = jnp.concatenate(full, axis=0)
    low, high = full[:, :half], full[:, half:]
    mine_ref[...] = jnp.zeros_like(mine_ref)
    theirs_ref[...] = jnp.zeros_like(theirs_ref)
    mine_ref[0:8, :half] = jnp.where(first, low, high)
    theirs_ref[0:8, :half] = jnp.where(first, high, low)
    units = mine_ref.shape[1]
    low, high = eb_ref[0:1, :units], eb_ref[0:1, units:]
    mine_ref[8:9, :] = jnp.where(first, low, high)
    theirs_ref[8:9, :] = jnp.where(first, high, low)


def collect(side, pack, eb, rows):
    vmem = pl.BlockSpec(memory_space=pltpu.VMEM)
    out = shape_of((16, eb.shape[1] // 2), F32)
    return pl.pallas_call(
        collect_kernel,
        in_specs=[pl.BlockSpec(memory_space=pltpu.SMEM)] + [vmem] * (2 + len(rows)),
        out_shape=[out, out],
        name="collect",
    )(side, pack, eb, *rows)


def add_kernel(a_ref, b_ref, out_ref):
    out_ref[...] = a_ref[...] + b_ref[...]


def add(a, b):
    return pl.pallas_call(add_kernel, out_shape=shape_of(a.shape, a.dtype), name="add")(a, b)


def divide_kernel(a_ref, b_ref, *outs):
    total = a_ref[...] + b_ref[...]
    for i, out in enumerate(outs):
        out[...] = total[i : i + 1, : out.shape[0]].reshape(out.shape[0])


def divide(a, b, sizes):
    return pl.pallas_call(
        divide_kernel, out_shape=[shape_of((n,), F32) for n in sizes], name="divide"
    )(a, b)


def prep_kernel(side_ref, x_ref, c_ref, cols_ref, own_ref, away_ref, cot_ref, sum_ref, act_ref):
    x = x_ref[...].astype(F32)
    half = x.shape[0] // 2
    side = side_ref[0]
    centred = x - jnp.mean(x, axis=0, keepdims=True)
    inverse = lax.rsqrt(jnp.mean(centred * centred, axis=0, keepdims=True) + EPS)
    act_ref[...] = (centred * inverse * cols_ref[:, 0:1] + cols_ref[:, 1:2]).astype(BF16)
    for ref, which in ((own_ref, side), (away_ref, 1 - side)):
        ref[:, :half] = act_ref[pl.ds(pl.multiple_of(which * half, 16), half), :].T
        ref[:, half:] = jnp.zeros((ref.shape[0], ref.shape[1] - half), BF16)
    cot = c_ref[...].T
    cot_ref[...] = cot
    part = jnp.sum(cot.astype(F32), axis=0, keepdims=True)
    part = jnp.broadcast_to(part, sum_ref.shape)

    @pl.when(pl.program_id(0) == 0)
    def _():
        sum_ref[...] = part

    @pl.when(pl.program_id(0) > 0)
    def _():
        sum_ref[...] += part


def prep(side, tok_t, cot_t, cols):
    width, rows = tok_t.shape
    block = min(128, rows)
    half = round_up(width // 2, 128)
    nat = pl.BlockSpec((block, width), lambda i, *_: (i, 0))
    turned = pl.BlockSpec((width, block), lambda i, *_: (0, i))
    pair = pl.BlockSpec((block, half), lambda i, *_: (i, 0))
    return pl.pallas_call(
        prep_kernel,
        grid_spec=pltpu.PrefetchScalarGridSpec(
            num_scalar_prefetch=1,
            grid=(rows // block,),
            in_specs=[turned, turned, pl.BlockSpec((width, 128), lambda i, *_: (0, 0))],
            out_specs=[pair, pair, nat, pl.BlockSpec((8, width), lambda i, *_: (0, 0))],
            scratch_shapes=[pltpu.VMEM((width, block), BF16)],
        ),
        out_shape=[
            shape_of((rows, half), BF16),
            shape_of((rows, half), BF16),
            shape_of((rows, width), BF16),
            shape_of((8, width), F32),
        ],
        compiler_params=params(),
        cost_estimate=cost(0, 8 * rows * width),
        name="prep",
    )(side, tok_t, cot_t, cols)


def heads_kernel(own_ref, away_ref, wo_ref, wa_ref, bias_ref, out_ref):
    total = joined_dot(own_ref[...], away_ref[...], wo_ref[...], wa_ref[...])
    out_ref[...] = (total + bias_ref[...]).astype(BF16)


def heads_project(own, away, w_own, w_away, bias):
    rows, wide = own.shape
    half, columns = w_own.shape
    tile = 1280
    left = pl.BlockSpec((rows, wide), lambda i: (0, 0))
    right = pl.BlockSpec((half, tile), lambda i: (0, i))
    return pl.pallas_call(
        heads_kernel,
        grid=(pl.cdiv(columns, tile),),
        in_specs=[left, left, right, right, pl.BlockSpec((1, tile), lambda i: (0, i))],
        out_specs=pl.BlockSpec((rows, tile), lambda i: (0, i)),
        out_shape=shape_of((rows, columns), BF16),
        compiler_params=params(),
        cost_estimate=cost(4 * rows * half * columns, 4 * half * columns + 2 * rows * columns),
        name="heads",
    )(own, away, w_own, w_away, bias)


def lane_ids(shape):
    return lax.broadcasted_iota(jnp.int32, shape, len(shape) - 1)


def pair_of(left, right):
    return jnp.concatenate([left[:, HD:], right[:, :HD]], axis=1)


def causal_fill(scores, fill):
    rows, cols = scores.shape
    shift = cols - rows
    keep = lax.broadcasted_iota(jnp.int32, (rows, rows), 0) >= lax.broadcasted_iota(
        jnp.int32, (rows, rows), 1
    )
    diag = jnp.where(keep, scores[:, shift:], fill)
    return diag if shift == 0 else jnp.concatenate([scores[:, :shift], diag], axis=1)


def attend_kernel(q_ref, ka_ref, kb_ref, v_ref, o_ref, lse_ref):
    p = pl.program_id(1)
    lanes = lane_ids((LEN, 2 * HD))
    q = q_ref[...] * BF16(HD**-0.5)
    k = pair_of(ka_ref[...], kb_ref[...])
    v = jnp.concatenate([v_ref[...], jnp.ones((LEN, 2 * HD), BF16)], axis=1)
    for at in range(0, LEN, QB):
        end = at + QB
        low = lanes[at:end] < HD
        parts = []
        for h in range(2):
            qh = jnp.where(low == (h == 0), q[at:end], BF16(0))
            s = lax.dot_general(qh, k[:end], NT, preferred_element_type=F32)
            s = causal_fill(s, -jnp.inf)
            m = jnp.max(s, axis=1, keepdims=True)
            e = jnp.exp(s - m)
            both = jnp.dot(e.astype(BF16), v[:end], preferred_element_type=F32)
            parts.append((m, both[:, : 2 * HD], both[:, 2 * HD :]))
        out = jnp.where(low, parts[0][1], parts[1][1])
        sums = jnp.where(low, parts[0][2], parts[1][2])
        o_ref[at:end, :] = (out / sums).astype(BF16)
        ln = lanes[at:end]
        for h in range(2):
            value = parts[h][0] + jnp.log(parts[h][2])
            lse_ref[at:end, :] = jnp.where(ln == 2 * p + h, value, lse_ref[at:end, :])


def attend(packed):
    rows = packed.shape[0]
    width = packed.shape[1] // 3
    seqs = rows // LEN
    pairs = pl.cdiv(width, 2 * HD)
    kb, vb = width // (2 * HD), 2 * width // (2 * HD)

    def blk(f):
        return pl.BlockSpec((LEN, 2 * HD), f)

    return pl.pallas_call(
        attend_kernel,
        grid=(seqs, pairs),
        in_specs=[
            blk(lambda s, p: (s, p)),
            blk(lambda s, p: (s, p + kb)),
            blk(lambda s, p: (s, p + kb + 1)),
            blk(lambda s, p: (s, p + vb)),
        ],
        out_specs=[blk(lambda s, p: (s, p)), blk(lambda s, p: (s, 0))],
        out_shape=[shape_of((rows, width), BF16), shape_of((rows, 2 * HD), F32)],
        cost_estimate=cost(rows * LEN * width * 12, 8 * rows * width),
        name="attend",
    )(packed, packed, packed, packed)


def attend_back_kernel(width, q_ref, ka_ref, kb_ref, v_ref, do_ref, o_ref, lse_ref, out_ref, dq_ref):
    p = pl.program_id(1)
    lanes = lane_ids((LEN, 2 * HD))
    low = lanes < HD
    q = q_ref[...] * BF16(HD**-0.5)
    k = pair_of(ka_ref[...], kb_ref[...])
    real = lanes + 2 * HD * p < width
    v = jnp.where(real, v_ref[...], BF16(0))
    dot_t = do_ref[...]
    do = jnp.where(real, dot_t.T, BF16(0))
    o = jnp.where(real, o_ref[...], BF16(0))
    prod = do.astype(F32) * o.astype(F32)
    lse = lse_ref[...]
    q_t = q.T
    for h in range(2):
        mine = low if h == 0 else jnp.logical_not(low)
        qh = jnp.where(mine, q, BF16(0))
        doh = jnp.where(mine, do, BF16(0))
        delta = jnp.sum(jnp.where(mine, prod, 0.0), axis=1, keepdims=True)
        norm = jnp.sum(jnp.where(lanes == 2 * p + h, lse, 0.0), axis=1, keepdims=True)
        rows = slice(h * HD, (h + 1) * HD)
        dk = None
        for at in range(LEN - QB, -1, -QB):
            end = at + QB
            s = lax.dot_general(qh[at:end], k[:end], NT, preferred_element_type=F32)
            w = causal_fill(jnp.exp(s - norm[at:end]), 0.0)
            wb = w.astype(BF16)
            dp = lax.dot_general(doh[at:end], v[:end], NT, preferred_element_type=F32)
            ds = (w * (dp - delta[at:end])).astype(BF16)
            dq = jnp.dot(ds, k[:end], preferred_element_type=F32) * HD**-0.5
            if h == 0:
                dq_ref[at:end, :] = dq.astype(BF16)
            else:
                dq_ref[at:end, :] = jnp.where(low[at:end], dq_ref[at:end, :], dq.astype(BF16))
            dk_part = jnp.dot(q_t[rows, at:end], ds, preferred_element_type=F32)
            dv_part = jnp.dot(dot_t[rows, at:end], wb, preferred_element_type=F32)
            if dk is None:
                dk, dv = dk_part, dv_part
            else:
                dk = jnp.concatenate([dk[:, :end] + dk_part, dk[:, end:]], axis=1)
                dv = jnp.concatenate([dv[:, :end] + dv_part, dv[:, end:]], axis=1)
        out_ref[1, rows, :] = dk.astype(BF16)
        out_ref[2, rows, :] = dv.astype(BF16)
    out_ref[0, :, :] = dq_ref[...].T


def attend_back(packed, grad_t, attended, lse):
    rows = packed.shape[0]
    width = packed.shape[1] // 3
    seqs = rows // LEN
    pairs = pl.cdiv(width, 2 * HD)
    kb, vb = width // (2 * HD), 2 * width // (2 * HD)

    def blk(f):
        return pl.BlockSpec((LEN, 2 * HD), f)

    out = pl.pallas_call(
        functools.partial(attend_back_kernel, width),
        grid=(seqs, pairs),
        in_specs=[
            blk(lambda s, p: (s, p)),
            blk(lambda s, p: (s, p + kb)),
            blk(lambda s, p: (s, p + kb + 1)),
            blk(lambda s, p: (s, p + vb)),
            pl.BlockSpec((2 * HD, LEN), lambda s, p: (p, s)),
            blk(lambda s, p: (s, p)),
            blk(lambda s, p: (s, 0)),
        ],
        out_specs=pl.BlockSpec((3, 2 * HD, LEN), lambda s, p: (0, p, s)),
        out_shape=shape_of((3, width, rows), BF16),
        scratch_shapes=[pltpu.VMEM((LEN, 2 * HD), BF16)],
        cost_estimate=cost(rows * LEN * width * 12, 14 * rows * width),
        name="aback",
    )(packed, packed, packed, packed, grad_t, attended, lse)
    return out.reshape(3 * width, rows)


def project_kernel(
    side_ref, att_ref, x_ref, wo_ref, wa_ref, rows_ref,
    ao_ref, aa_ref, mid_ref, so_ref, sa_ref, n_ref, inv_ref,
):
    side = side_ref[0]
    store_pair(side, att_ref[...], ao_ref, aa_ref)
    mid = joined_dot(ao_ref[...], aa_ref[...], wo_ref[...], wa_ref[...])
    mid += x_ref[...].T.astype(F32) + rows_ref[4:5, :]
    mid_ref[...] = mid.astype(BF16).T
    centred = mid - jnp.mean(mid, axis=1, keepdims=True)
    inverse = lax.rsqrt(jnp.mean(centred * centred, axis=1, keepdims=True) + EPS)
    normed = centred * inverse
    act = (normed * rows_ref[5:6, :] + rows_ref[6:7, :]).astype(BF16)
    store_pair(side, act, so_ref, sa_ref)
    n_ref[...] = normed.astype(BF16).T
    inv_ref[...] = jnp.broadcast_to(inverse, (inverse.shape[0], 128)).T[:8]


def project(side, attended, tok_t, w_own, w_away, small_rows):
    width, rows = tok_t.shape
    half = width // 2
    wide = round_up(half, 128)
    block = min(256, rows)
    nat = pl.BlockSpec((block, width), lambda i, *_: (i, 0))
    pair = pl.BlockSpec((block, wide), lambda i, *_: (i, 0))
    whole = pl.BlockSpec((half, width), lambda i, *_: (0, 0))
    turned = pl.BlockSpec((width, block), lambda i, *_: (0, i))
    return pl.pallas_call(
        project_kernel,
        grid_spec=pltpu.PrefetchScalarGridSpec(
            num_scalar_prefetch=1,
            grid=(rows // block,),
            in_specs=[nat, turned, whole, whole, pl.BlockSpec((8, width), lambda i, *_: (0, 0))],
            out_specs=[
                pair, pair, turned, pair, pair, turned,
                pl.BlockSpec((8, block), lambda i, *_: (0, i)),
            ],
        ),
        out_shape=[
            shape_of((rows, wide), BF16),
            shape_of((rows, wide), BF16),
            shape_of((width, rows), BF16),
            shape_of((rows, wide), BF16),
            shape_of((rows, wide), BF16),
            shape_of((width, rows), BF16),
            shape_of((8, rows), F32),
        ],
        compiler_params=params(),
        cost_estimate=cost(4 * rows * half * width, 4 * half * width + 14 * rows * width),
        name="project",
    )(side, attended, tok_t, w_own, w_away, small_rows)


def hidden_kernel(start_ref, so_ref, sa_ref, wo_ref, wa_ref, bias_ref, act_ref, slope_ref):
    rows = so_ref.shape[0] // 2
    wo, wa = wo_ref[...], wa_ref[...]
    for at in range(0, so_ref.shape[0], rows):
        part = slice(at, at + rows)
        v = joined_dot(so_ref[part, :], sa_ref[part, :], wo, wa)
        v += bias_ref[8:9, :]
        square = v * v
        t = jnp.tanh(TANH_COEF * v * (1.0 + CUBIC * square))
        grown = 0.5 * (1.0 + t)
        act_ref[part, :] = (v * grown).astype(BF16)
        slope = grown * (1.0 + v * (1.0 - t) * (TANH_COEF + 3.0 * TANH_COEF * CUBIC * square))
        slope_ref[part, :] = slope.astype(BF16)


def hidden(start, own, away, w_own, w_away, bias, units):
    rows, wide = own.shape
    half = w_own.shape[0]
    tile = 640
    resident = pl.BlockSpec((rows, wide), lambda i, s: (0, 0))
    right = pl.BlockSpec((half, tile), lambda i, s: (0, s[0] + i))
    out = pl.BlockSpec((rows, tile), lambda i, s: (0, i))
    return pl.pallas_call(
        hidden_kernel,
        grid_spec=pltpu.PrefetchScalarGridSpec(
            num_scalar_prefetch=1,
            grid=(units // tile,),
            in_specs=[resident, resident, right, right, pl.BlockSpec((16, tile), lambda i, s: (0, i))],
            out_specs=[out, out],
        ),
        out_shape=[shape_of((rows, units), BF16)] * 2,
        compiler_params=params(),
        cost_estimate=cost(4 * rows * units * half, 4 * units * half + 4 * rows * units),
        name="hidden",
    )(start, own, away, w_own, w_away, bias)


def hidden_back_kernel(meta_ref, cot_ref, w1_hbm, w2_hbm, s1_hbm, s2_hbm, ge_ref, sum_ref, w_buf, s_buf, sem):
    steps, _, tile = w_buf.shape

    def block_of(first, second):
        return lambda i: (first if i < steps // 2 else second).at[:, pl.ds(i % (steps // 2) * tile, tile)]

    step = pl.program_id(0)
    stream(step, steps, (block_of(w1_hbm, w2_hbm), block_of(s1_hbm, s2_hbm)), (w_buf, s_buf), sem)
    ge = jnp.dot(cot_ref[...], w_buf[step], preferred_element_type=F32) * s_buf[step].astype(F32)
    ge_ref[...] = ge.astype(BF16).T
    sum_ref[...] = jnp.broadcast_to(jnp.sum(ge, axis=0, keepdims=True), sum_ref.shape)


def hidden_back(meta, cot, w_first_t, w_second_t, slope_first, slope_second):
    width, units = w_first_t.shape
    rows = cot.shape[0]
    tile = 640
    steps = units // tile
    place = lambda i, m: jnp.where(i < steps, (1 - m[0]) * steps + i, m[0] * steps + i - steps)
    return pl.pallas_call(
        hidden_back_kernel,
        grid_spec=pltpu.PrefetchScalarGridSpec(
            num_scalar_prefetch=1,
            grid=(2 * steps,),
            in_specs=[pl.BlockSpec((rows, width), lambda i, m: (0, 0))] + [ANYWHERE] * 4,
            out_specs=[
                pl.BlockSpec((tile, rows), lambda i, m: (place(i, m), 0)),
                pl.BlockSpec((8, tile), lambda i, m: (0, place(i, m))),
            ],
            scratch_shapes=[
                pltpu.VMEM((2 * steps, width, tile), BF16),
                pltpu.VMEM((2 * steps, rows, tile), BF16),
                pltpu.SemaphoreType.DMA((2, 2 * steps)),
            ],
        ),
        out_shape=[shape_of((2 * units, rows), BF16), shape_of((8, 2 * units), F32)],
        compiler_params=params(),
        cost_estimate=cost(4 * rows * units * width, 4 * units * width + 8 * rows * units),
        name="hback",
    )(meta, cot, w_first_t, w_second_t, slope_first, slope_second)


ROWS = 160


def middle_kernel(
    meta_ref, g_ref, wo_hbm, wa_hbm, n_hbm, inv_ref, gain_ref, cot_hbm, po_hbm, pa_hbm,
    gm_ref, gmb_ref, ga_ref, s_gain_ref, s_shift_ref, s_bias_ref,
    acc_ref, prod_ref, wo_buf, wa_buf, n_ref, cot_ref, p_ref, sem, sem_late,
):
    side = meta_ref[0]
    width = acc_ref.shape[0]
    half = width // 2
    i = pl.program_id(0)
    steps, tile, _ = wo_buf.shape
    rows = lambda ref: lambda i: ref.at[pl.ds(i * tile, tile), :]
    stream(i, steps, (rows(wo_hbm), rows(wa_hbm)), (wo_buf, wa_buf), sem)
    late = [
        pltpu.make_async_copy(src, dst, sem_late.at[j])
        for j, (src, dst) in enumerate(
            ((n_hbm, n_ref), (cot_hbm, cot_ref), (po_hbm, p_ref.at[0]), (pa_hbm, p_ref.at[1]))
        )
    ]

    @pl.when(i == 0)
    def _():
        for c in late:
            c.start()

    left = jnp.concatenate([wo_buf[i], wa_buf[i]], axis=0)
    total = jnp.dot(left, g_ref[...], preferred_element_type=F32)
    acc_ref[pl.ds(pl.multiple_of(side * half + i * tile, 8), tile), :] = total[:tile]
    acc_ref[pl.ds(pl.multiple_of((1 - side) * half + i * tile, 8), tile), :] = total[tile:]

    @pl.when(i == steps - 1)
    def _():
        for c in late:
            c.wait()
        tokens = acc_ref.shape[1]
        inverse = inv_ref[0:1, :]

        def first(j, sums):
            at = pl.ds(j * ROWS, ROWS)
            e, n = acc_ref[at, :], n_ref[at, :].astype(F32)
            w = e * gain_ref[at, 5:6]
            gmb_ref[at, :] = e.astype(BF16)
            prod_ref[at, :] = (e * n).astype(BF16)
            return (
                sums[0] + jnp.sum(w, axis=0, keepdims=True),
                sums[1] + jnp.sum(w * n, axis=0, keepdims=True),
            )

        zero = jnp.zeros((1, tokens), F32)
        one, two = lax.fori_loop(0, width // ROWS, first, (zero, zero))
        one, two = one / width, two / width
        s_gain_ref[...] = row_sums(prod_ref[...])
        s_shift_ref[...] = row_sums(gmb_ref[...])

        def second(j, _):
            at = pl.ds(j * ROWS, ROWS)
            n = n_ref[at, :].astype(F32)
            back = inverse * (acc_ref[at, :] * gain_ref[at, 5:6] - one - n * two)
            g = cot_ref[at, :].astype(F32) + back
            gm_ref[at, :] = g
            gmb_ref[at, :] = g.astype(BF16)
            return 0

        lax.fori_loop(0, width // ROWS, second, 0)
        g = gmb_ref[...]
        s_bias_ref[...] = row_sums(g)
        part = half // 2

        def attended(j, _):
            which = jnp.bitwise_xor(j // 2, side)
            at = pl.multiple_of(j % 2 * part, 16)
            ga_ref[pl.ds(pl.multiple_of(which * half + at, 16), part), :] = jnp.dot(
                p_ref[j // 2, pl.ds(at, part), :], gmb_ref[...], preferred_element_type=F32
            ).astype(BF16)
            return 0

        lax.fori_loop(0, 4, attended, 0)


def middle_back(meta, ge, w_own, w_away, normed_t, inv_t, cols, cot_t, p_own, p_away):
    units, rows = ge.shape
    half = w_own.shape[0]
    width = 2 * half
    tile = 200
    steps = half // tile
    once = pl.Buffered(1)
    const = lambda shape: pl.BlockSpec(shape, lambda i, m: (0, 0), pipeline_mode=once)
    out = lambda shape: pl.BlockSpec(shape, lambda i, m: (0, 0))
    small = shape_of((8, width), F32)
    return pl.pallas_call(
        middle_kernel,
        grid_spec=pltpu.PrefetchScalarGridSpec(
            num_scalar_prefetch=1,
            grid=(steps,),
            in_specs=[
                const((units, rows)), ANYWHERE, ANYWHERE, ANYWHERE,
                const((8, rows)), const((width, 128)), ANYWHERE, ANYWHERE, ANYWHERE,
            ],
            out_specs=[out((width, rows))] * 3 + [out((8, width))] * 3,
            scratch_shapes=[
                pltpu.VMEM((width, rows), F32),
                pltpu.VMEM((width, rows), BF16),
                pltpu.VMEM((steps, tile, units), BF16),
                pltpu.VMEM((steps, tile, units), BF16),
                pltpu.VMEM((width, rows), BF16),
                pltpu.VMEM((width, rows), BF16),
                pltpu.VMEM((2, half, width), BF16),
                pltpu.SemaphoreType.DMA((2, steps)),
                pltpu.SemaphoreType.DMA((4,)),
            ],
        ),
        out_shape=[
            shape_of((width, rows), F32),
            shape_of((width, rows), BF16),
            shape_of((width, rows), BF16),
            small, small, small,
        ],
        compiler_params=params(),
        cost_estimate=cost(
            2 * rows * units * width + 2 * rows * width * width, 2 * units * width + 12 * rows * width
        ),
        name="middle",
    )(meta, ge, w_own, w_away, normed_t, inv_t, cols, cot_t, p_own, p_away)


def first_kernel(
    meta_ref, gp_ref, wo_hbm, wa_hbm, tok_hbm, gain_ref, gm_hbm,
    out_ref, s_gain_ref, s_shift_ref, s_pack_ref,
    acc_ref, prod_ref, e_ref, wo_buf, wa_buf, tok_ref, gm_ref, sem, sem_late,
):
    side = meta_ref[0]
    width = acc_ref.shape[0]
    half = width // 2
    i = pl.program_id(0)
    steps, tile, _ = wo_buf.shape
    rows = lambda ref: lambda i: ref.at[pl.ds(i * tile, tile), :]
    stream(i, steps, (rows(wo_hbm), rows(wa_hbm)), (wo_buf, wa_buf), sem)
    late = [
        pltpu.make_async_copy(src, dst, sem_late.at[j])
        for j, (src, dst) in enumerate(((tok_hbm, tok_ref), (gm_hbm, gm_ref)))
    ]

    @pl.when(i == 0)
    def _():
        for c in late:
            c.start()

    g = gp_ref[...]
    total = jnp.dot(
        jnp.concatenate([wo_buf[i], wa_buf[i]], axis=0), g, preferred_element_type=F32
    )
    acc_ref[pl.ds(pl.multiple_of(side * half + i * tile, 8), tile), :] = total[:tile]
    acc_ref[pl.ds(pl.multiple_of((1 - side) * half + i * tile, 8), tile), :] = total[tile:]

    @pl.when(i == 0)
    def _():
        s_pack_ref[...] = row_sums(g)

    @pl.when(i == pl.num_programs(0) - 1)
    def _():
        for c in late:
            c.wait()
        tokens = acc_ref.shape[1]
        zero = jnp.zeros((1, tokens), F32)
        loops = width // ROWS

        def total(j, s):
            return s + jnp.sum(tok_ref[pl.ds(j * ROWS, ROWS), :].astype(F32), axis=0, keepdims=True)

        mean = lax.fori_loop(0, loops, total, zero) / width

        def spread_of(j, s):
            c = tok_ref[pl.ds(j * ROWS, ROWS), :].astype(F32) - mean
            return s + jnp.sum(c * c, axis=0, keepdims=True)

        inverse = lax.rsqrt(lax.fori_loop(0, loops, spread_of, zero) / width + EPS)

        def first(j, sums):
            at = pl.ds(j * ROWS, ROWS)
            e = acc_ref[at, :]
            n = (tok_ref[at, :].astype(F32) - mean) * inverse
            w = e * gain_ref[at, 0:1]
            e_ref[at, :] = e.astype(BF16)
            prod_ref[at, :] = (e * n).astype(BF16)
            return (
                sums[0] + jnp.sum(w, axis=0, keepdims=True),
                sums[1] + jnp.sum(w * n, axis=0, keepdims=True),
            )

        one, two = lax.fori_loop(0, loops, first, (zero, zero))
        one, two = one / width, two / width
        s_gain_ref[...] = row_sums(prod_ref[...])
        s_shift_ref[...] = row_sums(e_ref[...])

        def second(j, _):
            at = pl.ds(j * ROWS, ROWS)
            n = (tok_ref[at, :].astype(F32) - mean) * inverse
            back = inverse * (acc_ref[at, :] * gain_ref[at, 0:1] - one - n * two)
            out_ref[at, :] = (gm_ref[at, :] + back).astype(BF16)
            return 0

        lax.fori_loop(0, loops, second, 0)


def first_back(meta, gp_t, w_own, w_away, tok_t, cols, gm_t):
    columns, rows = gp_t.shape
    half = w_own.shape[0]
    width = 2 * half
    tile = 200
    steps = half // tile
    const = lambda shape: pl.BlockSpec(shape, lambda i, m: (0, 0))
    return pl.pallas_call(
        first_kernel,
        grid_spec=pltpu.PrefetchScalarGridSpec(
            num_scalar_prefetch=1,
            grid=(steps,),
            in_specs=[
                const((columns, rows)), ANYWHERE, ANYWHERE, ANYWHERE, const((width, 128)), ANYWHERE,
            ],
            out_specs=[const((width, rows)), const((8, width)), const((8, width)), const((8, columns))],
            scratch_shapes=[
                pltpu.VMEM((width, rows), F32),
                pltpu.VMEM((width, rows), BF16),
                pltpu.VMEM((width, rows), BF16),
                pltpu.VMEM((steps, tile, columns), BF16),
                pltpu.VMEM((steps, tile, columns), BF16),
                pltpu.VMEM((width, rows), BF16),
                pltpu.VMEM((width, rows), F32),
                pltpu.SemaphoreType.DMA((2, steps)),
                pltpu.SemaphoreType.DMA((2,)),
            ],
        ),
        out_shape=[
            shape_of((width, rows), BF16),
            shape_of((8, width), F32),
            shape_of((8, width), F32),
            shape_of((8, columns), F32),
        ],
        compiler_params=params(),
        cost_estimate=cost(4 * rows * half * columns, 4 * half * columns + 2 * rows * columns + 10 * rows * width),
        name="first",
    )(meta, gp_t, w_own, w_away, tok_t, cols, gm_t)


def output_kernel(a1_ref, a2_ref, w1_hbm, w2_hbm, mid_ref, cols_ref, out_ref, w1_buf, w2_buf, sem):
    i = pl.program_id(0)
    steps, tile, _ = w1_buf.shape
    rows = lambda ref: lambda i: ref.at[pl.ds(i * tile, tile), :]
    stream(i, steps, (rows(w1_hbm), rows(w2_hbm)), (w1_buf, w2_buf), sem)
    weights = jnp.concatenate([w1_buf[i], w2_buf[i]], axis=1)
    acts = jnp.concatenate([a1_ref[...], a2_ref[...]], axis=1)
    total = lax.dot_general(weights, acts, NT, preferred_element_type=F32)
    out_ref[...] = (total + mid_ref[...].astype(F32) + cols_ref[:, 7:8]).astype(BF16)


def block_output(act_first, act_second, w_away_t, w_own_t, middle_t, cols):
    rows, units = act_first.shape
    width = w_own_t.shape[0]
    tile = 400
    left = pl.BlockSpec((rows, units), lambda i: (0, 0))
    steps = width // tile
    part = pl.BlockSpec((tile, rows), lambda i: (i, 0))
    return pl.pallas_call(
        output_kernel,
        grid=(width // tile,),
        in_specs=[left, left, ANYWHERE, ANYWHERE, part, pl.BlockSpec((tile, 128), lambda i: (i, 0))],
        out_specs=part,
        scratch_shapes=[pltpu.VMEM((steps, tile, units), BF16)] * 2 + [pltpu.SemaphoreType.DMA((2, steps))],
        out_shape=shape_of((width, rows), BF16),
        compiler_params=params(),
        cost_estimate=cost(4 * rows * units * width, 4 * units * width + 4 * rows * units + 6 * rows * width),
        name="output",
    )(act_first, act_second, w_away_t, w_own_t, middle_t, cols)


class Group:
    def __init__(self, count, lanes, chunks, plan):
        self.count, self.lanes, self.chunks = count, lanes, chunks
        shares, orders = plan
        bits = count.bit_length() - 1
        self.orders = [list(order) + list(range(len(order), bits)) for order in orders]
        tiles = lanes // 128
        one, two = (round(tiles * share) for share in shares)
        self.cuts = [0, one * 128, (one + two) * 128, tiles * 128]
        self.widths = [self.cuts[k + 1] - self.cuts[k] for k in range(3)]
        self.left_over = lanes % 128
        self.pieces = self.widths[2] // self.left_over if self.left_over else 0

    def padded(self, which):
        return round_up(self.chunks[which], 16)

    def each(self, which):
        return pl.cdiv(self.chunks[which], self.pieces)

    def packed(self, which):
        return round_up(self.each(which), 16) if self.left_over else 0

    def rows(self, k, which):
        return self.padded(which) + (self.packed(which) if k == 2 else 0)

    def base(self, k, which):
        return sum(self.rows(k, w) for w in range(which))

    def total_rows(self, k):
        return self.base(k, len(self.chunks))


SLOTS = 4


def spread_kernel(spec, meta_ref, *refs):
    group, batches, starts = spec
    members = len(batches)
    inputs, refs = refs[: 4 * members], refs[4 * members :]
    keeps, sends, refs = refs[:3], refs[3:6], refs[6:]
    step = pl.program_id(0)
    rank = meta_ref[0]
    half = group.count // 2
    lanes = group.lanes

    def member(which):
        lo_ref, la_ref, ro_ref, ra_ref = inputs[4 * which : 4 * which + 4]
        stages, sem = refs[4 * which : 4 * which + 3], refs[4 * which + 3]
        chunk, batch = group.chunks[which], batches[which]
        padded = group.padded(which)

        def rows_of(k):
            return pl.ds(group.base(k, which), group.rows(k, which))

        def wait_slot(slot):
            for k in range(3):
                pltpu.make_async_copy(
                    stages[k].at[slot], keeps[k].at[0, rows_of(k), :], sem.at[k, slot]
                ).wait()

        def work():
            local = step - starts[which]
            total = joined_dot(lo_ref[...], la_ref[...], ro_ref[:, :lanes], ra_ref[:, :lanes])
            for s in range(batch):
                index = local * batch + s
                slot = s % SLOTS if batch % SLOTS == 0 else lax.rem(index, SLOTS)
                if s >= SLOTS:
                    wait_slot(slot)
                else:
                    pl.when(index >= SLOTS)(lambda slot=slot: wait_slot(slot))
                mixed = jnp.bitwise_xor(index, rank)
                part = total[s * chunk : (s + 1) * chunk]
                for k in range(3):
                    low, width = group.cuts[k], group.widths[k]
                    stages[k][slot, :chunk, :] = part[:, low : low + width].astype(BF16)
                    if k == 2 and group.left_over:
                        each, pieces = group.each(which), group.pieces
                        extra = part[:, low + width :]
                        if pieces * each > chunk:
                            extra = jnp.concatenate(
                                [extra, jnp.zeros((pieces * each - chunk, group.left_over), F32)], axis=0
                            )
                        extra = jnp.concatenate(
                            [extra[j * each : (j + 1) * each] for j in range(pieces)], axis=1
                        )
                        stages[k][slot, padded : padded + each, :] = extra.astype(BF16)
                    place = jnp.int32(0)
                    order = group.orders[k]
                    for depth, bit in enumerate(order):
                        place += ((mixed >> bit) & 1) << (len(order) - 1 - depth)

                    @pl.when(place < half)
                    def _(k=k, slot=slot, place=place):
                        pltpu.make_async_copy(
                            stages[k].at[slot], keeps[k].at[place, rows_of(k), :], sem.at[k, slot]
                        ).start()

                    @pl.when(place >= half)
                    def _(k=k, slot=slot, place=place):
                        pltpu.make_async_copy(
                            stages[k].at[slot], sends[k].at[place - half, rows_of(k), :], sem.at[k, slot]
                        ).start()

        return work, wait_slot

    parts = [member(which) for which in range(members)]
    for which, (work, _) in enumerate(parts):
        if members == 1:
            work()
        else:
            pl.when((step >= starts[which]) & (step < starts[which + 1]))(work)

    @pl.when(step == starts[members] - 1)
    def _():
        for _, wait_slot in parts:
            for slot in range(SLOTS):
                wait_slot(slot)


def spread(group, meta, lefts, rights):
    count = group.count
    batches, starts, specs, scratch, ins = [], [0], [], [], []
    flops = 0
    for which, ((left_own, left_away), right) in enumerate(zip(lefts, rights)):
        columns, tokens = left_own.shape
        chunk = group.chunks[which]
        batch = 1
        while batch * chunk % 16:
            batch *= 2
        steps, start = columns // (batch * chunk), starts[-1]
        left = pl.BlockSpec(
            (batch * chunk, tokens),
            lambda i, *_, start=start, steps=steps: (jnp.clip(i - start, 0, steps - 1), 0),
        )
        whole = pl.BlockSpec(right[0].shape, lambda i, *_: (0, 0))
        specs += [left, left, whole, whole]
        ins += [left_own, left_away, *right]
        scratch += [pltpu.VMEM((SLOTS, group.rows(k, which), group.widths[k]), BF16) for k in range(3)]
        scratch.append(pltpu.SemaphoreType.DMA((3, SLOTS)))
        batches.append(batch)
        starts.append(start + steps)
        flops += 4 * columns * tokens * group.lanes
    outs = [shape_of((count // 2, group.total_rows(k), group.widths[k]), BF16) for k in range(3)] * 2
    return pl.pallas_call(
        functools.partial(spread_kernel, (group, batches, starts)),
        grid_spec=pltpu.PrefetchScalarGridSpec(
            num_scalar_prefetch=1,
            grid=(starts[-1],),
            in_specs=specs,
            out_specs=[ANYWHERE] * len(outs),
            scratch_shapes=scratch,
        ),
        out_shape=outs,
        compiler_params=params(),
        cost_estimate=cost(flops, flops // 256),
        name="spread",
    )(meta, *ins)


def merge_kernel(*refs):
    for k in range(3):
        keep_low, came_low, keep_high, came_high = refs[4 * k : 4 * k + 4]
        keep, send = refs[12 + k], refs[15 + k]
        keep[...] = (keep_low[...].astype(F32) + came_low[...].astype(F32)).astype(BF16)
        send[...] = (keep_high[...].astype(F32) + came_high[...].astype(F32)).astype(BF16)


def merge(keeps, arrived):
    half = keeps[0].shape[0] // 2
    ins, specs, outs, out_specs = [], [], [], []
    moved = 0
    for keep, came in zip(keeps, arrived):
        shape = (1,) + keep.shape[1:]
        low = pl.BlockSpec(shape, lambda i: (i, 0, 0))
        high = pl.BlockSpec(shape, lambda i: (i + half, 0, 0))
        ins += [keep, came, keep, came]
        specs += [low, low, high, high]
        outs.append(shape_of((half,) + keep.shape[1:], BF16))
        out_specs.append(low)
        moved += 6 * keep.size
    return pl.pallas_call(
        merge_kernel,
        grid=(half,),
        in_specs=specs,
        out_specs=out_specs * 2,
        out_shape=outs * 2,
        compiler_params=params(),
        cost_estimate=cost(0, moved),
        name="merge",
    )(*ins)


def finish_kernel(group, *refs):
    outs = refs[6:]
    totals = [refs[2 * k][0].astype(F32) + refs[2 * k + 1][0].astype(F32) for k in range(3)]
    for which, chunk in enumerate(group.chunks):
        out = outs[which]
        for k in range(3):
            base = group.base(k, which)
            out[:, group.cuts[k] : group.cuts[k + 1]] = totals[k][base : base + chunk]
        width = group.left_over
        if width:
            base = group.base(2, which) + group.padded(which)
            rest = totals[2][base : base + group.each(which)]
            rest = jnp.concatenate([rest[:, j * width : (j + 1) * width] for j in range(group.pieces)], axis=0)
            out[:, group.cuts[3] :] = rest[:chunk]


def finish(group, keeps, arrived):
    ins = []
    for keep, came in zip(keeps, arrived):
        ins += [keep, came]
    res = pl.pallas_call(
        functools.partial(finish_kernel, group),
        out_shape=[shape_of((chunk, group.lanes), F32) for chunk in group.chunks],
        compiler_params=params(),
        cost_estimate=cost(0, 8 * sum(group.chunks) * group.lanes),
        name="finish",
    )(*ins)
    return [x.T for x in res]


ORDER = (
    "sc", "hb", "mid", "mc", "e", "ab", "mc", "sh", "me", "mc", "first", "s", "mh", "s", "me",
    "mh", "s", "me", "out", "s", "mc", "s", "mh", "s", "me", "mh",
)

PLANS = (
    ((0.36, 0.36), ((0, 2, 1, 3), (1, 0, 2, 3), (2, 1, 0, 3))),
    ((0.33, 0.33), ((0, 1, 2, 3), (1, 2, 0, 3), (2, 0, 1, 3))),
    ((0.5, 0.33), ((0, 1, 2, 3), (1, 0, 2, 3), (2, 1, 0, 3))),
)


def all_steps(bits):
    steps = list(ORDER)
    for name in ("mc", "me", "mh"):
        steps += [name] * (bits - steps.count(name))
    return steps + ["s"] * (bits + 2 - steps.count("s"))


def solution(mesh):
    count = mesh.shape["rep"]
    assert mesh.shape["grp"] == 2
    bits = count.bit_length() - 1
    assert 1 << bits == count and bits >= 4

    def per_device(
        tokens,
        first_gain,
        first_shift,
        w_heads,
        query_bias,
        value_bias,
        w_project,
        project_bias,
        second_gain,
        second_shift,
        w_expand,
        expand_bias,
        w_contract,
        contract_bias,
        cotangent,
    ):
        width = tokens.shape[1]
        units = w_contract.shape[0]
        side = lax.axis_index("grp")
        rank = lax.axis_index("rep")
        sides = jnp.reshape(side, (1,))

        smalls = (
            first_gain,
            first_shift,
            query_bias,
            value_bias,
            project_bias,
            second_gain,
            second_shift,
            contract_bias,
            expand_bias,
        )
        tok_t, cot_t, contract_own = tokens.T, cotangent.T, w_contract.T
        own_small = gather_smalls(smalls)
        away_small = swap_group(own_small)
        heads_in, _ = lax.optimization_barrier((w_heads, away_small))
        heads_away = swap_group(heads_in)
        small_rows, cols, packed_row = unpack_smalls(sides, own_small, away_small, width)
        first_own, first_out, cot, cot_sum = prep(sides, tok_t, cot_t, cols)
        w_project_in, _ = lax.optimization_barrier((w_project, first_own))
        project_away = swap_group(w_project_in)
        packed = heads_project(first_own, first_out, w_heads, heads_away, packed_row)

        latest = [packed]


        def hold(x):
            return lax.optimization_barrier((x, latest[0]))[0]

        def held(out):
            latest[0] = jax.tree.leaves(out)[0]
            return out

        w_expand_in, _ = lax.optimization_barrier((hold(w_expand), project_away))
        expand_away = swap_group(w_expand_in)
        contract_away = swap_group(hold(contract_own))
        cot_away_t = swap_group(hold(cot_t))
        first_away = swap_group(hold(first_out))

        tiles = units // 640
        start_first = jnp.reshape((1 - side) * tiles, (1,)).astype(jnp.int32)
        start_second = jnp.reshape(side * tiles, (1,)).astype(jnp.int32)

        def do_hidden(start, bias):
            return held(hidden(hold(start), second_own, second_out, w_expand, expand_away, bias, units))

        attended, lse = held(attend(packed))
        att_own, att_out, middle_t, second_own, second_out, normed_t, inv_t = held(project(
            sides, attended, tok_t, w_project, project_away, small_rows
        ))
        act_first, slope_first = do_hidden(start_first, away_small)
        act_away = swap_group(act_first)
        act_second, slope_second = do_hidden(start_second, own_small)

        chunk_d = width // count
        chunk_f = 2 * units // count
        chunk_h = w_heads.shape[1] // count
        groups = {
            "c": Group(count, units, [chunk_d], PLANS[0]),
            "e": Group(count, width // 2, [chunk_f, chunk_d], PLANS[1]),
            "h": Group(count, width // 2, [chunk_h], PLANS[2]),
        }
        rank_of = jnp.reshape(rank, (1,)).astype(jnp.int32)
        state, results = {}, {}
        r = types.SimpleNamespace()

        def send(name, buffers):
            group = groups[name]
            state[name] = [list(buffers[:3]), 0, [
                exchange(buffers[3 + k], 1 << group.orders[k][0], count) for k in range(3)
            ]]

        def advance(name):
            group = groups[name]
            keeps, depth, arrived = state[name]
            keeps = [hold(keeps[0])] + keeps[1:]
            if depth == bits - 1:
                results[name] = held(finish(group, keeps, arrived))
                return
            buffers = held(merge(keeps, arrived))
            state[name] = [list(buffers[:3]), depth + 1, [
                exchange(buffers[3 + k], 1 << group.orders[k][depth + 1], count) for k in range(3)
            ]]

        def do_contract():
            send("c", held(spread(
                groups["c"], hold(rank_of), [(cot_t, cot_away_t)], [(act_second, act_away)]
            )))

        def do_hidden_back():
            r.ge, r.eb = held(hidden_back(
                hold(sides), cot, contract_away, contract_own, slope_first, slope_second
            ))
            r.ge_away = swap_group(r.ge)
            r.second_away = swap_group(second_out)
            r.att_away = swap_group(att_out)

        def do_middle():
            r.gm_t, r.gmb_t, r.ga_t, r.s_gain2, r.s_shift2, r.s_pb = held(middle_back(
                hold(sides), r.ge, w_expand, expand_away, normed_t, inv_t,
                cols, cot_t, w_project, project_away,
            ))
            r.gmb_away = swap_group(r.gmb_t)

        def do_expand():
            send("e", held(spread(
                groups["e"], hold(rank_of), [(r.ge, r.ge_away), (r.gmb_t, r.gmb_away)],
                [(second_own, r.second_away), (att_own, r.att_away)],
            )))

        def do_attend_back():
            r.gp_t = held(attend_back(hold(packed), r.ga_t, attended, lse))
            r.gp_away = swap_group(r.gp_t)

        def do_heads():
            send("h", held(spread(
                groups["h"], hold(rank_of), [(r.gp_t, r.gp_away)], [(first_own, first_away)]
            )))

        def do_first():
            r.grad_tokens_t, r.s_gain1, r.s_shift1, r.s_pack = held(first_back(
                hold(sides), r.gp_t, w_heads, heads_away, tok_t, cols, r.gm_t
            ))

        def do_output():
            r.block_out_t = held(
                block_output(hold(act_first), act_second, contract_away, contract_own, middle_t, cols)
            )

        small = []

        def do_small():
            if not small:
                mine, theirs = held(collect(
                    hold(sides), r.s_pack, r.eb,
                    [r.s_gain1, r.s_shift1, r.s_pb, r.s_gain2, r.s_shift2, cot_sum],
                ))
                small.extend([mine, swap_group(theirs), 0])
                return
            vector, arrived, bit = small
            if bit == bits:
                small[0] = held(divide(hold(vector), arrived, [width // 2] * 8 + [units]))
                return
            vector = held(add(hold(vector), arrived))
            small[:] = [vector, exchange(vector, 1 << (bits - 1 - bit), count), bit + 1]

        steps = {
            "sc": do_contract, "hb": do_hidden_back, "mid": do_middle,
            "e": do_expand, "ab": do_attend_back,
            "sh": do_heads, "first": do_first, "out": do_output, "s": do_small,
            "mc": lambda: advance("c"), "me": lambda: advance("e"),
            "mh": lambda: advance("h"),
        }
        for name in all_steps(bits):
            steps[name]()
        finals = small[0]
        (out_w_contract,) = results["c"]
        out_w_expand, out_w_project = results["e"]
        (out_w_heads,) = results["h"]
        grad_tokens_t, block_out_t = r.grad_tokens_t, r.block_out_t

        return (
            block_out_t.T,
            grad_tokens_t.T,
            finals[0],
            finals[1],
            out_w_heads,
            finals[2],
            finals[3],
            out_w_project,
            finals[4],
            finals[5],
            finals[6],
            out_w_expand,
            finals[8],
            out_w_contract,
            finals[7],
        )

    placed = (
        P(("rep", "grp"), None),
        P("grp"),
        P("grp"),
        P("grp", None),
        P("grp"),
        P("grp"),
        P("grp", None),
        P("grp"),
        P("grp"),
        P("grp"),
        P("grp", None),
        P("grp"),
        P("grp", None),
        P("grp"),
        P(("rep", "grp"), None),
    )
    return jax.shard_map(
        per_device,
        mesh=mesh,
        in_specs=placed,
        out_specs=(
            P(("rep", "grp"), None),
            P(("rep", "grp"), None),
            P("grp"),
            P("grp"),
            P("grp", "rep"),
            P("grp"),
            P("grp"),
            P("grp", "rep"),
            P("grp"),
            P("grp"),
            P("grp"),
            P("grp", "rep"),
            P("grp"),
            P("grp", "rep"),
            P("grp"),
        ),
        check_vma=False,
    )
```

```python
import functools
import types

import jax
import jax.numpy as jnp
from jax import lax
from jax.experimental import pallas as pl
from jax.experimental.pallas import tpu as pltpu
from jax.sharding import PartitionSpec as P


HD = 64
LEN = 512
QB = 256
EPS = 1e-05
TANH_COEF = 0.7978845608028654
CUBIC = 0.044715
F32 = jnp.float32
BF16 = jnp.bfloat16
NT = (((1,), (1,)), ((), ()))
VMEM_LIMIT = 67_043_328


def shape_of(shape, dtype):
    return jax.ShapeDtypeStruct(shape, dtype)


def params():
    return pltpu.CompilerParams(vmem_limit_bytes=VMEM_LIMIT)


def cost(flops, moved):
    return pl.CostEstimate(flops=int(flops), bytes_accessed=int(moved), transcendentals=0)


def round_up(n, k):
    return -(-n // k) * k


def swap_group(x):
    return lax.ppermute(x, "grp", [(0, 1), (1, 0)])


def exchange(x, mask, count):
    return lax.ppermute(x, "rep", [(i, i ^ mask) for i in range(count)])


def row_sums(x):
    ones = jnp.ones((8, x.shape[1]), BF16)
    return lax.dot_general(ones, x, NT, preferred_element_type=F32)


def joined_dot(left_one, left_two, right_one, right_two):
    missing = left_one.shape[1] - right_one.shape[0]
    rights = [right_one, right_two]
    if missing:
        fill = jnp.zeros((missing, right_one.shape[1]), right_one.dtype)
        rights = [right_one, fill, right_two, fill]
    left = jnp.concatenate([left_one, left_two], axis=1)
    return jnp.dot(left, jnp.concatenate(rights, axis=0), preferred_element_type=F32)


def stream(step, steps, sources, buffers, sem):
    @pl.when(step == 0)
    def _():
        for i in range(steps):
            for j, (source, buffer) in enumerate(zip(sources, buffers)):
                pltpu.make_async_copy(source(i), buffer.at[i], sem.at[j, i]).start()

    for j, (source, buffer) in enumerate(zip(sources, buffers)):
        pltpu.make_async_copy(source(0), buffer.at[step], sem.at[j, step]).wait()


ANYWHERE = pl.BlockSpec(memory_space=pl.ANY)


def store_pair(side, value, own_ref, away_ref):
    half = value.shape[1] // 2
    fill = jnp.zeros((value.shape[0], own_ref.shape[1] - half), value.dtype)
    low = jnp.concatenate([value[:, :half], fill], axis=1)
    high = jnp.concatenate([value[:, half:], fill], axis=1)

    @pl.when(side == 0)
    def _():
        own_ref[...] = low
        away_ref[...] = high

    @pl.when(side == 1)
    def _():
        own_ref[...] = high
        away_ref[...] = low


def gather_kernel(*refs):
    out = refs[-1]
    out[...] = jnp.zeros_like(out)
    for i, ref in enumerate(refs[:-1]):
        out[i : i + 1, : ref.shape[0]] = ref[...].astype(F32).reshape(1, ref.shape[0])


def gather_smalls(smalls):
    widest = max(x.shape[0] for x in smalls)
    return pl.pallas_call(gather_kernel, out_shape=shape_of((16, widest), F32), compiler_params=params(), name="gather")(*smalls)


def unpack_kernel(side_ref, own_ref, away_ref, rows_ref, cols_ref, packed_ref):
    half = rows_ref.shape[1] // 2
    first = side_ref[0] == 0
    own, away = own_ref[0:8, :half], away_ref[0:8, :half]
    low = jnp.where(first, own, away)
    high = jnp.where(first, away, own)
    rows = jnp.concatenate([low, high], axis=1)
    rows_ref[...] = rows
    cols_ref[...] = jnp.concatenate([rows, jnp.zeros((120, 2 * half), F32)], axis=0).T
    packed_ref[...] = jnp.concatenate([rows[2:3], jnp.zeros((1, 2 * half), F32), rows[3:4]], axis=1)


def unpack_smalls(side, own, away, width):
    vmem = pl.BlockSpec(memory_space=pltpu.VMEM)
    return pl.pallas_call(
        unpack_kernel,
        in_specs=[pl.BlockSpec(memory_space=pltpu.SMEM), vmem, vmem],
        out_shape=[shape_of((8, width), F32), shape_of((width, 128), F32), shape_of((1, 3 * width), F32)],
        compiler_params=params(), name="unpack",
    )(side, own, away)


def collect_kernel(side_ref, pack_ref, eb_ref, *refs):
    rows, (mine_ref, theirs_ref) = refs[:-2], refs[-2:]
    width = rows[0].shape[1]
    half = width // 2
    first = side_ref[0] == 0
    pack = pack_ref[0:1, :]
    full = [r[0:1, :] for r in rows[:2]] + [pack[:, :width], pack[:, 2 * width :]]
    full += [r[0:1, :] for r in rows[2:]]
    full = jnp.concatenate(full, axis=0)
    low, high = full[:, :half], full[:, half:]
    mine_ref[...] = jnp.zeros_like(mine_ref)
    theirs_ref[...] = jnp.zeros_like(theirs_ref)
    mine_ref[0:8, :half] = jnp.where(first, low, high)
    theirs_ref[0:8, :half] = jnp.where(first, high, low)
    units = mine_ref.shape[1]
    low, high = eb_ref[0:1, :units], eb_ref[0:1, units:]
    mine_ref[8:9, :] = jnp.where(first, low, high)
    theirs_ref[8:9, :] = jnp.where(first, high, low)


def collect(side, pack, eb, rows):
    vmem = pl.BlockSpec(memory_space=pltpu.VMEM)
    out = shape_of((16, eb.shape[1] // 2), F32)
    return pl.pallas_call(
        collect_kernel,
        in_specs=[pl.BlockSpec(memory_space=pltpu.SMEM)] + [vmem] * (2 + len(rows)),
        out_shape=[out, out],
        compiler_params=params(), name="collect",
    )(side, pack, eb, *rows)


def add_kernel(a_ref, b_ref, out_ref):
    out_ref[...] = a_ref[...] + b_ref[...]


def add(a, b):
    return pl.pallas_call(add_kernel, out_shape=shape_of(a.shape, a.dtype), compiler_params=params(), name="add")(a, b)


def divide_kernel(a_ref, b_ref, *outs):
    total = a_ref[...] + b_ref[...]
    for i, out in enumerate(outs):
        out[...] = total[i : i + 1, : out.shape[0]].reshape(out.shape[0])


def divide(a, b, sizes):
    return pl.pallas_call(
        divide_kernel, out_shape=[shape_of((n,), F32) for n in sizes], compiler_params=params(), name="divide"
    )(a, b)


def prep_kernel(side_ref, x_ref, c_ref, cols_ref, own_ref, away_ref, cot_ref, sum_ref, act_ref):
    x = x_ref[...].astype(F32)
    half = x.shape[0] // 2
    side = side_ref[0]
    centred = x - jnp.mean(x, axis=0, keepdims=True)
    inverse = lax.rsqrt(jnp.mean(centred * centred, axis=0, keepdims=True) + EPS)
    act_ref[...] = (centred * inverse * cols_ref[:, 0:1] + cols_ref[:, 1:2]).astype(BF16)
    for ref, which in ((own_ref, side), (away_ref, 1 - side)):
        ref[:, :half] = act_ref[pl.ds(pl.multiple_of(which * half, 16), half), :].T
        ref[:, half:] = jnp.zeros((ref.shape[0], ref.shape[1] - half), BF16)
    cot = c_ref[...].T
    cot_ref[...] = cot
    part = jnp.sum(cot.astype(F32), axis=0, keepdims=True)
    part = jnp.broadcast_to(part, sum_ref.shape)

    @pl.when(pl.program_id(0) == 0)
    def _():
        sum_ref[...] = part

    @pl.when(pl.program_id(0) > 0)
    def _():
        sum_ref[...] += part


def prep(side, tok_t, cot_t, cols):
    width, rows = tok_t.shape
    block = min(128, rows)
    half = round_up(width // 2, 128)
    nat = pl.BlockSpec((block, width), lambda i, *_: (i, 0))
    turned = pl.BlockSpec((width, block), lambda i, *_: (0, i))
    pair = pl.BlockSpec((block, half), lambda i, *_: (i, 0))
    return pl.pallas_call(
        prep_kernel,
        grid_spec=pltpu.PrefetchScalarGridSpec(
            num_scalar_prefetch=1,
            grid=(rows // block,),
            in_specs=[turned, turned, pl.BlockSpec((width, 128), lambda i, *_: (0, 0))],
            out_specs=[pair, pair, nat, pl.BlockSpec((8, width), lambda i, *_: (0, 0))],
            scratch_shapes=[pltpu.VMEM((width, block), BF16)],
        ),
        out_shape=[
            shape_of((rows, half), BF16),
            shape_of((rows, half), BF16),
            shape_of((rows, width), BF16),
            shape_of((8, width), F32),
        ],
        compiler_params=params(),
        cost_estimate=cost(0, 8 * rows * width),
        name="prep",
    )(side, tok_t, cot_t, cols)


def heads_kernel(own_ref, away_ref, wo_ref, wa_ref, bias_ref, out_ref):
    total = joined_dot(own_ref[...], away_ref[...], wo_ref[...], wa_ref[...])
    out_ref[...] = (total + bias_ref[...]).astype(BF16)


def heads_project(own, away, w_own, w_away, bias):
    rows, wide = own.shape
    half, columns = w_own.shape
    tile = 1280
    left = pl.BlockSpec((rows, wide), lambda i: (0, 0))
    right = pl.BlockSpec((half, tile), lambda i: (0, i))
    return pl.pallas_call(
        heads_kernel,
        grid=(pl.cdiv(columns, tile),),
        in_specs=[left, left, right, right, pl.BlockSpec((1, tile), lambda i: (0, i))],
        out_specs=pl.BlockSpec((rows, tile), lambda i: (0, i)),
        out_shape=shape_of((rows, columns), BF16),
        compiler_params=params(),
        cost_estimate=cost(4 * rows * half * columns, 4 * half * columns + 2 * rows * columns),
        name="heads",
    )(own, away, w_own, w_away, bias)


def lane_ids(shape):
    return lax.broadcasted_iota(jnp.int32, shape, len(shape) - 1)


def pair_of(left, right):
    return jnp.concatenate([left[:, HD:], right[:, :HD]], axis=1)


def causal_fill(scores, fill):
    rows, cols = scores.shape
    shift = cols - rows
    keep = lax.broadcasted_iota(jnp.int32, (rows, rows), 0) >= lax.broadcasted_iota(
        jnp.int32, (rows, rows), 1
    )
    diag = jnp.where(keep, scores[:, shift:], fill)
    return diag if shift == 0 else jnp.concatenate([scores[:, :shift], diag], axis=1)


def attend_kernel(q_ref, ka_ref, kb_ref, v_ref, o_ref, lse_ref):
    p = pl.program_id(1)
    lanes = lane_ids((LEN, 2 * HD))
    q = q_ref[...] * BF16(HD**-0.5)
    k = pair_of(ka_ref[...], kb_ref[...])
    v = jnp.concatenate([v_ref[...], jnp.ones((LEN, 2 * HD), BF16)], axis=1)
    for at in range(0, LEN, QB):
        end = at + QB
        low = lanes[at:end] < HD
        parts = []
        for h in range(2):
            qh = jnp.where(low == (h == 0), q[at:end], BF16(0))
            s = lax.dot_general(qh, k[:end], NT, preferred_element_type=F32)
            s = causal_fill(s, -jnp.inf)
            m = jnp.max(s, axis=1, keepdims=True)
            e = jnp.exp(s - m)
            both = jnp.dot(e.astype(BF16), v[:end], preferred_element_type=F32)
            parts.append((m, both[:, : 2 * HD], both[:, 2 * HD :]))
        out = jnp.where(low, parts[0][1], parts[1][1])
        sums = jnp.where(low, parts[0][2], parts[1][2])
        o_ref[at:end, :] = (out / sums).astype(BF16)
        ln = lanes[at:end]
        for h in range(2):
            value = parts[h][0] + jnp.log(parts[h][2])
            lse_ref[at:end, :] = jnp.where(ln == 2 * p + h, value, lse_ref[at:end, :])


def attend(packed):
    rows = packed.shape[0]
    width = packed.shape[1] // 3
    seqs = rows // LEN
    pairs = pl.cdiv(width, 2 * HD)
    kb, vb = width // (2 * HD), 2 * width // (2 * HD)

    def blk(f):
        return pl.BlockSpec((LEN, 2 * HD), f)

    return pl.pallas_call(
        attend_kernel,
        grid=(seqs, pairs),
        in_specs=[
            blk(lambda s, p: (s, p)),
            blk(lambda s, p: (s, p + kb)),
            blk(lambda s, p: (s, p + kb + 1)),
            blk(lambda s, p: (s, p + vb)),
        ],
        out_specs=[blk(lambda s, p: (s, p)), blk(lambda s, p: (s, 0))],
        out_shape=[shape_of((rows, width), BF16), shape_of((rows, 2 * HD), F32)],
        cost_estimate=cost(rows * LEN * width * 12, 8 * rows * width),
        compiler_params=params(), name="attend",
    )(packed, packed, packed, packed)


def attend_back_kernel(width, q_ref, ka_ref, kb_ref, v_ref, do_ref, o_ref, lse_ref, out_ref, dq_ref):
    p = pl.program_id(1)
    lanes = lane_ids((LEN, 2 * HD))
    low = lanes < HD
    q = q_ref[...] * BF16(HD**-0.5)
    k = pair_of(ka_ref[...], kb_ref[...])
    real = lanes + 2 * HD * p < width
    v = jnp.where(real, v_ref[...], BF16(0))
    dot_t = do_ref[...]
    do = jnp.where(real, dot_t.T, BF16(0))
    o = jnp.where(real, o_ref[...], BF16(0))
    prod = do.astype(F32) * o.astype(F32)
    lse = lse_ref[...]
    q_t = q.T
    for h in range(2):
        mine = low if h == 0 else jnp.logical_not(low)
        qh = jnp.where(mine, q, BF16(0))
        doh = jnp.where(mine, do, BF16(0))
        delta = jnp.sum(jnp.where(mine, prod, 0.0), axis=1, keepdims=True)
        norm = jnp.sum(jnp.where(lanes == 2 * p + h, lse, 0.0), axis=1, keepdims=True)
        rows = slice(h * HD, (h + 1) * HD)
        dk = None
        for at in range(LEN - QB, -1, -QB):
            end = at + QB
            s = lax.dot_general(qh[at:end], k[:end], NT, preferred_element_type=F32)
            w = causal_fill(jnp.exp(s - norm[at:end]), 0.0)
            wb = w.astype(BF16)
            dp = lax.dot_general(doh[at:end], v[:end], NT, preferred_element_type=F32)
            ds = (w * (dp - delta[at:end])).astype(BF16)
            dq = jnp.dot(ds, k[:end], preferred_element_type=F32) * HD**-0.5
            if h == 0:
                dq_ref[at:end, :] = dq.astype(BF16)
            else:
                dq_ref[at:end, :] = jnp.where(low[at:end], dq_ref[at:end, :], dq.astype(BF16))
            dk_part = jnp.dot(q_t[rows, at:end], ds, preferred_element_type=F32)
            dv_part = jnp.dot(dot_t[rows, at:end], wb, preferred_element_type=F32)
            if dk is None:
                dk, dv = dk_part, dv_part
            else:
                dk = jnp.concatenate([dk[:, :end] + dk_part, dk[:, end:]], axis=1)
                dv = jnp.concatenate([dv[:, :end] + dv_part, dv[:, end:]], axis=1)
        out_ref[1, rows, :] = dk.astype(BF16)
        out_ref[2, rows, :] = dv.astype(BF16)
    out_ref[0, :, :] = dq_ref[...].T


def attend_back(packed, grad_t, attended, lse):
    rows = packed.shape[0]
    width = packed.shape[1] // 3
    seqs = rows // LEN
    pairs = pl.cdiv(width, 2 * HD)
    kb, vb = width // (2 * HD), 2 * width // (2 * HD)

    def blk(f):
        return pl.BlockSpec((LEN, 2 * HD), f)

    out = pl.pallas_call(
        functools.partial(attend_back_kernel, width),
        grid=(seqs, pairs),
        in_specs=[
            blk(lambda s, p: (s, p)),
            blk(lambda s, p: (s, p + kb)),
            blk(lambda s, p: (s, p + kb + 1)),
            blk(lambda s, p: (s, p + vb)),
            pl.BlockSpec((2 * HD, LEN), lambda s, p: (p, s)),
            blk(lambda s, p: (s, p)),
            blk(lambda s, p: (s, 0)),
        ],
        out_specs=pl.BlockSpec((3, 2 * HD, LEN), lambda s, p: (0, p, s)),
        out_shape=shape_of((3, width, rows), BF16),
        scratch_shapes=[pltpu.VMEM((LEN, 2 * HD), BF16)],
        cost_estimate=cost(rows * LEN * width * 12, 14 * rows * width),
        compiler_params=params(), name="aback",
    )(packed, packed, packed, packed, grad_t, attended, lse)
    return out.reshape(3 * width, rows)


def project_kernel(
    side_ref, att_ref, x_ref, wo_ref, wa_ref, rows_ref,
    ao_ref, aa_ref, mid_ref, so_ref, sa_ref, n_ref, inv_ref,
):
    side = side_ref[0]
    store_pair(side, att_ref[...], ao_ref, aa_ref)
    mid = joined_dot(ao_ref[...], aa_ref[...], wo_ref[...], wa_ref[...])
    mid += x_ref[...].T.astype(F32) + rows_ref[4:5, :]
    mid_ref[...] = mid.astype(BF16).T
    centred = mid - jnp.mean(mid, axis=1, keepdims=True)
    inverse = lax.rsqrt(jnp.mean(centred * centred, axis=1, keepdims=True) + EPS)
    normed = centred * inverse
    act = (normed * rows_ref[5:6, :] + rows_ref[6:7, :]).astype(BF16)
    store_pair(side, act, so_ref, sa_ref)
    n_ref[...] = normed.astype(BF16).T
    inv_ref[...] = jnp.broadcast_to(inverse, (inverse.shape[0], 128)).T[:8]


def project(side, attended, tok_t, w_own, w_away, small_rows):
    width, rows = tok_t.shape
    half = width // 2
    wide = round_up(half, 128)
    block = min(256, rows)
    nat = pl.BlockSpec((block, width), lambda i, *_: (i, 0))
    pair = pl.BlockSpec((block, wide), lambda i, *_: (i, 0))
    whole = pl.BlockSpec((half, width), lambda i, *_: (0, 0))
    turned = pl.BlockSpec((width, block), lambda i, *_: (0, i))
    return pl.pallas_call(
        project_kernel,
        grid_spec=pltpu.PrefetchScalarGridSpec(
            num_scalar_prefetch=1,
            grid=(rows // block,),
            in_specs=[nat, turned, whole, whole, pl.BlockSpec((8, width), lambda i, *_: (0, 0))],
            out_specs=[
                pair, pair, turned, pair, pair, turned,
                pl.BlockSpec((8, block), lambda i, *_: (0, i)),
            ],
        ),
        out_shape=[
            shape_of((rows, wide), BF16),
            shape_of((rows, wide), BF16),
            shape_of((width, rows), BF16),
            shape_of((rows, wide), BF16),
            shape_of((rows, wide), BF16),
            shape_of((width, rows), BF16),
            shape_of((8, rows), F32),
        ],
        compiler_params=params(),
        cost_estimate=cost(4 * rows * half * width, 4 * half * width + 14 * rows * width),
        name="project",
    )(side, attended, tok_t, w_own, w_away, small_rows)


def hidden_kernel(start_ref, so_ref, sa_ref, wo_ref, wa_ref, bias_ref, act_ref, slope_ref):
    rows = so_ref.shape[0] // 2
    wo, wa = wo_ref[...], wa_ref[...]
    for at in range(0, so_ref.shape[0], rows):
        part = slice(at, at + rows)
        v = joined_dot(so_ref[part, :], sa_ref[part, :], wo, wa)
        v += bias_ref[8:9, :]
        square = v * v
        t = jnp.tanh(TANH_COEF * v * (1.0 + CUBIC * square))
        grown = 0.5 * (1.0 + t)
        act_ref[part, :] = (v * grown).astype(BF16)
        slope = grown * (1.0 + v * (1.0 - t) * (TANH_COEF + 3.0 * TANH_COEF * CUBIC * square))
        slope_ref[part, :] = slope.astype(BF16)


def hidden(start, own, away, w_own, w_away, bias, units):
    rows, wide = own.shape
    half = w_own.shape[0]
    tile = 640
    resident = pl.BlockSpec((rows, wide), lambda i, s: (0, 0))
    right = pl.BlockSpec((half, tile), lambda i, s: (0, s[0] + i))
    out = pl.BlockSpec((rows, tile), lambda i, s: (0, i))
    return pl.pallas_call(
        hidden_kernel,
        grid_spec=pltpu.PrefetchScalarGridSpec(
            num_scalar_prefetch=1,
            grid=(units // tile,),
            in_specs=[resident, resident, right, right, pl.BlockSpec((16, tile), lambda i, s: (0, i))],
            out_specs=[out, out],
        ),
        out_shape=[shape_of((rows, units), BF16)] * 2,
        compiler_params=params(),
        cost_estimate=cost(4 * rows * units * half, 4 * units * half + 4 * rows * units),
        name="hidden",
    )(start, own, away, w_own, w_away, bias)


def hidden_back_kernel(meta_ref, cot_ref, w1_hbm, w2_hbm, s1_hbm, s2_hbm, ge_ref, sum_ref, w_buf, s_buf, sem):
    steps, _, tile = w_buf.shape

    def block_of(first, second):
        return lambda i: (first if i < steps // 2 else second).at[:, pl.ds(i % (steps // 2) * tile, tile)]

    step = pl.program_id(0)
    stream(step, steps, (block_of(w1_hbm, w2_hbm), block_of(s1_hbm, s2_hbm)), (w_buf, s_buf), sem)
    ge = jnp.dot(cot_ref[...], w_buf[step], preferred_element_type=F32) * s_buf[step].astype(F32)
    ge_ref[...] = ge.astype(BF16).T
    sum_ref[...] = jnp.broadcast_to(jnp.sum(ge, axis=0, keepdims=True), sum_ref.shape)


def hidden_back(meta, cot, w_first_t, w_second_t, slope_first, slope_second):
    width, units = w_first_t.shape
    rows = cot.shape[0]
    tile = 640
    steps = units // tile
    place = lambda i, m: jnp.where(i < steps, (1 - m[0]) * steps + i, m[0] * steps + i - steps)
    return pl.pallas_call(
        hidden_back_kernel,
        grid_spec=pltpu.PrefetchScalarGridSpec(
            num_scalar_prefetch=1,
            grid=(2 * steps,),
            in_specs=[pl.BlockSpec((rows, width), lambda i, m: (0, 0))] + [ANYWHERE] * 4,
            out_specs=[
                pl.BlockSpec((tile, rows), lambda i, m: (place(i, m), 0)),
                pl.BlockSpec((8, tile), lambda i, m: (0, place(i, m))),
            ],
            scratch_shapes=[
                pltpu.VMEM((2 * steps, width, tile), BF16),
                pltpu.VMEM((2 * steps, rows, tile), BF16),
                pltpu.SemaphoreType.DMA((2, 2 * steps)),
            ],
        ),
        out_shape=[shape_of((2 * units, rows), BF16), shape_of((8, 2 * units), F32)],
        compiler_params=params(),
        cost_estimate=cost(4 * rows * units * width, 4 * units * width + 8 * rows * units),
        name="hback",
    )(meta, cot, w_first_t, w_second_t, slope_first, slope_second)


ROWS = 160


def middle_kernel(
    meta_ref, g_ref, wo_hbm, wa_hbm, n_hbm, inv_ref, gain_ref, cot_hbm, po_hbm, pa_hbm,
    gm_ref, gmb_ref, ga_ref, s_gain_ref, s_shift_ref, s_bias_ref,
    acc_ref, prod_ref, wo_buf, wa_buf, n_ref, cot_ref, p_ref, sem, sem_late,
):
    side = meta_ref[0]
    width = acc_ref.shape[0]
    half = width // 2
    i = pl.program_id(0)
    steps, tile, _ = wo_buf.shape
    rows = lambda ref: lambda i: ref.at[pl.ds(i * tile, tile), :]
    stream(i, steps, (rows(wo_hbm), rows(wa_hbm)), (wo_buf, wa_buf), sem)
    late = [
        pltpu.make_async_copy(src, dst, sem_late.at[j])
        for j, (src, dst) in enumerate(
            ((n_hbm, n_ref), (cot_hbm, cot_ref), (po_hbm, p_ref.at[0]), (pa_hbm, p_ref.at[1]))
        )
    ]

    @pl.when(i == 0)
    def _():
        for c in late:
            c.start()

    left = jnp.concatenate([wo_buf[i], wa_buf[i]], axis=0)
    total = jnp.dot(left, g_ref[...], preferred_element_type=F32)
    acc_ref[pl.ds(pl.multiple_of(side * half + i * tile, 8), tile), :] = total[:tile]
    acc_ref[pl.ds(pl.multiple_of((1 - side) * half + i * tile, 8), tile), :] = total[tile:]

    @pl.when(i == steps - 1)
    def _():
        for c in late:
            c.wait()
        tokens = acc_ref.shape[1]
        inverse = inv_ref[0:1, :]

        def first(j, sums):
            at = pl.ds(j * ROWS, ROWS)
            e, n = acc_ref[at, :], n_ref[at, :].astype(F32)
            w = e * gain_ref[at, 5:6]
            gmb_ref[at, :] = e.astype(BF16)
            prod_ref[at, :] = (e * n).astype(BF16)
            return (
                sums[0] + jnp.sum(w, axis=0, keepdims=True),
                sums[1] + jnp.sum(w * n, axis=0, keepdims=True),
            )

        zero = jnp.zeros((1, tokens), F32)
        one, two = lax.fori_loop(0, width // ROWS, first, (zero, zero))
        one, two = one / width, two / width
        s_gain_ref[...] = row_sums(prod_ref[...])
        s_shift_ref[...] = row_sums(gmb_ref[...])

        def second(j, _):
            at = pl.ds(j * ROWS, ROWS)
            n = n_ref[at, :].astype(F32)
            back = inverse * (acc_ref[at, :] * gain_ref[at, 5:6] - one - n * two)
            g = cot_ref[at, :].astype(F32) + back
            gm_ref[at, :] = g
            gmb_ref[at, :] = g.astype(BF16)
            return 0

        lax.fori_loop(0, width // ROWS, second, 0)
        g = gmb_ref[...]
        s_bias_ref[...] = row_sums(g)
        part = half // 2

        def attended(j, _):
            which = jnp.bitwise_xor(j // 2, side)
            at = pl.multiple_of(j % 2 * part, 16)
            ga_ref[pl.ds(pl.multiple_of(which * half + at, 16), part), :] = jnp.dot(
                p_ref[j // 2, pl.ds(at, part), :], gmb_ref[...], preferred_element_type=F32
            ).astype(BF16)
            return 0

        lax.fori_loop(0, 4, attended, 0)


def middle_back(meta, ge, w_own, w_away, normed_t, inv_t, cols, cot_t, p_own, p_away):
    units, rows = ge.shape
    half = w_own.shape[0]
    width = 2 * half
    tile = 200
    steps = half // tile
    once = pl.Buffered(1)
    const = lambda shape: pl.BlockSpec(shape, lambda i, m: (0, 0), pipeline_mode=once)
    out = lambda shape: pl.BlockSpec(shape, lambda i, m: (0, 0))
    small = shape_of((8, width), F32)
    return pl.pallas_call(
        middle_kernel,
        grid_spec=pltpu.PrefetchScalarGridSpec(
            num_scalar_prefetch=1,
            grid=(steps,),
            in_specs=[
                const((units, rows)), ANYWHERE, ANYWHERE, ANYWHERE,
                const((8, rows)), const((width, 128)), ANYWHERE, ANYWHERE, ANYWHERE,
            ],
            out_specs=[out((width, rows))] * 3 + [out((8, width))] * 3,
            scratch_shapes=[
                pltpu.VMEM((width, rows), F32),
                pltpu.VMEM((width, rows), BF16),
                pltpu.VMEM((steps, tile, units), BF16),
                pltpu.VMEM((steps, tile, units), BF16),
                pltpu.VMEM((width, rows), BF16),
                pltpu.VMEM((width, rows), BF16),
                pltpu.VMEM((2, half, width), BF16),
                pltpu.SemaphoreType.DMA((2, steps)),
                pltpu.SemaphoreType.DMA((4,)),
            ],
        ),
        out_shape=[
            shape_of((width, rows), F32),
            shape_of((width, rows), BF16),
            shape_of((width, rows), BF16),
            small, small, small,
        ],
        compiler_params=params(),
        cost_estimate=cost(
            2 * rows * units * width + 2 * rows * width * width, 2 * units * width + 12 * rows * width
        ),
        name="middle",
    )(meta, ge, w_own, w_away, normed_t, inv_t, cols, cot_t, p_own, p_away)


def first_kernel(
    meta_ref, gp_ref, wo_hbm, wa_hbm, tok_hbm, gain_ref, gm_hbm,
    out_ref, s_gain_ref, s_shift_ref, s_pack_ref,
    acc_ref, prod_ref, e_ref, wo_buf, wa_buf, tok_ref, gm_ref, sem, sem_late,
):
    side = meta_ref[0]
    width = acc_ref.shape[0]
    half = width // 2
    i = pl.program_id(0)
    steps, tile, _ = wo_buf.shape
    rows = lambda ref: lambda i: ref.at[pl.ds(i * tile, tile), :]
    stream(i, steps, (rows(wo_hbm), rows(wa_hbm)), (wo_buf, wa_buf), sem)
    late = [
        pltpu.make_async_copy(src, dst, sem_late.at[j])
        for j, (src, dst) in enumerate(((tok_hbm, tok_ref), (gm_hbm, gm_ref)))
    ]

    @pl.when(i == 0)
    def _():
        for c in late:
            c.start()

    g = gp_ref[...]
    total = jnp.dot(
        jnp.concatenate([wo_buf[i], wa_buf[i]], axis=0), g, preferred_element_type=F32
    )
    acc_ref[pl.ds(pl.multiple_of(side * half + i * tile, 8), tile), :] = total[:tile]
    acc_ref[pl.ds(pl.multiple_of((1 - side) * half + i * tile, 8), tile), :] = total[tile:]

    @pl.when(i == 0)
    def _():
        s_pack_ref[...] = row_sums(g)

    @pl.when(i == pl.num_programs(0) - 1)
    def _():
        for c in late:
            c.wait()
        tokens = acc_ref.shape[1]
        zero = jnp.zeros((1, tokens), F32)
        loops = width // ROWS

        def total(j, s):
            return s + jnp.sum(tok_ref[pl.ds(j * ROWS, ROWS), :].astype(F32), axis=0, keepdims=True)

        mean = lax.fori_loop(0, loops, total, zero) / width

        def spread_of(j, s):
            c = tok_ref[pl.ds(j * ROWS, ROWS), :].astype(F32) - mean
            return s + jnp.sum(c * c, axis=0, keepdims=True)

        inverse = lax.rsqrt(lax.fori_loop(0, loops, spread_of, zero) / width + EPS)

        def first(j, sums):
            at = pl.ds(j * ROWS, ROWS)
            e = acc_ref[at, :]
            n = (tok_ref[at, :].astype(F32) - mean) * inverse
            w = e * gain_ref[at, 0:1]
            e_ref[at, :] = e.astype(BF16)
            prod_ref[at, :] = (e * n).astype(BF16)
            return (
                sums[0] + jnp.sum(w, axis=0, keepdims=True),
                sums[1] + jnp.sum(w * n, axis=0, keepdims=True),
            )

        one, two = lax.fori_loop(0, loops, first, (zero, zero))
        one, two = one / width, two / width
        s_gain_ref[...] = row_sums(prod_ref[...])
        s_shift_ref[...] = row_sums(e_ref[...])

        def second(j, _):
            at = pl.ds(j * ROWS, ROWS)
            n = (tok_ref[at, :].astype(F32) - mean) * inverse
            back = inverse * (acc_ref[at, :] * gain_ref[at, 0:1] - one - n * two)
            out_ref[at, :] = (gm_ref[at, :] + back).astype(BF16)
            return 0

        lax.fori_loop(0, loops, second, 0)


def first_back(meta, gp_t, w_own, w_away, tok_t, cols, gm_t):
    columns, rows = gp_t.shape
    half = w_own.shape[0]
    width = 2 * half
    tile = 200
    steps = half // tile
    const = lambda shape: pl.BlockSpec(shape, lambda i, m: (0, 0))
    return pl.pallas_call(
        first_kernel,
        grid_spec=pltpu.PrefetchScalarGridSpec(
            num_scalar_prefetch=1,
            grid=(steps,),
            in_specs=[
                const((columns, rows)), ANYWHERE, ANYWHERE, ANYWHERE, const((width, 128)), ANYWHERE,
            ],
            out_specs=[const((width, rows)), const((8, width)), const((8, width)), const((8, columns))],
            scratch_shapes=[
                pltpu.VMEM((width, rows), F32),
                pltpu.VMEM((width, rows), BF16),
                pltpu.VMEM((width, rows), BF16),
                pltpu.VMEM((steps, tile, columns), BF16),
                pltpu.VMEM((steps, tile, columns), BF16),
                pltpu.VMEM((width, rows), BF16),
                pltpu.VMEM((width, rows), F32),
                pltpu.SemaphoreType.DMA((2, steps)),
                pltpu.SemaphoreType.DMA((2,)),
            ],
        ),
        out_shape=[
            shape_of((width, rows), BF16),
            shape_of((8, width), F32),
            shape_of((8, width), F32),
            shape_of((8, columns), F32),
        ],
        compiler_params=params(),
        cost_estimate=cost(4 * rows * half * columns, 4 * half * columns + 2 * rows * columns + 10 * rows * width),
        name="first",
    )(meta, gp_t, w_own, w_away, tok_t, cols, gm_t)


def output_kernel(a1_ref, a2_ref, w1_hbm, w2_hbm, mid_ref, cols_ref, out_ref, w1_buf, w2_buf, sem):
    i = pl.program_id(0)
    steps, tile, _ = w1_buf.shape
    rows = lambda ref: lambda i: ref.at[pl.ds(i * tile, tile), :]
    stream(i, steps, (rows(w1_hbm), rows(w2_hbm)), (w1_buf, w2_buf), sem)
    weights = jnp.concatenate([w1_buf[i], w2_buf[i]], axis=1)
    acts = jnp.concatenate([a1_ref[...], a2_ref[...]], axis=1)
    total = lax.dot_general(weights, acts, NT, preferred_element_type=F32)
    out_ref[...] = (total + mid_ref[...].astype(F32) + cols_ref[:, 7:8]).astype(BF16)


def block_output(act_first, act_second, w_away_t, w_own_t, middle_t, cols):
    rows, units = act_first.shape
    width = w_own_t.shape[0]
    tile = 400
    left = pl.BlockSpec((rows, units), lambda i: (0, 0))
    steps = width // tile
    part = pl.BlockSpec((tile, rows), lambda i: (i, 0))
    return pl.pallas_call(
        output_kernel,
        grid=(width // tile,),
        in_specs=[left, left, ANYWHERE, ANYWHERE, part, pl.BlockSpec((tile, 128), lambda i: (i, 0))],
        out_specs=part,
        scratch_shapes=[pltpu.VMEM((steps, tile, units), BF16)] * 2 + [pltpu.SemaphoreType.DMA((2, steps))],
        out_shape=shape_of((width, rows), BF16),
        compiler_params=params(),
        cost_estimate=cost(4 * rows * units * width, 4 * units * width + 4 * rows * units + 6 * rows * width),
        name="output",
    )(act_first, act_second, w_away_t, w_own_t, middle_t, cols)


class Group:
    def __init__(self, count, lanes, chunks, plan):
        self.count, self.lanes, self.chunks = count, lanes, chunks
        shares, orders = plan
        bits = count.bit_length() - 1
        self.orders = [list(order) + list(range(len(order), bits)) for order in orders]
        tiles = lanes // 128
        one, two = (round(tiles * share) for share in shares)
        self.cuts = [0, one * 128, (one + two) * 128, tiles * 128]
        self.widths = [self.cuts[k + 1] - self.cuts[k] for k in range(3)]
        self.left_over = lanes % 128
        self.pieces = self.widths[2] // self.left_over if self.left_over else 0

    def padded(self, which):
        return round_up(self.chunks[which], 16)

    def each(self, which):
        return pl.cdiv(self.chunks[which], self.pieces)

    def packed(self, which):
        return round_up(self.each(which), 16) if self.left_over else 0

    def rows(self, k, which):
        return self.padded(which) + (self.packed(which) if k == 2 else 0)

    def base(self, k, which):
        return sum(self.rows(k, w) for w in range(which))

    def total_rows(self, k):
        return self.base(k, len(self.chunks))


SLOTS = 4


def spread_kernel(spec, meta_ref, *refs):
    group, batches, starts = spec
    members = len(batches)
    inputs, refs = refs[: 4 * members], refs[4 * members :]
    keeps, sends, refs = refs[:3], refs[3:6], refs[6:]
    step = pl.program_id(0)
    rank = meta_ref[0]
    half = group.count // 2
    lanes = group.lanes

    def member(which):
        lo_ref, la_ref, ro_ref, ra_ref = inputs[4 * which : 4 * which + 4]
        stages, sem = refs[4 * which : 4 * which + 3], refs[4 * which + 3]
        chunk, batch = group.chunks[which], batches[which]
        padded = group.padded(which)

        def rows_of(k):
            return pl.ds(group.base(k, which), group.rows(k, which))

        def wait_slot(slot):
            for k in range(3):
                pltpu.make_async_copy(
                    stages[k].at[slot], keeps[k].at[0, rows_of(k), :], sem.at[k, slot]
                ).wait()

        def work():
            local = step - starts[which]
            total = joined_dot(lo_ref[...], la_ref[...], ro_ref[:, :lanes], ra_ref[:, :lanes])
            for s in range(batch):
                index = local * batch + s
                slot = s % SLOTS if batch % SLOTS == 0 else lax.rem(index, SLOTS)
                if s >= SLOTS:
                    wait_slot(slot)
                else:
                    pl.when(index >= SLOTS)(lambda slot=slot: wait_slot(slot))
                mixed = jnp.bitwise_xor(index, rank)
                part = total[s * chunk : (s + 1) * chunk]
                for k in range(3):
                    low, width = group.cuts[k], group.widths[k]
                    stages[k][slot, :chunk, :] = part[:, low : low + width].astype(BF16)
                    if k == 2 and group.left_over:
                        each, pieces = group.each(which), group.pieces
                        extra = part[:, low + width :]
                        if pieces * each > chunk:
                            extra = jnp.concatenate(
                                [extra, jnp.zeros((pieces * each - chunk, group.left_over), F32)], axis=0
                            )
                        extra = jnp.concatenate(
                            [extra[j * each : (j + 1) * each] for j in range(pieces)], axis=1
                        )
                        stages[k][slot, padded : padded + each, :] = extra.astype(BF16)
                    place = jnp.int32(0)
                    order = group.orders[k]
                    for depth, bit in enumerate(order):
                        place += ((mixed >> bit) & 1) << (len(order) - 1 - depth)

                    @pl.when(place < half)
                    def _(k=k, slot=slot, place=place):
                        pltpu.make_async_copy(
                            stages[k].at[slot], keeps[k].at[place, rows_of(k), :], sem.at[k, slot]
                        ).start()

                    @pl.when(place >= half)
                    def _(k=k, slot=slot, place=place):
                        pltpu.make_async_copy(
                            stages[k].at[slot], sends[k].at[place - half, rows_of(k), :], sem.at[k, slot]
                        ).start()

        return work, wait_slot

    parts = [member(which) for which in range(members)]
    for which, (work, _) in enumerate(parts):
        if members == 1:
            work()
        else:
            pl.when((step >= starts[which]) & (step < starts[which + 1]))(work)

    @pl.when(step == starts[members] - 1)
    def _():
        for _, wait_slot in parts:
            for slot in range(SLOTS):
                wait_slot(slot)


def spread(group, meta, lefts, rights):
    count = group.count
    batches, starts, specs, scratch, ins = [], [0], [], [], []
    flops = 0
    for which, ((left_own, left_away), right) in enumerate(zip(lefts, rights)):
        columns, tokens = left_own.shape
        chunk = group.chunks[which]
        batch = 1
        while batch * chunk % 16:
            batch *= 2
        steps, start = columns // (batch * chunk), starts[-1]
        left = pl.BlockSpec(
            (batch * chunk, tokens),
            lambda i, *_, start=start, steps=steps: (jnp.clip(i - start, 0, steps - 1), 0),
        )
        whole = pl.BlockSpec(right[0].shape, lambda i, *_: (0, 0))
        specs += [left, left, whole, whole]
        ins += [left_own, left_away, *right]
        scratch += [pltpu.VMEM((SLOTS, group.rows(k, which), group.widths[k]), BF16) for k in range(3)]
        scratch.append(pltpu.SemaphoreType.DMA((3, SLOTS)))
        batches.append(batch)
        starts.append(start + steps)
        flops += 4 * columns * tokens * group.lanes
    outs = [shape_of((count // 2, group.total_rows(k), group.widths[k]), BF16) for k in range(3)] * 2
    return pl.pallas_call(
        functools.partial(spread_kernel, (group, batches, starts)),
        grid_spec=pltpu.PrefetchScalarGridSpec(
            num_scalar_prefetch=1,
            grid=(starts[-1],),
            in_specs=specs,
            out_specs=[ANYWHERE] * len(outs),
            scratch_shapes=scratch,
        ),
        out_shape=outs,
        compiler_params=params(),
        cost_estimate=cost(flops, flops // 256),
        name="spread",
    )(meta, *ins)


def merge_kernel(*refs):
    for k in range(3):
        keep_low, came_low, keep_high, came_high = refs[4 * k : 4 * k + 4]
        keep, send = refs[12 + k], refs[15 + k]
        keep[...] = (keep_low[...].astype(F32) + came_low[...].astype(F32)).astype(BF16)
        send[...] = (keep_high[...].astype(F32) + came_high[...].astype(F32)).astype(BF16)


def merge(keeps, arrived):
    half = keeps[0].shape[0] // 2
    ins, specs, outs, out_specs = [], [], [], []
    moved = 0
    for keep, came in zip(keeps, arrived):
        shape = (1,) + keep.shape[1:]
        low = pl.BlockSpec(shape, lambda i: (i, 0, 0))
        high = pl.BlockSpec(shape, lambda i: (i + half, 0, 0))
        ins += [keep, came, keep, came]
        specs += [low, low, high, high]
        outs.append(shape_of((half,) + keep.shape[1:], BF16))
        out_specs.append(low)
        moved += 6 * keep.size
    return pl.pallas_call(
        merge_kernel,
        grid=(half,),
        in_specs=specs,
        out_specs=out_specs * 2,
        out_shape=outs * 2,
        compiler_params=params(),
        cost_estimate=cost(0, moved),
        name="merge",
    )(*ins)


def finish_kernel(group, *refs):
    outs = refs[6:]
    totals = [refs[2 * k][0].astype(F32) + refs[2 * k + 1][0].astype(F32) for k in range(3)]
    for which, chunk in enumerate(group.chunks):
        out = outs[which]
        for k in range(3):
            base = group.base(k, which)
            out[:, group.cuts[k] : group.cuts[k + 1]] = totals[k][base : base + chunk]
        width = group.left_over
        if width:
            base = group.base(2, which) + group.padded(which)
            rest = totals[2][base : base + group.each(which)]
            rest = jnp.concatenate([rest[:, j * width : (j + 1) * width] for j in range(group.pieces)], axis=0)
            out[:, group.cuts[3] :] = rest[:chunk]


def finish(group, keeps, arrived):
    ins = []
    for keep, came in zip(keeps, arrived):
        ins += [keep, came]
    res = pl.pallas_call(
        functools.partial(finish_kernel, group),
        out_shape=[shape_of((chunk, group.lanes), F32) for chunk in group.chunks],
        compiler_params=params(),
        cost_estimate=cost(0, 8 * sum(group.chunks) * group.lanes),
        name="finish",
    )(*ins)
    return [x.T for x in res]


ORDER = (
    "sc", "hb", "mid", "mc", "e", "ab", "mc", "sh", "me", "mc", "first", "s", "mh", "s", "me",
    "mh", "s", "me", "out", "s", "mc", "s", "mh", "s", "me", "mh",
)

PLANS = (
    ((0.36, 0.36), ((0, 2, 1, 3), (1, 0, 2, 3), (2, 1, 0, 3))),
    ((0.33, 0.33), ((0, 1, 2, 3), (1, 2, 0, 3), (2, 0, 1, 3))),
    ((0.5, 0.33), ((0, 1, 2, 3), (1, 0, 2, 3), (2, 1, 0, 3))),
)


def all_steps(bits):
    steps = list(ORDER)
    for name in ("mc", "me", "mh"):
        steps += [name] * (bits - steps.count(name))
    return steps + ["s"] * (bits + 2 - steps.count("s"))


def solution(mesh):
    count = mesh.shape["rep"]
    assert mesh.shape["grp"] == 2
    bits = count.bit_length() - 1
    assert 1 << bits == count and bits >= 4

    def per_device(
        tokens,
        first_gain,
        first_shift,
        w_heads,
        query_bias,
        value_bias,
        w_project,
        project_bias,
        second_gain,
        second_shift,
        w_expand,
        expand_bias,
        w_contract,
        contract_bias,
        cotangent,
    ):
        width = tokens.shape[1]
        units = w_contract.shape[0]
        side = lax.axis_index("grp")
        rank = lax.axis_index("rep")
        sides = jnp.reshape(side, (1,))

        smalls = (
            first_gain,
            first_shift,
            query_bias,
            value_bias,
            project_bias,
            second_gain,
            second_shift,
            contract_bias,
            expand_bias,
        )
        tok_t, cot_t, contract_own = tokens.T, cotangent.T, w_contract.T
        own_small = gather_smalls(smalls)
        away_small = swap_group(own_small)
        heads_in, _ = lax.optimization_barrier((w_heads, own_small))
        heads_away = swap_group(heads_in)
        small_rows, cols, packed_row = unpack_smalls(sides, own_small, away_small, width)
        first_own, first_out, cot, cot_sum = prep(sides, tok_t, cot_t, cols)
        w_project_in, _ = lax.optimization_barrier((w_project, first_own))
        project_away = swap_group(w_project_in)
        packed = heads_project(first_own, first_out, w_heads, heads_away, packed_row)

        latest = [packed]


        def hold(x):
            return lax.optimization_barrier((x, latest[0]))[0]

        def held(out):
            latest[0] = jax.tree.leaves(out)[0]
            return out

        w_expand_in, _ = lax.optimization_barrier((hold(w_expand), project_away))
        expand_away = swap_group(w_expand_in)
        contract_away = swap_group(hold(contract_own))
        cot_away_t = swap_group(hold(cot_t))
        first_away = swap_group(hold(first_out))

        tiles = units // 640
        start_first = jnp.reshape((1 - side) * tiles, (1,)).astype(jnp.int32)
        start_second = jnp.reshape(side * tiles, (1,)).astype(jnp.int32)

        def do_hidden(start, bias):
            return held(hidden(start, second_own, second_out, w_expand, expand_away, hold(bias), units))

        attended, lse = held(attend(packed))
        att_own, att_out, middle_t, second_own, second_out, normed_t, inv_t = held(project(
            sides, attended, tok_t, w_project, project_away, small_rows
        ))
        act_first, slope_first = do_hidden(start_first, away_small)
        act_away = swap_group(act_first)
        act_second, slope_second = do_hidden(start_second, own_small)

        chunk_d = width // count
        chunk_f = 2 * units // count
        chunk_h = w_heads.shape[1] // count
        groups = {
            "c": Group(count, units, [chunk_d], PLANS[0]),
            "e": Group(count, width // 2, [chunk_f, chunk_d], PLANS[1]),
            "h": Group(count, width // 2, [chunk_h], PLANS[2]),
        }
        rank_of = jnp.reshape(rank, (1,)).astype(jnp.int32)
        state, results = {}, {}
        r = types.SimpleNamespace()

        def send(name, buffers):
            group = groups[name]
            state[name] = [list(buffers[:3]), 0, [
                exchange(buffers[3 + k], 1 << group.orders[k][0], count) for k in range(3)
            ]]

        def advance(name):
            group = groups[name]
            keeps, depth, arrived = state[name]
            keeps = [hold(keeps[0])] + keeps[1:]
            if depth == bits - 1:
                results[name] = held(finish(group, keeps, arrived))
                return
            buffers = held(merge(keeps, arrived))
            state[name] = [list(buffers[:3]), depth + 1, [
                exchange(buffers[3 + k], 1 << group.orders[k][depth + 1], count) for k in range(3)
            ]]

        def do_contract():
            send("c", held(spread(
                groups["c"], hold(rank_of), [(cot_t, cot_away_t)], [(act_second, act_away)]
            )))

        def do_hidden_back():
            r.ge, r.eb = held(hidden_back(
                hold(sides), cot, contract_away, contract_own, slope_first, slope_second
            ))
            r.ge_away = swap_group(r.ge)
            r.second_away = swap_group(second_out)
            r.att_away = swap_group(att_out)

        def do_middle():
            r.gm_t, r.gmb_t, r.ga_t, r.s_gain2, r.s_shift2, r.s_pb = held(middle_back(
                hold(sides), r.ge, w_expand, expand_away, normed_t, inv_t,
                cols, cot_t, w_project, project_away,
            ))
            r.gmb_away = swap_group(r.gmb_t)

        def do_expand():
            send("e", held(spread(
                groups["e"], hold(rank_of), [(r.ge, r.ge_away), (r.gmb_t, r.gmb_away)],
                [(second_own, r.second_away), (att_own, r.att_away)],
            )))

        def do_attend_back():
            r.gp_t = held(attend_back(hold(packed), r.ga_t, attended, lse))
            r.gp_away = swap_group(r.gp_t)

        def do_heads():
            send("h", held(spread(
                groups["h"], hold(rank_of), [(r.gp_t, r.gp_away)], [(first_own, first_away)]
            )))

        def do_first():
            r.grad_tokens_t, r.s_gain1, r.s_shift1, r.s_pack = held(first_back(
                hold(sides), r.gp_t, w_heads, heads_away, tok_t, cols, r.gm_t
            ))

        def do_output():
            r.block_out_t = held(
                block_output(hold(act_first), act_second, contract_away, contract_own, middle_t, cols)
            )

        small = []

        def do_small():
            if not small:
                mine, theirs = held(collect(
                    hold(sides), r.s_pack, r.eb,
                    [r.s_gain1, r.s_shift1, r.s_pb, r.s_gain2, r.s_shift2, cot_sum],
                ))
                small.extend([mine, swap_group(theirs), 0])
                return
            vector, arrived, bit = small
            if bit == bits:
                small[0] = held(divide(hold(vector), arrived, [width // 2] * 8 + [units]))
                return
            vector = held(add(hold(vector), arrived))
            small[:] = [vector, exchange(vector, 1 << (bits - 1 - bit), count), bit + 1]

        steps = {
            "sc": do_contract, "hb": do_hidden_back, "mid": do_middle,
            "e": do_expand, "ab": do_attend_back,
            "sh": do_heads, "first": do_first, "out": do_output, "s": do_small,
            "mc": lambda: advance("c"), "me": lambda: advance("e"),
            "mh": lambda: advance("h"),
        }
        for name in all_steps(bits):
            steps[name]()
        finals = small[0]
        (out_w_contract,) = results["c"]
        out_w_expand, out_w_project = results["e"]
        (out_w_heads,) = results["h"]
        grad_tokens_t, block_out_t = r.grad_tokens_t, r.block_out_t

        return (
            block_out_t.T,
            grad_tokens_t.T,
            finals[0],
            finals[1],
            out_w_heads,
            finals[2],
            finals[3],
            out_w_project,
            finals[4],
            finals[5],
            finals[6],
            out_w_expand,
            finals[8],
            out_w_contract,
            finals[7],
        )

    placed = (
        P(("rep", "grp"), None),
        P("grp"),
        P("grp"),
        P("grp", None),
        P("grp"),
        P("grp"),
        P("grp", None),
        P("grp"),
        P("grp"),
        P("grp"),
        P("grp", None),
        P("grp"),
        P("grp", None),
        P("grp"),
        P(("rep", "grp"), None),
    )
    return jax.shard_map(
        per_device,
        mesh=mesh,
        in_specs=placed,
        out_specs=(
            P(("rep", "grp"), None),
            P(("rep", "grp"), None),
            P("grp"),
            P("grp"),
            P("grp", "rep"),
            P("grp"),
            P("grp"),
            P("grp", "rep"),
            P("grp"),
            P("grp"),
            P("grp"),
            P("grp", "rep"),
            P("grp"),
            P("grp", "rep"),
            P("grp"),
        ),
        check_vma=False,
    )
```
